32 devices in a mesh: row: 2 (over y), col: 4 (over z), layer: 4 (over x, core).
Axes of the slice: x: 2, y: 2, z: 4, core: 2. Of those that a mesh axis runs over, the one named last changes fastest.
Arguments:
- density_tiles: bfloat16 [192, 4, 2, 128, 128], P(('row', 'col')), may hold values from -1.5 to 1.5
- tile_columns: int32 [192, 4, 2], P(('row', 'col')), may hold values from -1 to 191, as said below
Outputs:
- square_tiles: bfloat16 [192, 4, 2, 128, 128], P(('row', 'col'), None, None, 'layer')
The draws below stay inside these ranges and needn't reach their ends.
Inputs may be any that keep to these rules, and one draw needn't show every extreme that they name: `tile_columns`: entry [i, g, s] is a tile column in group g (columns g * 48 to (g + 1) * 48 - 1) or -1; within one block row and group the listed columns are distinct and empty slots come after the listed ones; block row i lists its own column i in the first slot of its group, whose 2 slots are all listed; other groups hold 0 to 2 listed tiles.
All inputs are finite; a program needn't handle non-finite values.
Results may differ from the reference program's by a relative error of at most 0.0048.
Values may be sent and summed in bfloat16 or wider, within the bound.
A program may use at most 128 MiB of HBM per device.

```python
import jax
import jax.numpy as jnp
from jax import lax

TB = 128
NB = 192
KG = 2
NGROUP = 4
GWIDTH = 48
N_LAYER = 4


def draw_tile_columns(key, part):
    shuffle_key, anchor_key, count_key = jax.random.split(jax.random.fold_in(key, 17), 3)
    row_index = jnp.arange(NB, dtype=jnp.int32)
    group_index = jnp.arange(NGROUP, dtype=jnp.int32)

    def shuffled(sub_key):
        return jax.random.permutation(sub_key, GWIDTH - 1)[:KG - 1].astype(jnp.int32)
    offsets = jax.vmap(shuffled)(jax.random.split(shuffle_key, NB * NGROUP)).reshape(NB, NGROUP, KG - 1)
    anchors = jax.random.randint(anchor_key, (NB, NGROUP), 0, GWIDTH).astype(jnp.int32)
    own_group = row_index // GWIDTH
    is_own = own_group[:, None] == group_index[None, :]
    anchors = jnp.where(is_own, (row_index % GWIDTH)[:, None], anchors)
    local_column = jnp.concatenate([anchors[:, :, None], (anchors[:, :, None] + 1 + offsets) % GWIDTH], axis=-1)
    apart = jnp.abs(group_index[None, :] - own_group[:, None])
    distance = jnp.minimum(apart, NGROUP - apart)
    drawn_count = jax.random.randint(count_key, (NB, NGROUP), 0, KG + 1).astype(jnp.int32)
    live_count = jnp.where(distance <= 1, KG, drawn_count)
    slot_index = jnp.arange(KG, dtype=jnp.int32)
    columns = local_column + group_index[None, :, None] * GWIDTH
    return jnp.where(slot_index[None, None, :] < live_count[:, :, None], columns, -1).astype(jnp.int32)


def block_scale(own_key, dims, shards, smallest, high):
    factor_of = 1.0
    for axis_at, parts in shards:
        steps = jax.random.uniform(jax.random.fold_in(jax.random.fold_in(own_key, 6), axis_at), (parts,), jnp.float32, smallest / len(shards), high / len(shards))
        factor_of = factor_of * jnp.repeat(jnp.exp(steps), dims[axis_at] // parts).reshape((-1,) + (1,) * (len(dims) - 1 - axis_at))
    return factor_of


def gaussian(key, extent, width, most, cuts=(), kind=jnp.bfloat16):
    gain = block_scale(key, extent, cuts, -0.22, 0.18) if cuts else 1.0
    result = jax.random.normal(key, extent, jnp.float32) * width * gain
    return jnp.minimum(jnp.maximum(result, -most), most).astype(kind)


def setup_inputs(seed: int = 0) -> dict:
    key_list = jax.random.split(jax.random.key(seed), 3)
    density_tiles = gaussian(key_list[0], (NB, NGROUP, KG, TB, TB), 0.25, 1.5, ((0, 8),))
    tile_columns = draw_tile_columns(jax.random.fold_in(key_list[2], 71), 0)
    return dict(density_tiles=density_tiles, tile_columns=tile_columns)


def reference(density_tiles, tile_columns):
    block_count, group_count, group_slots, tile_side, _ = density_tiles.shape
    row_width = group_count * group_slots
    per_layer = group_count // N_LAYER
    flat_tiles = density_tiles.reshape(block_count, row_width, tile_side, tile_side)
    flat_columns = tile_columns.reshape(block_count, row_width)

    def one_row(row_index):
        own_columns = flat_columns[row_index]
        own_tiles = flat_tiles[row_index]
        is_live = own_columns >= 0
        inner_rows = jnp.where(is_live, own_columns, 0).astype(jnp.int32)
        inner_columns = flat_columns[inner_rows]
        matches = (inner_columns[:, None, :] == own_columns[None, :, None]) & is_live[:, None, None] & is_live[None, :, None]
        slot_index = jnp.argmax(matches.astype(jnp.int32), axis=-1).astype(jnp.int32)
        located = jnp.any(matches, axis=-1)
        selected = flat_tiles[inner_rows[:, None], slot_index].astype(jnp.float32)
        selected = jnp.where(located[:, :, None, None], selected, jnp.float32(0.0))
        left_tiles = own_tiles.astype(jnp.float32).reshape(N_LAYER, per_layer * group_slots, tile_side, tile_side)
        selected = selected.reshape(N_LAYER, per_layer * group_slots, row_width, tile_side, tile_side)
        partial_value = jnp.einsum("larc,lascd->lsrd", left_tiles, selected)
        rounded = lax.optimization_barrier(partial_value.astype(jnp.bfloat16))
        layer_total = jnp.sum(rounded.astype(jnp.float32), axis=0)
        return layer_total.astype(jnp.bfloat16).reshape(group_count, group_slots, tile_side, tile_side)

    return lax.map(one_row, jnp.arange(block_count, dtype=jnp.int32))
```

```python
import functools

import jax
import jax.numpy as jnp
from jax import lax
from jax.experimental import pallas as pl
from jax.experimental.pallas import tpu as pltpu
from jax.sharding import PartitionSpec as P

MESH = pl.DeviceIdType.MESH


def divisor(total, most):
    return max(d for d in range(1, most + 1) if total % d == 0)


def kernel(
    sizes, columns_ref, tiles_ref, meta_ref, out_ref,
    left, right, meta_all, meta_smem, stage,
    local_sem, meta_send, meta_recv, send_sem, recv_sem, out_send, out_recv,
):
    row_count, col_count, layer_count, chunks, out_chunks, is_balanced = sizes
    n, group_count, slots, tile, _ = tiles_ref.shape
    cells = row_count * col_count
    per_layer = group_count // layer_count
    quarter = tile // layer_count
    width = group_count * slots
    r, c, l = lax.axis_index("row"), lax.axis_index("col"), lax.axis_index("layer")
    me = r * col_count + c
    own_groups = pl.ds(l * per_layer, per_layer)

    own_copy = pltpu.make_async_copy(
        tiles_ref.at[:, own_groups], right.at[pl.ds(me * n, n)], local_sem.at[0]
    )
    left_copy = pltpu.make_async_copy(tiles_ref, left, local_sem.at[1])
    meta_copy = pltpu.make_async_copy(meta_ref, meta_all.at[pl.ds(me * n, n)], local_sem.at[2])
    own_copy.start()
    meta_copy.start()
    left_copy.start()
    right[cells * n] = jnp.zeros(right.shape[1:], right.dtype)

    def cell_id(offset):
        target = lax.rem(me + offset, cells)
        return {"row": lax.div(target, col_count), "col": lax.rem(target, col_count)}

    def layer_id(offset):
        return {"layer": lax.rem(l + offset, layer_count)}

    barrier = pltpu.get_barrier_semaphore()
    for offset in range(1, cells):
        pl.semaphore_signal(barrier, inc=1, device_id=cell_id(offset), device_id_type=MESH)
    for offset in range(1, layer_count):
        pl.semaphore_signal(barrier, inc=1, device_id=layer_id(offset), device_id_type=MESH)
    pl.semaphore_wait(barrier, cells - 1 + layer_count - 1)
    own_copy.wait()

    step_rows = n // chunks
    sent = []

    def rows_of(cell, chunk):
        return pl.ds(cell * n + chunk * step_rows, step_rows)

    def copy_of(cell, chunk, way, device):
        return pltpu.make_async_remote_copy(
            src_ref=right.at[rows_of(cell, chunk)],
            dst_ref=right.at[rows_of(cell, chunk)],
            send_sem=send_sem.at[way, cell, chunk],
            recv_sem=recv_sem.at[cell, chunk],
            device_id=device,
            device_id_type=MESH,
        )

    ways = {
        "up": (0, c < col_count - 1, {"col": jnp.minimum(c + 1, col_count - 1)}),
        "down": (1, c > 0, {"col": jnp.maximum(c - 1, 0)}),
        "south": (2, r < row_count - 1, {"row": jnp.minimum(r + 1, row_count - 1)}),
        "north": (3, r > 0, {"row": jnp.maximum(r - 1, 0)}),
    }

    def send(cell, chunk, way, condition=True):
        index, exists, device = ways[way]
        wanted = jnp.logical_and(exists, condition)

        @pl.when(wanted)
        def _():
            copy_of(cell, chunk, index, device).start()

        sent.append((wanted, cell, chunk, index, device))

    def await_arrival(cell, chunk):
        copy_of(cell, chunk, 0, {"col": c}).wait_recv()

    for chunk in range(chunks):
        for way in ("up", "down", "south", "north"):
            send(me, chunk, way)

    meta_copy.wait()
    meta_copies = []
    for offset in range(1, cells):
        copy = pltpu.make_async_remote_copy(
            src_ref=meta_ref,
            dst_ref=meta_all.at[pl.ds(me * n, n)],
            send_sem=meta_send.at[offset],
            recv_sem=meta_recv.at[offset],
            device_id=cell_id(offset),
            device_id_type=MESH,
        )
        copy.start()
        meta_copies.append(copy)

    even = lax.rem(c, 2) == 0
    for step in range(1, col_count):
        for chunk in range(chunks):
            for origin, has, way, is_pair in (
                (c - step, c >= step, "up", jnp.logical_not(even)),
                (c + step, c + step < col_count, "down", even),
            ):
                origin = jnp.clip(origin, 0, col_count - 1)
                cell = r * col_count + origin

                @pl.when(has)
                def _():
                    await_arrival(cell, chunk)

                send(cell, chunk, way, has)
                across = has
                if is_balanced and step == 1 and chunk >= chunks // 2:
                    across = jnp.logical_and(has, jnp.logical_not(is_pair))
                send(cell, chunk, "south", across)
                send(cell, chunk, "north", across)

    if is_balanced:
        other = (1 - r) * col_count + c
        for chunk in range(chunks):
            await_arrival(other, chunk)
            if chunk >= chunks // 2:
                send(other, chunk, "up", even)
                send(other, chunk, "down", jnp.logical_not(even))
        for step in range(1, col_count):
            origin = (1 - r) * col_count + lax.rem(c + step, col_count)
            for chunk in range(chunks):
                await_arrival(origin, chunk)
    else:
        for step in range(1, row_count):
            for shift in range(col_count):
                for chunk in range(chunks):
                    for origin, has, way in (
                        (r - step, r >= step, "south"),
                        (r + step, r + step < row_count, "north"),
                    ):
                        origin = jnp.clip(origin, 0, row_count - 1)
                        cell = origin * col_count + lax.rem(c + shift, col_count)

                        @pl.when(has)
                        def _():
                            await_arrival(cell, chunk)

                        send(cell, chunk, way, has)

    for copy in meta_copies:
        copy.wait()
    table_copy = pltpu.make_async_copy(meta_all, meta_smem, local_sem.at[3])
    table_copy.start()
    table_copy.wait()
    left_copy.wait()

    def one_row(i, carry):
        targets = [
            columns_ref[i * width + l * per_layer * slots + s] for s in range(per_layer * slots)
        ]
        strips = []
        for a in range(width):
            k = columns_ref[i * width + a]
            inner = jnp.maximum(k, 0)
            pieces = []
            for s in range(per_layer * slots):
                group = s // slots
                row_index = jnp.int32(cells * n)
                slot_index = jnp.int32(0)
                is_live = (k >= 0) & (targets[s] >= 0)
                for t in range(slots):
                    hit = (meta_smem[inner, 0, group * slots + t] == targets[s]) & is_live
                    row_index = jnp.where(hit, inner, row_index)
                    slot_index = jnp.where(hit, t, slot_index)
                pieces.append(right[row_index, group, slot_index])
            strips.append(jnp.concatenate(pieces, axis=1))
        rights = jnp.concatenate(strips, axis=0)
        lefts = jnp.concatenate(
            [left[i, a // slots, a % slots] for a in range(width)], axis=1
        )
        total = jnp.dot(lefts, rights, preferred_element_type=jnp.float32).astype(stage.dtype)
        for q in range(layer_count):
            for s in range(per_layer * slots):
                stage[q, i, s // slots, s % slots] = total[
                    q * quarter:(q + 1) * quarter, s * tile:(s + 1) * tile
                ]
        return carry

    out_rows = n // out_chunks

    def out_copies(chunk):
        rows = pl.ds(chunk * out_rows, out_rows)
        copies = []
        for offset in range(layer_count):
            q = lax.rem(l + offset, layer_count)
            if offset == 0:
                copies.append(pltpu.make_async_copy(
                    stage.at[q, rows], out_ref.at[rows, own_groups], out_send.at[0, chunk]
                ))
            else:
                copies.append(pltpu.make_async_remote_copy(
                    src_ref=stage.at[q, rows],
                    dst_ref=out_ref.at[rows, own_groups],
                    send_sem=out_send.at[offset, chunk],
                    recv_sem=out_recv.at[offset, chunk],
                    device_id=layer_id(offset),
                    device_id_type=MESH,
                ))
        return copies

    all_out = []
    for chunk in range(out_chunks + 1):
        if chunk < out_chunks:
            lax.fori_loop(chunk * out_rows, (chunk + 1) * out_rows, one_row, 0)
        if chunk > 0:
            copies = out_copies(chunk - 1)
            for copy in copies[1:] + copies[:1]:
                copy.start()
            all_out.extend(copies)

    for wanted, cell, chunk, index, device in sent:
        @pl.when(wanted)
        def _():
            copy_of(cell, chunk, index, device).wait_send()

    for copy in all_out:
        copy.wait()


def on_device(density_tiles, tile_columns):
    row_count = lax.axis_size("row")
    col_count = lax.axis_size("col")
    layer_count = lax.axis_size("layer")
    n, group_count, slots, tile, _ = density_tiles.shape
    cells = row_count * col_count
    per_layer = group_count // layer_count
    quarter = tile // layer_count
    kept = per_layer * slots
    chunks = divisor(n, 4)
    out_chunks = divisor(n, 4)
    is_balanced = row_count == 2 and col_count % 2 == 0 and chunks % 2 == 0
    own = lax.dynamic_slice_in_dim(tile_columns, lax.axis_index("layer") * per_layer, per_layer, 1)
    meta = jnp.pad(own.reshape(n, 1, kept), ((0, 0), (0, 0), (0, 128 - kept)), constant_values=-1)
    dtype = density_tiles.dtype
    sizes = (row_count, col_count, layer_count, chunks, out_chunks, is_balanced)
    return pl.pallas_call(
        functools.partial(kernel, sizes),
        out_shape=jax.ShapeDtypeStruct((n, group_count, slots, quarter, tile), dtype),
        in_specs=[
            pl.BlockSpec(memory_space=pltpu.SMEM),
            pl.BlockSpec(memory_space=pl.ANY),
            pl.BlockSpec(memory_space=pltpu.VMEM),
        ],
        out_specs=pl.BlockSpec(memory_space=pl.ANY),
        scratch_shapes=[
            pltpu.VMEM(density_tiles.shape, dtype),
            pltpu.VMEM((cells * n + 1, per_layer, slots, tile, tile), dtype),
            pltpu.VMEM((cells * n, 1, 128), jnp.int32),
            pltpu.SMEM((cells * n, 1, 128), jnp.int32),
            pltpu.VMEM((layer_count, n, per_layer, slots, quarter, tile), dtype),
            pltpu.SemaphoreType.DMA((4,)),
            pltpu.SemaphoreType.DMA((cells,)),
            pltpu.SemaphoreType.DMA((cells,)),
            pltpu.SemaphoreType.DMA((4, cells, chunks)),
            pltpu.SemaphoreType.DMA((cells, chunks)),
            pltpu.SemaphoreType.DMA((layer_count, out_chunks)),
            pltpu.SemaphoreType.DMA((layer_count, out_chunks)),
        ],
        compiler_params=pltpu.CompilerParams(
            collective_id=0, has_side_effects=True, vmem_limit_bytes=60 * 1024 * 1024
        ),
    )(tile_columns.reshape(-1), density_tiles, meta)


def paired_kernel(
    sizes, tiles_ref, meta_ref, out_ref,
    left, right, meta_all, meta_smem, stage,
    local_sem, meta_send, meta_recv, send_sem, recv_sem, left_send, left_recv, out_send, out_recv,
):
    col_count, layer_count, chunks, out_chunks = sizes
    n, group_count, slots, tile, _ = tiles_ref.shape
    cells = 2 * col_count
    per_layer = group_count // layer_count
    quarter = tile // layer_count
    width = group_count * slots
    r, c, l = lax.axis_index("row"), lax.axis_index("col"), lax.axis_index("layer")
    high, k = lax.div(l, 2), lax.rem(l, 2)
    me = r * col_count + c
    base = k * col_count + c
    is_home = k == r
    is_guest = jnp.logical_not(is_home)
    group = 2 * high + r
    own_groups = pl.ds(group * per_layer, per_layer)
    other_groups = pl.ds((2 * high + 1 - r) * per_layer, per_layer)
    facing = {"row": 1 - r}
    partner = {"layer": 2 * high + 1 - k}

    own_copy = pltpu.make_async_copy(
        tiles_ref.at[:, own_groups], right.at[pl.ds(me * n, n)], local_sem.at[0]
    )
    left_copy = pltpu.make_async_copy(tiles_ref, left, local_sem.at[1])
    meta_copy = pltpu.make_async_copy(meta_ref, meta_all.at[pl.ds(me * n, n)], local_sem.at[2])
    own_copy.start()
    meta_copy.start()

    @pl.when(is_home)
    def _():
        left_copy.start()

    right[cells * n] = jnp.zeros(right.shape[1:], right.dtype)

    def cell_id(offset):
        target = lax.rem(me + offset, cells)
        return {"row": lax.div(target, col_count), "col": lax.rem(target, col_count)}

    barrier = pltpu.get_barrier_semaphore()
    for offset in range(1, cells):
        pl.semaphore_signal(barrier, inc=1, device_id=cell_id(offset), device_id_type=MESH)
    for offset in range(1, layer_count):
        for row in (r, 1 - r):
            pl.semaphore_signal(
                barrier,
                inc=1,
                device_id={"row": row, "layer": lax.rem(l + offset, layer_count)},
                device_id_type=MESH,
            )
    pl.semaphore_wait(barrier, cells - 1 + 2 * (layer_count - 1))

    step_rows = n // chunks
    sent = []

    def rows_of(cell, chunk):
        return pl.ds(cell * n + chunk * step_rows, step_rows)

    def copy_of(cell, chunk, way, device):
        source = right.at[rows_of(cell, chunk)]
        if way == 3:
            source = tiles_ref.at[pl.ds(chunk * step_rows, step_rows), other_groups]
        return pltpu.make_async_remote_copy(
            src_ref=source,
            dst_ref=right.at[rows_of(cell, chunk)],
            send_sem=send_sem.at[way, cell, chunk],
            recv_sem=recv_sem.at[cell, chunk],
            device_id=device,
            device_id_type=MESH,
        )

    ways = {
        "up": (0, c < col_count - 1, {"col": jnp.minimum(c + 1, col_count - 1)}),
        "down": (1, c > 0, {"col": jnp.maximum(c - 1, 0)}),
        "partner": (2, True, partner),
        "facing": (3, True, facing),
    }

    def send(cell, chunk, way, condition):
        index, exists, device = ways[way]
        wanted = jnp.logical_and(exists, condition)

        @pl.when(wanted)
        def _():
            copy_of(cell, chunk, index, device).start()

        sent.append((wanted, cell, chunk, index, device))

    def await_arrival(cell, chunk, condition):
        @pl.when(condition)
        def _():
            copy_of(cell, chunk, 2, partner).wait_recv()

    for chunk in range(chunks):
        send(me, chunk, "facing", is_home)
    own_copy.wait()
    for chunk in range(chunks):
        for way in ("up", "down"):
            send(me, chunk, way, is_home)
    left_out = pltpu.make_async_remote_copy(
        src_ref=tiles_ref, dst_ref=left, send_sem=left_send, recv_sem=left_recv,
        device_id=facing, device_id_type=MESH,
    )

    meta_copy.wait()
    meta_copies = []
    for offset in range(1, cells):
        copy = pltpu.make_async_remote_copy(
            src_ref=meta_ref,
            dst_ref=meta_all.at[pl.ds(me * n, n)],
            send_sem=meta_send.at[offset],
            recv_sem=meta_recv.at[offset],
            device_id=cell_id(offset),
            device_id_type=MESH,
        )
        copy.start()
        meta_copies.append(copy)

    @pl.when(is_home)
    def _():
        left_out.start()

    for chunk in range(chunks):
        await_arrival(base, chunk, is_guest)
        for way in ("up", "down", "partner"):
            send(base, chunk, way, is_guest)

    for step in range(1, col_count):
        for chunk in range(chunks):
            for origin, has, way in (
                (c - step, c >= step, "up"),
                (c + step, c + step < col_count, "down"),
            ):
                cell = k * col_count + jnp.clip(origin, 0, col_count - 1)
                await_arrival(cell, chunk, has)
                send(cell, chunk, way, has)
                send(cell, chunk, "partner", has)

    for chunk in range(chunks):
        await_arrival((1 - k) * col_count + c, chunk, is_home)
    for step in range(1, col_count):
        cell = (1 - k) * col_count + lax.rem(c + step, col_count)
        for chunk in range(chunks):
            await_arrival(cell, chunk, True)

    for copy in meta_copies:
        copy.wait()
    table_copy = pltpu.make_async_copy(meta_all, meta_smem, local_sem.at[3])
    table_copy.start()
    table_copy.wait()

    @pl.when(is_home)
    def _():
        left_copy.wait()

    @pl.when(is_guest)
    def _():
        left_out.wait_recv()

    first = group * per_layer * slots

    def one_row(i, carry):
        block_row = base * n + i
        targets = [meta_smem[block_row, 0, first + s] for s in range(per_layer * slots)]
        strips = []
        for a in range(width):
            column = meta_smem[block_row, 0, a]
            inner = jnp.maximum(column, 0)
            pieces = []
            for s in range(per_layer * slots):
                part = s // slots
                row_index = jnp.int32(cells * n)
                slot_index = jnp.int32(0)
                is_live = (column >= 0) & (targets[s] >= 0)
                for t in range(slots):
                    hit = (meta_smem[inner, 0, first + part * slots + t] == targets[s]) & is_live
                    row_index = jnp.where(hit, inner, row_index)
                    slot_index = jnp.where(hit, t, slot_index)
                pieces.append(right[row_index, part, slot_index])
            strips.append(jnp.concatenate(pieces, axis=1))
        rights = jnp.concatenate(strips, axis=0)
        lefts = jnp.concatenate(
            [left[i, a // slots, a % slots] for a in range(width)], axis=1
        )
        total = jnp.dot(lefts, rights, preferred_element_type=jnp.float32).astype(stage.dtype)
        for q in range(layer_count):
            for s in range(per_layer * slots):
                stage[q, i, s // slots, s % slots] = total[
                    q * quarter:(q + 1) * quarter, s * tile:(s + 1) * tile
                ]
        return carry

    out_rows = n // out_chunks

    def out_copy(chunk, q, source):
        rows = pl.ds(chunk * out_rows, out_rows)
        return pltpu.make_async_remote_copy(
            src_ref=stage.at[q, rows],
            dst_ref=out_ref.at[rows, pl.ds(source * per_layer, per_layer)],
            send_sem=out_send.at[q, chunk],
            recv_sem=out_recv.at[source, chunk],
            device_id={"row": k, "layer": q},
            device_id_type=MESH,
        )

    def kept_copy(chunk):
        rows = pl.ds(chunk * out_rows, out_rows)
        return pltpu.make_async_copy(
            stage.at[l, rows], out_ref.at[rows, own_groups], out_send.at[l, chunk]
        )

    for chunk in range(out_chunks + 1):
        if chunk < out_chunks:
            lax.fori_loop(chunk * out_rows, (chunk + 1) * out_rows, one_row, 0)
        if chunk > 0:
            for offset in range(layer_count - 1, -1, -1):
                q = lax.rem(l + offset, layer_count)
                if offset:
                    out_copy(chunk - 1, q, group).start()
                else:
                    @pl.when(is_guest)
                    def _():
                        out_copy(chunk - 1, q, group).start()

                    @pl.when(is_home)
                    def _():
                        kept_copy(chunk - 1).start()

    for wanted, cell, chunk, index, device in sent:
        @pl.when(wanted)
        def _():
            copy_of(cell, chunk, index, device).wait_send()

    @pl.when(is_home)
    def _():
        left_out.wait_send()

    for chunk in range(out_chunks):
        for offset in range(layer_count):
            q = lax.rem(l + offset, layer_count)
            source = lax.rem(group + offset, layer_count)
            if offset:
                out_copy(chunk, q, source).wait()
            else:
                @pl.when(is_guest)
                def _():
                    out_copy(chunk, q, source).wait()

                @pl.when(is_home)
                def _():
                    kept_copy(chunk).wait()


def on_device_paired(density_tiles, tile_columns):
    col_count = lax.axis_size("col")
    layer_count = lax.axis_size("layer")
    n, group_count, slots, tile, _ = density_tiles.shape
    cells = 2 * col_count
    per_layer = group_count // layer_count
    quarter = tile // layer_count
    width = group_count * slots
    chunks = divisor(n, 2)
    out_chunks = divisor(n, 12)
    lanes = -(-width // 128) * 128
    meta = jnp.pad(
        tile_columns.reshape(n, 1, width), ((0, 0), (0, 0), (0, lanes - width)), constant_values=-1
    )
    dtype = density_tiles.dtype
    return pl.pallas_call(
        functools.partial(paired_kernel, (col_count, layer_count, chunks, out_chunks)),
        out_shape=jax.ShapeDtypeStruct((n, group_count, slots, quarter, tile), dtype),
        in_specs=[
            pl.BlockSpec(memory_space=pl.ANY),
            pl.BlockSpec(memory_space=pltpu.VMEM),
        ],
        out_specs=pl.BlockSpec(memory_space=pl.ANY),
        scratch_shapes=[
            pltpu.VMEM(density_tiles.shape, dtype),
            pltpu.VMEM((cells * n + 1, per_layer, slots, tile, tile), dtype),
            pltpu.VMEM((cells * n, 1, lanes), jnp.int32),
            pltpu.SMEM((cells * n, 1, lanes), jnp.int32),
            pltpu.VMEM((layer_count, n, per_layer, slots, quarter, tile), dtype),
            pltpu.SemaphoreType.DMA((4,)),
            pltpu.SemaphoreType.DMA((cells,)),
            pltpu.SemaphoreType.DMA((cells,)),
            pltpu.SemaphoreType.DMA((4, cells, chunks)),
            pltpu.SemaphoreType.DMA((cells, chunks)),
            pltpu.SemaphoreType.DMA,
            pltpu.SemaphoreType.DMA,
            pltpu.SemaphoreType.DMA((layer_count, out_chunks)),
            pltpu.SemaphoreType.DMA((layer_count, out_chunks)),
        ],
        compiler_params=pltpu.CompilerParams(
            collective_id=1, has_side_effects=True, vmem_limit_bytes=60 * 1024 * 1024
        ),
    )(density_tiles, meta)


def sparse_kernel(
    sizes, tiles_ref, meta_ref, out_ref, flag_ref,
    left, diag, extra, pack, stage, meta_all, meta_smem,
    send_list, send_smem, row_list, row_smem, flag_all,
    local_sem, meta_send, meta_recv, flag_send, flag_recv,
    main_send, main_recv, side_send, side_recv,
):
    row_count, col_count, layer_count, group_count, per_pair, per_row, padded = sizes
    n, width, tile, _ = tiles_ref.shape
    cells = row_count * col_count
    quarter = tile // layer_count
    entries = padded * width
    span = -(-(cells * n) // 128) * 128
    r, c, l = lax.axis_index("row"), lax.axis_index("col"), lax.axis_index("layer")
    x, k = lax.div(l, 2), lax.rem(l, 2)
    facing_layer = 2 * (1 - x) + k
    me = r * col_count + c
    own_slot = lax.div(me * n * group_count, cells * n) * (width // group_count)
    partner = {"layer": 2 * x + 1 - k}
    facing = {"layer": facing_layer}

    meta_copy = pltpu.make_async_copy(meta_ref, meta_all.at[me], local_sem.at[0])
    diag_copy = pltpu.make_async_copy(
        tiles_ref.at[:, own_slot], diag.at[pl.ds(me * n, n)], local_sem.at[1]
    )
    left_copy = pltpu.make_async_copy(tiles_ref, left, local_sem.at[2])
    table_copy = pltpu.make_async_copy(meta_ref, meta_smem, local_sem.at[3])
    diag_copy.start()
    meta_copy.start()
    table_copy.start()
    left_copy.start()

    def cell_id(cell):
        return {"row": lax.div(cell, col_count), "col": lax.rem(cell, col_count)}

    def other_cell(offset):
        return lax.rem(me + offset, cells)

    barrier = pltpu.get_barrier_semaphore()
    for offset in range(1, cells):
        pl.semaphore_signal(
            barrier, inc=1, device_id=cell_id(other_cell(offset)), device_id_type=MESH
        )
    for device in (partner, facing):
        pl.semaphore_signal(barrier, inc=1, device_id=device, device_id_type=MESH)
    pl.semaphore_wait(barrier, cells - 1 + 2)

    sent = []

    def remote(source, target, send, recv, device):
        return pltpu.make_async_remote_copy(
            src_ref=source, dst_ref=target, send_sem=send, recv_sem=recv,
            device_id=device, device_id_type=MESH,
        )

    def launch(copy, condition=True):
        if condition is True:
            copy.start()
        else:
            @pl.when(condition)
            def _():
                copy.start()
        sent.append((copy, condition))

    def await_recv(copy, condition=True):
        if condition is True:
            copy.wait_recv()
        else:
            @pl.when(condition)
            def _():
                copy.wait_recv()

    def part(kind, cell, q):
        buffer, count = ((diag, n), (extra, per_pair))[kind]
        return buffer.at[pl.ds(cell * count, count), pl.ds(q * quarter, quarter)]

    up = {"col": jnp.minimum(c + 1, col_count - 1)}
    down = {"col": jnp.maximum(c - 1, 0)}
    across = {"row": 1 - r}

    def line_copy(cell, way):
        device = (up, down, across)[way]
        piece = part(0, cell, l)
        return remote(piece, piece, main_send.at[0, way, cell], main_recv.at[0, cell], device)

    def side_copy(kind, cell, way):
        device = (partner, facing, partner)[way]
        piece = part(kind, cell, facing_layer if way == 2 else l)
        return remote(
            piece, piece, side_send.at[kind, way, cell], side_recv.at[kind, way, cell], device
        )

    diag_copy.wait()
    launch(line_copy(me, 0), c < col_count - 1)
    launch(line_copy(me, 1), c > 0)
    launch(line_copy(me, 2))
    meta_copies = []
    for offset in range(1, cells):
        copy = remote(
            meta_ref, meta_all.at[me], meta_send.at[offset], meta_recv.at[offset],
            cell_id(other_cell(offset)),
        )
        copy.start()
        meta_copies.append(copy)
    meta_copy.wait()
    for copy in meta_copies:
        copy.wait_recv()

    small_row = lax.broadcasted_iota(jnp.int32, (padded, 128), 0)
    small_lane = lax.broadcasted_iota(jnp.int32, (padded, 128), 1)
    wide_row = lax.broadcasted_iota(jnp.int32, (padded, span), 0)
    wide_lane = lax.broadcasted_iota(jnp.int32, (padded, span), 1)
    tall_row = lax.broadcasted_iota(jnp.int32, (span, 128), 0)
    entry_row = lax.broadcasted_iota(jnp.int32, (entries, 128), 0)
    entry_lane = lax.broadcasted_iota(jnp.int32, (entries, 128), 1).astype(jnp.float32)
    before = (
        lax.broadcasted_iota(jnp.int32, (entries, entries), 0)
        > lax.broadcasted_iota(jnp.int32, (entries, entries), 1)
    ).astype(jnp.float32).astype(jnp.bfloat16)
    ones = jnp.ones((128, 128), jnp.bfloat16)

    def dot(a, b):
        return jnp.dot(a, b, preferred_element_type=jnp.float32)

    def chosen(cell):
        columns = meta_all[cell, 0:padded]
        pieces = []
        for b in range(width):
            hit = (columns[:, b:b + 1] == wide_lane) & (wide_lane != wide_row + cell * n)
            pieces.append(jnp.where(hit, 1.0, 0.0))
        return jnp.concatenate(pieces, axis=0).astype(jnp.bfloat16)

    def listing(cell):
        rows = meta_all[cell, padded:padded + width]
        total = jnp.zeros((span, 128), jnp.float32)
        for a in range(width):
            total = jnp.where(rows[a:a + 1] == tall_row, a + 1.0, total)
        return total.astype(jnp.bfloat16)

    def inner_listing(source, cell):
        rows = meta_all[cell, padded:padded + width]
        total = jnp.zeros((padded, 128), jnp.float32)
        for a in range(width):
            total = jnp.where(rows[a:a + 1] == small_row + source * n, a + 1.0, total)
        total = jnp.where(small_row + source * n == small_lane + cell * n, 0.0, total)
        return jnp.concatenate([total] * width, axis=0)

    def matches(picked, listed, inner):
        goal = dot(picked, listed)
        hit = jnp.where((goal > 0) & (inner > 0), 1.0, 0.0)
        needed = jnp.where(dot(hit.astype(jnp.bfloat16), ones) > 0, 1.0, 0.0)
        rank = dot(before, needed.astype(jnp.bfloat16))
        return goal, hit, needed, rank

    lane_slot = lax.rem(entry_row, padded) * width + lax.div(entry_row, padded)
    slot_value = lane_slot.astype(jnp.float32)
    mine = chosen(me)

    def send_step(cell, carry):
        _, _, needed, rank = matches(mine, listing(cell), inner_listing(me, cell))
        picks = jnp.where((rank == entry_lane) & (needed > 0), slot_value, 0.0)
        send_list[pl.ds(cell, 1)] = jnp.sum(picks, axis=0, keepdims=True).astype(jnp.int32)
        return carry

    lax.fori_loop(0, cells, send_step, 0)
    send_copy = pltpu.make_async_copy(send_list, send_smem, local_sem.at[4])
    send_copy.start()
    send_copy.wait()
    left_copy.wait()

    def pack_step(m, carry):
        for offset in range(cells):
            cell = other_cell(offset)
            slot = jnp.clip(send_smem[cell, m], 0, n * width - 1)
            row, at = lax.div(slot, width), lax.rem(slot, width)
            if offset:
                pack[offset, m] = left[row, at, pl.ds(pl.multiple_of(l * quarter, quarter), quarter)]
            else:
                extra[me * per_pair + m] = left[row, at]
        return carry

    lax.fori_loop(0, per_pair, pack_step, 0)

    def extra_copy(offset, source):
        return remote(
            pack.at[offset], part(1, source, l), main_send.at[1, 0, offset],
            main_recv.at[1, source], cell_id(other_cell(offset)),
        )

    for offset in range(1, cells):
        launch(extra_copy(offset, me))

    def share(kind, cell, condition=True):
        launch(side_copy(kind, cell, 0), condition)
        launch(side_copy(kind, cell, 1), condition)

    line = []
    for step in range(1, col_count):
        line.append((c - step, c >= step, 0))
        line.append((c + step, c + step < col_count, 1))
    for origin, has, way in line:
        cell = r * col_count + jnp.clip(origin, 0, col_count - 1)
        await_recv(line_copy(cell, way), has)
        more = c < col_count - 1 if way == 0 else c > 0
        launch(line_copy(cell, way), jnp.logical_and(has, more))
        launch(line_copy(cell, 2), has)
        share(0, cell, has)
    beyond = [((1 - r) * col_count + c, True)]
    for origin, has, way in line:
        beyond.append(((1 - r) * col_count + jnp.clip(origin, 0, col_count - 1), has))
    for cell, has in beyond:
        await_recv(line_copy(cell, 2), has)
        share(0, cell, has)

    listed = listing(me)
    lists = -(-per_row // 8) * 8
    list_row = lax.broadcasted_iota(jnp.int32, (lists, 128), 0)

    def row_step(source, carry):
        held, running, most = carry
        inner = inner_listing(source, me)
        goal, hit, needed, rank = matches(chosen(source), listed, inner)
        place = dot(before, hit.astype(jnp.bfloat16)) + running
        value = ((rank + (source * per_pair).astype(jnp.float32)) * 16.0 + (inner - 1.0)) * 16.0 + goal
        value = value * hit
        for q in range(per_row):
            line_sum = jnp.sum(jnp.where(place == float(q), value, 0.0), axis=0, keepdims=True)
            held = held + jnp.where(list_row == q, line_sum, 0.0)
        running = running + jnp.sum(hit, axis=0, keepdims=True)
        most = jnp.maximum(most, jnp.max(rank + needed, axis=0, keepdims=True))
        return held, running, most

    zero = jnp.zeros((1, 128), jnp.float32)
    held, running, most = lax.fori_loop(
        0, cells, row_step, (jnp.zeros((lists, 128), jnp.float32), zero, zero)
    )
    row_list[...] = held.astype(jnp.int32)
    over = jnp.where((most > per_pair) | (running > per_row), 1, 0)
    flag_all[me] = jnp.broadcast_to(jnp.max(over), (8, 128))
    row_copy = pltpu.make_async_copy(row_list, row_smem, local_sem.at[5])
    row_copy.start()
    flag_copies = []
    for offset in range(1, cells):
        copy = remote(
            flag_all.at[me], flag_all.at[me], flag_send.at[offset], flag_recv.at[offset],
            cell_id(other_cell(offset)),
        )
        copy.start()
        flag_copies.append(copy)

    every = [other_cell(offset) for offset in range(1, cells)]

    def pass_on(kind, cell, condition=True):
        await_recv(side_copy(kind, cell, 1), condition)
        launch(side_copy(kind, cell, 2), condition)

    def settle(kind, cell):
        await_recv(side_copy(kind, cell, 0))
        await_recv(side_copy(kind, cell, 2))

    for cell in every:
        await_recv(extra_copy(1, cell))
        share(1, cell)
    for origin, has, way in line:
        pass_on(0, r * col_count + jnp.clip(origin, 0, col_count - 1), has)
    for cell, has in beyond:
        pass_on(0, cell, has)
    for cell in every:
        pass_on(1, cell)
    for cell in every:
        settle(0, cell)
        settle(1, cell)
    row_copy.wait()
    table_copy.wait()

    def one_row(i, carry):
        part_rows = pl.ds(pl.multiple_of(l * quarter, quarter), quarter)
        own = left[i, own_slot, part_rows]
        pieces = []
        for t in range(width):
            column = meta_smem[i, t]
            lower = diag[jnp.maximum(column, 0)]
            own_left = left[i, t, part_rows]
            own_left = jnp.where(own_slot == t, jnp.zeros_like(own_left), own_left)
            value = dot(
                jnp.concatenate([own, own_left], axis=1),
                jnp.concatenate([left[i, t], lower], axis=0),
            )
            pieces.append(jnp.where(column >= 0, value, 0.0))
        lefts = []
        rights = []
        for q in range(per_row):
            code = jnp.clip(row_smem[q, i], 0, cells * per_pair * 256 - 1)
            goal = lax.rem(code, 16)
            at = jnp.minimum(lax.rem(lax.div(code, 16), 16), width - 1)
            piece = left[i, at, part_rows]
            lefts.append(jnp.concatenate(
                [jnp.where(goal == t + 1, piece, jnp.zeros_like(piece)) for t in range(width)], axis=0
            ))
            rights.append(extra[lax.div(code, 256)])
        total = jnp.concatenate(pieces, axis=0) + dot(
            jnp.concatenate(lefts, axis=1), jnp.concatenate(rights, axis=0)
        )
        stage[i] = total.astype(stage.dtype).reshape(width, quarter, tile)
        return carry

    lax.fori_loop(0, n, one_row, 0)
    out_copy = pltpu.make_async_copy(stage, out_ref, local_sem.at[6])
    out_copy.start()
    for copy in flag_copies:
        copy.wait_recv()
    flag_ref[...] = jnp.max(flag_all[...], axis=0)
    for copy in meta_copies + flag_copies:
        copy.wait_send()
    for copy, condition in sent:
        if condition is True:
            copy.wait_send()
        else:
            @pl.when(condition)
            def _():
                copy.wait_send()
    out_copy.wait()


def on_device_sparse(density_tiles, tile_columns):
    row_count = lax.axis_size("row")
    col_count = lax.axis_size("col")
    layer_count = lax.axis_size("layer")
    n, group_count, slots, tile, _ = density_tiles.shape
    cells = row_count * col_count
    quarter = tile // layer_count
    width = group_count * slots
    per_pair, per_row = 16, 8
    padded = -(-n // 32) * 32
    dtype = density_tiles.dtype
    columns = tile_columns.reshape(n, width)
    meta = jnp.concatenate([
        jnp.pad(columns, ((0, padded - n), (0, 128 - width)), constant_values=-1),
        jnp.pad(columns.T, ((0, 0), (0, 128 - n)), constant_values=-1),
    ], axis=0)
    sizes = (row_count, col_count, layer_count, group_count, per_pair, per_row, padded)
    lists = -(-per_row // 8) * 8
    out, flag = pl.pallas_call(
        functools.partial(sparse_kernel, sizes),
        out_shape=(
            jax.ShapeDtypeStruct((n, width, quarter, tile), dtype),
            jax.ShapeDtypeStruct((8, 128), jnp.int32),
        ),
        in_specs=[
            pl.BlockSpec(memory_space=pl.ANY),
            pl.BlockSpec(memory_space=pltpu.VMEM),
        ],
        out_specs=(
            pl.BlockSpec(memory_space=pl.ANY),
            pl.BlockSpec(memory_space=pltpu.VMEM),
        ),
        scratch_shapes=[
            pltpu.VMEM((n, width, tile, tile), dtype),
            pltpu.VMEM((cells * n, tile, tile), dtype),
            pltpu.VMEM((cells * per_pair, tile, tile), dtype),
            pltpu.VMEM((cells, per_pair, quarter, tile), dtype),
            pltpu.VMEM((n, width, quarter, tile), dtype),
            pltpu.VMEM((cells, padded + width, 128), jnp.int32),
            pltpu.SMEM((padded + width, 128), jnp.int32),
            pltpu.VMEM((cells, 128), jnp.int32),
            pltpu.SMEM((cells, 128), jnp.int32),
            pltpu.VMEM((lists, 128), jnp.int32),
            pltpu.SMEM((lists, 128), jnp.int32),
            pltpu.VMEM((cells, 8, 128), jnp.int32),
            pltpu.SemaphoreType.DMA((7,)),
            pltpu.SemaphoreType.DMA((cells,)),
            pltpu.SemaphoreType.DMA((cells,)),
            pltpu.SemaphoreType.DMA((cells,)),
            pltpu.SemaphoreType.DMA((cells,)),
            pltpu.SemaphoreType.DMA((2, 3, cells)),
            pltpu.SemaphoreType.DMA((2, cells)),
            pltpu.SemaphoreType.DMA((2, 3, cells)),
            pltpu.SemaphoreType.DMA((2, 3, cells)),
        ],
        compiler_params=pltpu.CompilerParams(
            collective_id=2, has_side_effects=True, vmem_limit_bytes=60 * 1024 * 1024
        ),
    )(density_tiles.reshape(n, width, tile, tile), meta)
    out = out.reshape(n, group_count, slots, quarter, tile)
    return lax.cond(
        flag[0, 0] > 0,
        lambda: on_device_paired(density_tiles, tile_columns),
        lambda: out,
    )


def solution(mesh):
    paired = mesh.shape["row"] == 2 and mesh.shape["layer"] % 2 == 0
    four = paired and mesh.shape["layer"] == 4

    def on_each(density_tiles, tile_columns):
        n, group_count, slots, tile, _ = density_tiles.shape
        block_count = n * mesh.shape["row"] * mesh.shape["col"]
        fits = four and n % 8 == 0 and n <= 128 and group_count * slots <= 15 and slots > 0
        fits = fits and (block_count // group_count) % n == 0 and tile % 128 == 0
        fits = fits and mesh.shape["col"] <= 16
        if fits:
            return on_device_sparse(density_tiles, tile_columns)
        return (on_device_paired if paired else on_device)(density_tiles, tile_columns)

    in_specs = (P(("row", "col"), None, None, None, None), P(("row", "col"), None, None))
    out_specs = P(("row", "col"), None, None, "layer", None)
    return jax.shard_map(
        on_each, mesh=mesh, in_specs=in_specs, out_specs=out_specs, check_vma=False
    )
```

```python
import functools

import jax
import jax.numpy as jnp
from jax import lax
from jax.experimental import pallas as pl
from jax.experimental.pallas import tpu as pltpu
from jax.sharding import PartitionSpec as P

MESH = pl.DeviceIdType.MESH


def divisor(total, most):
    return max(d for d in range(1, most + 1) if total % d == 0)


def kernel(
    sizes, columns_ref, tiles_ref, meta_ref, out_ref,
    left, right, meta_all, meta_smem, stage,
    local_sem, meta_send, meta_recv, send_sem, recv_sem, out_send, out_recv,
):
    row_count, col_count, layer_count, chunks, out_chunks, is_balanced = sizes
    n, group_count, slots, tile, _ = tiles_ref.shape
    cells = row_count * col_count
    per_layer = group_count // layer_count
    quarter = tile // layer_count
    width = group_count * slots
    r, c, l = lax.axis_index("row"), lax.axis_index("col"), lax.axis_index("layer")
    me = r * col_count + c
    own_groups = pl.ds(l * per_layer, per_layer)

    own_copy = pltpu.make_async_copy(
        tiles_ref.at[:, own_groups], right.at[pl.ds(me * n, n)], local_sem.at[0]
    )
    left_copy = pltpu.make_async_copy(tiles_ref, left, local_sem.at[1])
    meta_copy = pltpu.make_async_copy(meta_ref, meta_all.at[pl.ds(me * n, n)], local_sem.at[2])
    own_copy.start()
    meta_copy.start()
    left_copy.start()
    right[cells * n] = jnp.zeros(right.shape[1:], right.dtype)

    def cell_id(offset):
        target = lax.rem(me + offset, cells)
        return {"row": lax.div(target, col_count), "col": lax.rem(target, col_count)}

    def layer_id(offset):
        return {"layer": lax.rem(l + offset, layer_count)}

    barrier = pltpu.get_barrier_semaphore()
    for offset in range(1, cells):
        pl.semaphore_signal(barrier, inc=1, device_id=cell_id(offset), device_id_type=MESH)
    for offset in range(1, layer_count):
        pl.semaphore_signal(barrier, inc=1, device_id=layer_id(offset), device_id_type=MESH)
    pl.semaphore_wait(barrier, cells - 1 + layer_count - 1)
    own_copy.wait()

    step_rows = n // chunks
    sent = []

    def rows_of(cell, chunk):
        return pl.ds(cell * n + chunk * step_rows, step_rows)

    def copy_of(cell, chunk, way, device):
        return pltpu.make_async_remote_copy(
            src_ref=right.at[rows_of(cell, chunk)],
            dst_ref=right.at[rows_of(cell, chunk)],
            send_sem=send_sem.at[way, cell, chunk],
            recv_sem=recv_sem.at[cell, chunk],
            device_id=device,
            device_id_type=MESH,
        )

    ways = {
        "up": (0, c < col_count - 1, {"col": jnp.minimum(c + 1, col_count - 1)}),
        "down": (1, c > 0, {"col": jnp.maximum(c - 1, 0)}),
        "south": (2, r < row_count - 1, {"row": jnp.minimum(r + 1, row_count - 1)}),
        "north": (3, r > 0, {"row": jnp.maximum(r - 1, 0)}),
    }

    def send(cell, chunk, way, condition=True):
        index, exists, device = ways[way]
        wanted = jnp.logical_and(exists, condition)

        @pl.when(wanted)
        def _():
            copy_of(cell, chunk, index, device).start()

        sent.append((wanted, cell, chunk, index, device))

    def await_arrival(cell, chunk):
        copy_of(cell, chunk, 0, {"col": c}).wait_recv()

    for chunk in range(chunks):
        for way in ("up", "down", "south", "north"):
            send(me, chunk, way)

    meta_copy.wait()
    meta_copies = []
    for offset in range(1, cells):
        copy = pltpu.make_async_remote_copy(
            src_ref=meta_ref,
            dst_ref=meta_all.at[pl.ds(me * n, n)],
            send_sem=meta_send.at[offset],
            recv_sem=meta_recv.at[offset],
            device_id=cell_id(offset),
            device_id_type=MESH,
        )
        copy.start()
        meta_copies.append(copy)

    even = lax.rem(c, 2) == 0
    for step in range(1, col_count):
        for chunk in range(chunks):
            for origin, has, way, is_pair in (
                (c - step, c >= step, "up", jnp.logical_not(even)),
                (c + step, c + step < col_count, "down", even),
            ):
                origin = jnp.clip(origin, 0, col_count - 1)
                cell = r * col_count + origin

                @pl.when(has)
                def _():
                    await_arrival(cell, chunk)

                send(cell, chunk, way, has)
                across = has
                if is_balanced and step == 1 and chunk >= chunks // 2:
                    across = jnp.logical_and(has, jnp.logical_not(is_pair))
                send(cell, chunk, "south", across)
                send(cell, chunk, "north", across)

    if is_balanced:
        other = (1 - r) * col_count + c
        for chunk in range(chunks):
            await_arrival(other, chunk)
            if chunk >= chunks // 2:
                send(other, chunk, "up", even)
                send(other, chunk, "down", jnp.logical_not(even))
        for step in range(1, col_count):
            origin = (1 - r) * col_count + lax.rem(c + step, col_count)
            for chunk in range(chunks):
                await_arrival(origin, chunk)
    else:
        for step in range(1, row_count):
            for shift in range(col_count):
                for chunk in range(chunks):
                    for origin, has, way in (
                        (r - step, r >= step, "south"),
                        (r + step, r + step < row_count, "north"),
                    ):
                        origin = jnp.clip(origin, 0, row_count - 1)
                        cell = origin * col_count + lax.rem(c + shift, col_count)

                        @pl.when(has)
                        def _():
                            await_arrival(cell, chunk)

                        send(cell, chunk, way, has)

    for copy in meta_copies:
        copy.wait()
    table_copy = pltpu.make_async_copy(meta_all, meta_smem, local_sem.at[3])
    table_copy.start()
    table_copy.wait()
    left_copy.wait()

    def one_row(i, carry):
        targets = [
            columns_ref[i * width + l * per_layer * slots + s] for s in range(per_layer * slots)
        ]
        strips = []
        for a in range(width):
            k = columns_ref[i * width + a]
            inner = jnp.maximum(k, 0)
            pieces = []
            for s in range(per_layer * slots):
                group = s // slots
                row_index = jnp.int32(cells * n)
                slot_index = jnp.int32(0)
                is_live = (k >= 0) & (targets[s] >= 0)
                for t in range(slots):
                    hit = (meta_smem[inner, 0, group * slots + t] == targets[s]) & is_live
                    row_index = jnp.where(hit, inner, row_index)
                    slot_index = jnp.where(hit, t, slot_index)
                pieces.append(right[row_index, group, slot_index])
            strips.append(jnp.concatenate(pieces, axis=1))
        rights = jnp.concatenate(strips, axis=0)
        lefts = jnp.concatenate(
            [left[i, a // slots, a % slots] for a in range(width)], axis=1
        )
        total = jnp.dot(lefts, rights, preferred_element_type=jnp.float32).astype(stage.dtype)
        for q in range(layer_count):
            for s in range(per_layer * slots):
                stage[q, i, s // slots, s % slots] = total[
                    q * quarter:(q + 1) * quarter, s * tile:(s + 1) * tile
                ]
        return carry

    out_rows = n // out_chunks

    def out_copies(chunk):
        rows = pl.ds(chunk * out_rows, out_rows)
        copies = []
        for offset in range(layer_count):
            q = lax.rem(l + offset, layer_count)
            if offset == 0:
                copies.append(pltpu.make_async_copy(
                    stage.at[q, rows], out_ref.at[rows, own_groups], out_send.at[0, chunk]
                ))
            else:
                copies.append(pltpu.make_async_remote_copy(
                    src_ref=stage.at[q, rows],
                    dst_ref=out_ref.at[rows, own_groups],
                    send_sem=out_send.at[offset, chunk],
                    recv_sem=out_recv.at[offset, chunk],
                    device_id=layer_id(offset),
                    device_id_type=MESH,
                ))
        return copies

    all_out = []
    for chunk in range(out_chunks + 1):
        if chunk < out_chunks:
            lax.fori_loop(chunk * out_rows, (chunk + 1) * out_rows, one_row, 0)
        if chunk > 0:
            copies = out_copies(chunk - 1)
            for copy in copies[1:] + copies[:1]:
                copy.start()
            all_out.extend(copies)

    for wanted, cell, chunk, index, device in sent:
        @pl.when(wanted)
        def _():
            copy_of(cell, chunk, index, device).wait_send()

    for copy in all_out:
        copy.wait()


def on_device(density_tiles, tile_columns):
    row_count = lax.axis_size("row")
    col_count = lax.axis_size("col")
    layer_count = lax.axis_size("layer")
    n, group_count, slots, tile, _ = density_tiles.shape
    cells = row_count * col_count
    per_layer = group_count // layer_count
    quarter = tile // layer_count
    kept = per_layer * slots
    chunks = divisor(n, 4)
    out_chunks = divisor(n, 4)
    is_balanced = row_count == 2 and col_count % 2 == 0 and chunks % 2 == 0
    own = lax.dynamic_slice_in_dim(tile_columns, lax.axis_index("layer") * per_layer, per_layer, 1)
    meta = jnp.pad(own.reshape(n, 1, kept), ((0, 0), (0, 0), (0, 128 - kept)), constant_values=-1)
    dtype = density_tiles.dtype
    sizes = (row_count, col_count, layer_count, chunks, out_chunks, is_balanced)
    return pl.pallas_call(
        functools.partial(kernel, sizes),
        out_shape=jax.ShapeDtypeStruct((n, group_count, slots, quarter, tile), dtype),
        in_specs=[
            pl.BlockSpec(memory_space=pltpu.SMEM),
            pl.BlockSpec(memory_space=pl.ANY),
            pl.BlockSpec(memory_space=pltpu.VMEM),
        ],
        out_specs=pl.BlockSpec(memory_space=pl.ANY),
        scratch_shapes=[
            pltpu.VMEM(density_tiles.shape, dtype),
            pltpu.VMEM((cells * n + 1, per_layer, slots, tile, tile), dtype),
            pltpu.VMEM((cells * n, 1, 128), jnp.int32),
            pltpu.SMEM((cells * n, 1, 128), jnp.int32),
            pltpu.VMEM((layer_count, n, per_layer, slots, quarter, tile), dtype),
            pltpu.SemaphoreType.DMA((4,)),
            pltpu.SemaphoreType.DMA((cells,)),
            pltpu.SemaphoreType.DMA((cells,)),
            pltpu.SemaphoreType.DMA((4, cells, chunks)),
            pltpu.SemaphoreType.DMA((cells, chunks)),
            pltpu.SemaphoreType.DMA((layer_count, out_chunks)),
            pltpu.SemaphoreType.DMA((layer_count, out_chunks)),
        ],
        compiler_params=pltpu.CompilerParams(
            collective_id=0, has_side_effects=True, vmem_limit_bytes=60 * 1024 * 1024
        ),
    )(tile_columns.reshape(-1), density_tiles, meta)


def paired_kernel(
    sizes, tiles_ref, meta_ref, out_ref,
    left, right, meta_all, meta_smem, stage,
    local_sem, meta_send, meta_recv, send_sem, recv_sem, left_send, left_recv, out_send, out_recv,
):
    col_count, layer_count, chunks, out_chunks = sizes
    n, group_count, slots, tile, _ = tiles_ref.shape
    cells = 2 * col_count
    per_layer = group_count // layer_count
    quarter = tile // layer_count
    width = group_count * slots
    r, c, l = lax.axis_index("row"), lax.axis_index("col"), lax.axis_index("layer")
    high, k = lax.div(l, 2), lax.rem(l, 2)
    me = r * col_count + c
    base = k * col_count + c
    is_home = k == r
    is_guest = jnp.logical_not(is_home)
    group = 2 * high + r
    own_groups = pl.ds(group * per_layer, per_layer)
    other_groups = pl.ds((2 * high + 1 - r) * per_layer, per_layer)
    facing = {"row": 1 - r}
    partner = {"layer": 2 * high + 1 - k}

    own_copy = pltpu.make_async_copy(
        tiles_ref.at[:, own_groups], right.at[pl.ds(me * n, n)], local_sem.at[0]
    )
    left_copy = pltpu.make_async_copy(tiles_ref, left, local_sem.at[1])
    meta_copy = pltpu.make_async_copy(meta_ref, meta_all.at[pl.ds(me * n, n)], local_sem.at[2])
    own_copy.start()
    meta_copy.start()

    @pl.when(is_home)
    def _():
        left_copy.start()

    right[cells * n] = jnp.zeros(right.shape[1:], right.dtype)

    def cell_id(offset):
        target = lax.rem(me + offset, cells)
        return {"row": lax.div(target, col_count), "col": lax.rem(target, col_count)}

    barrier = pltpu.get_barrier_semaphore()
    for offset in range(1, cells):
        pl.semaphore_signal(barrier, inc=1, device_id=cell_id(offset), device_id_type=MESH)
    for offset in range(1, layer_count):
        for row in (r, 1 - r):
            pl.semaphore_signal(
                barrier,
                inc=1,
                device_id={"row": row, "layer": lax.rem(l + offset, layer_count)},
                device_id_type=MESH,
            )
    pl.semaphore_wait(barrier, cells - 1 + 2 * (layer_count - 1))

    step_rows = n // chunks
    sent = []

    def rows_of(cell, chunk):
        return pl.ds(cell * n + chunk * step_rows, step_rows)

    def copy_of(cell, chunk, way, device):
        source = right.at[rows_of(cell, chunk)]
        if way == 3:
            source = tiles_ref.at[pl.ds(chunk * step_rows, step_rows), other_groups]
        return pltpu.make_async_remote_copy(
            src_ref=source,
            dst_ref=right.at[rows_of(cell, chunk)],
            send_sem=send_sem.at[way, cell, chunk],
            recv_sem=recv_sem.at[cell, chunk],
            device_id=device,
            device_id_type=MESH,
        )

    ways = {
        "up": (0, c < col_count - 1, {"col": jnp.minimum(c + 1, col_count - 1)}),
        "down": (1, c > 0, {"col": jnp.maximum(c - 1, 0)}),
        "partner": (2, True, partner),
        "facing": (3, True, facing),
    }

    def send(cell, chunk, way, condition):
        index, exists, device = ways[way]
        wanted = jnp.logical_and(exists, condition)

        @pl.when(wanted)
        def _():
            copy_of(cell, chunk, index, device).start()

        sent.append((wanted, cell, chunk, index, device))

    def await_arrival(cell, chunk, condition):
        @pl.when(condition)
        def _():
            copy_of(cell, chunk, 2, partner).wait_recv()

    for chunk in range(chunks):
        send(me, chunk, "facing", is_home)
    own_copy.wait()
    for chunk in range(chunks):
        for way in ("up", "down"):
            send(me, chunk, way, is_home)
    left_out = pltpu.make_async_remote_copy(
        src_ref=tiles_ref, dst_ref=left, send_sem=left_send, recv_sem=left_recv,
        device_id=facing, device_id_type=MESH,
    )

    meta_copy.wait()
    meta_copies = []
    for offset in range(1, cells):
        copy = pltpu.make_async_remote_copy(
            src_ref=meta_ref,
            dst_ref=meta_all.at[pl.ds(me * n, n)],
            send_sem=meta_send.at[offset],
            recv_sem=meta_recv.at[offset],
            device_id=cell_id(offset),
            device_id_type=MESH,
        )
        copy.start()
        meta_copies.append(copy)

    @pl.when(is_home)
    def _():
        left_out.start()

    for chunk in range(chunks):
        await_arrival(base, chunk, is_guest)
        for way in ("up", "down", "partner"):
            send(base, chunk, way, is_guest)

    for step in range(1, col_count):
        for chunk in range(chunks):
            for origin, has, way in (
                (c - step, c >= step, "up"),
                (c + step, c + step < col_count, "down"),
            ):
                cell = k * col_count + jnp.clip(origin, 0, col_count - 1)
                await_arrival(cell, chunk, has)
                send(cell, chunk, way, has)
                send(cell, chunk, "partner", has)

    for chunk in range(chunks):
        await_arrival((1 - k) * col_count + c, chunk, is_home)
    for step in range(1, col_count):
        cell = (1 - k) * col_count + lax.rem(c + step, col_count)
        for chunk in range(chunks):
            await_arrival(cell, chunk, True)

    for copy in meta_copies:
        copy.wait()
    table_copy = pltpu.make_async_copy(meta_all, meta_smem, local_sem.at[3])
    table_copy.start()
    table_copy.wait()

    @pl.when(is_home)
    def _():
        left_copy.wait()

    @pl.when(is_guest)
    def _():
        left_out.wait_recv()

    first = group * per_layer * slots

    def one_row(i, carry):
        block_row = base * n + i
        targets = [meta_smem[block_row, 0, first + s] for s in range(per_layer * slots)]
        strips = []
        for a in range(width):
            column = meta_smem[block_row, 0, a]
            inner = jnp.maximum(column, 0)
            pieces = []
            for s in range(per_layer * slots):
                part = s // slots
                row_index = jnp.int32(cells * n)
                slot_index = jnp.int32(0)
                is_live = (column >= 0) & (targets[s] >= 0)
                for t in range(slots):
                    hit = (meta_smem[inner, 0, first + part * slots + t] == targets[s]) & is_live
                    row_index = jnp.where(hit, inner, row_index)
                    slot_index = jnp.where(hit, t, slot_index)
                pieces.append(right[row_index, part, slot_index])
            strips.append(jnp.concatenate(pieces, axis=1))
        rights = jnp.concatenate(strips, axis=0)
        lefts = jnp.concatenate(
            [left[i, a // slots, a % slots] for a in range(width)], axis=1
        )
        total = jnp.dot(lefts, rights, preferred_element_type=jnp.float32).astype(stage.dtype)
        for q in range(layer_count):
            for s in range(per_layer * slots):
                stage[q, i, s // slots, s % slots] = total[
                    q * quarter:(q + 1) * quarter, s * tile:(s + 1) * tile
                ]
        return carry

    out_rows = n // out_chunks

    def out_copy(chunk, q, source):
        rows = pl.ds(chunk * out_rows, out_rows)
        return pltpu.make_async_remote_copy(
            src_ref=stage.at[q, rows],
            dst_ref=out_ref.at[rows, pl.ds(source * per_layer, per_layer)],
            send_sem=out_send.at[q, chunk],
            recv_sem=out_recv.at[source, chunk],
            device_id={"row": k, "layer": q},
            device_id_type=MESH,
        )

    def kept_copy(chunk):
        rows = pl.ds(chunk * out_rows, out_rows)
        return pltpu.make_async_copy(
            stage.at[l, rows], out_ref.at[rows, own_groups], out_send.at[l, chunk]
        )

    for chunk in range(out_chunks + 1):
        if chunk < out_chunks:
            lax.fori_loop(chunk * out_rows, (chunk + 1) * out_rows, one_row, 0)
        if chunk > 0:
            for offset in range(layer_count - 1, -1, -1):
                q = lax.rem(l + offset, layer_count)
                if offset:
                    out_copy(chunk - 1, q, group).start()
                else:
                    @pl.when(is_guest)
                    def _():
                        out_copy(chunk - 1, q, group).start()

                    @pl.when(is_home)
                    def _():
                        kept_copy(chunk - 1).start()

    for wanted, cell, chunk, index, device in sent:
        @pl.when(wanted)
        def _():
            copy_of(cell, chunk, index, device).wait_send()

    @pl.when(is_home)
    def _():
        left_out.wait_send()

    for chunk in range(out_chunks):
        for offset in range(layer_count):
            q = lax.rem(l + offset, layer_count)
            source = lax.rem(group + offset, layer_count)
            if offset:
                out_copy(chunk, q, source).wait()
            else:
                @pl.when(is_guest)
                def _():
                    out_copy(chunk, q, source).wait()

                @pl.when(is_home)
                def _():
                    kept_copy(chunk).wait()


def on_device_paired(density_tiles, tile_columns):
    col_count = lax.axis_size("col")
    layer_count = lax.axis_size("layer")
    n, group_count, slots, tile, _ = density_tiles.shape
    cells = 2 * col_count
    per_layer = group_count // layer_count
    quarter = tile // layer_count
    width = group_count * slots
    chunks = divisor(n, 2)
    out_chunks = divisor(n, 12)
    lanes = -(-width // 128) * 128
    meta = jnp.pad(
        tile_columns.reshape(n, 1, width), ((0, 0), (0, 0), (0, lanes - width)), constant_values=-1
    )
    dtype = density_tiles.dtype
    return pl.pallas_call(
        functools.partial(paired_kernel, (col_count, layer_count, chunks, out_chunks)),
        out_shape=jax.ShapeDtypeStruct((n, group_count, slots, quarter, tile), dtype),
        in_specs=[
            pl.BlockSpec(memory_space=pl.ANY),
            pl.BlockSpec(memory_space=pltpu.VMEM),
        ],
        out_specs=pl.BlockSpec(memory_space=pl.ANY),
        scratch_shapes=[
            pltpu.VMEM(density_tiles.shape, dtype),
            pltpu.VMEM((cells * n + 1, per_layer, slots, tile, tile), dtype),
            pltpu.VMEM((cells * n, 1, lanes), jnp.int32),
            pltpu.SMEM((cells * n, 1, lanes), jnp.int32),
            pltpu.VMEM((layer_count, n, per_layer, slots, quarter, tile), dtype),
            pltpu.SemaphoreType.DMA((4,)),
            pltpu.SemaphoreType.DMA((cells,)),
            pltpu.SemaphoreType.DMA((cells,)),
            pltpu.SemaphoreType.DMA((4, cells, chunks)),
            pltpu.SemaphoreType.DMA((cells, chunks)),
            pltpu.SemaphoreType.DMA,
            pltpu.SemaphoreType.DMA,
            pltpu.SemaphoreType.DMA((layer_count, out_chunks)),
            pltpu.SemaphoreType.DMA((layer_count, out_chunks)),
        ],
        compiler_params=pltpu.CompilerParams(
            collective_id=1, has_side_effects=True, vmem_limit_bytes=60 * 1024 * 1024
        ),
    )(density_tiles, meta)


def sparse_kernel(
    sizes, tiles_ref, columns_ref, out_ref, flag_ref,
    left, diag, extra, lent, borrowed, pack, arrived, stage, total, needs, ranks, meta_own, meta_all, meta_smem,
    send_list, send_smem, row_list, row_smem, flag_all,
    local_sem, meta_send, meta_recv, flag_send, flag_recv,
    main_send, main_recv, side_send, side_recv, lent_sem, pack_send, pack_recv, extra_send, extra_recv,
):
    row_count, col_count, layer_count, group_count, per_row, padded = sizes
    n, width, tile, _ = tiles_ref.shape
    per_lent, per_plane, pool = lent.shape[0], pack.shape[1], extra.shape[0]
    cells = row_count * col_count
    quarter = tile // layer_count
    entries = padded * width
    span = -(-(cells * n) // 128) * 128
    lists = -(-per_row // 8) * 8
    r, c, l = lax.axis_index("row"), lax.axis_index("col"), lax.axis_index("layer")
    x, k = lax.div(l, 2), lax.rem(l, 2)
    facing_layer = 2 * (1 - x) + k
    me = r * col_count + c
    opposite = (1 - r) * col_count + c
    own_slot = lax.div(me * n * group_count, cells * n) * (width // group_count)
    partner = {"layer": 2 * x + 1 - k}
    facing = {"layer": facing_layer}

    diag_copy = pltpu.make_async_copy(
        tiles_ref.at[:, own_slot], diag.at[pl.ds(me * n, n)], local_sem.at[1]
    )
    left_copy = pltpu.make_async_copy(tiles_ref, left, local_sem.at[2])
    table_copy = pltpu.make_async_copy(meta_own, meta_smem, local_sem.at[3])
    diag_copy.start()
    left_copy.start()
    meta_own[...] = jnp.full(meta_own.shape, -1, jnp.int32)
    meta_own[:, 0:n] = columns_ref[...]
    meta_all[me] = meta_own[...]

    def cell_id(cell):
        return {"row": lax.div(cell, col_count), "col": lax.rem(cell, col_count)}

    def other_cell(offset):
        return lax.rem(me + offset, cells)

    barrier = pltpu.get_barrier_semaphore()
    for offset in range(1, cells):
        pl.semaphore_signal(
            barrier, inc=1, device_id=cell_id(other_cell(offset)), device_id_type=MESH
        )
    for device in (partner, facing):
        pl.semaphore_signal(barrier, inc=1, device_id=device, device_id_type=MESH)
    pl.semaphore_wait(barrier, cells - 1 + 2)

    sent = []

    def remote(source, target, send, recv, device):
        return pltpu.make_async_remote_copy(
            src_ref=source, dst_ref=target, send_sem=send, recv_sem=recv,
            device_id=device, device_id_type=MESH,
        )

    def launch(copy, condition=True):
        if condition is True:
            copy.start()
        else:
            @pl.when(condition)
            def _():
                copy.start()
        sent.append((copy, condition))

    def await_recv(copy, condition=True):
        if condition is True:
            copy.wait_recv()
        else:
            @pl.when(condition)
            def _():
                copy.wait_recv()

    def part(cell, q):
        return diag.at[pl.ds(cell * n, n), pl.ds(q * quarter, quarter)]

    up = {"col": jnp.minimum(c + 1, col_count - 1)}
    down = {"col": jnp.maximum(c - 1, 0)}
    across = {"row": 1 - r}

    def line_copy(cell, way, wide=0):
        device = (up, down, across)[way]
        piece = part(cell, facing_layer if wide else l)
        return remote(
            piece, piece, main_send.at[wide, way, cell], main_recv.at[wide, cell], device
        )

    def side_copy(cell, way):
        device = (partner, facing, partner)[way]
        piece = part(cell, facing_layer if way == 2 else l)
        return remote(piece, piece, side_send.at[way, cell], side_recv.at[way, cell], device)

    meta_copies = []
    for offset in range(1, cells):
        copy = remote(
            meta_own, meta_all.at[me], meta_send.at[offset], meta_recv.at[offset],
            cell_id(other_cell(offset)),
        )
        copy.start()
        meta_copies.append(copy)
    diag_copy.wait()
    has_up, has_down = c < col_count - 1, c > 0
    launch(line_copy(me, 0), has_up)
    launch(line_copy(me, 1), has_down)
    launch(line_copy(me, 2))
    launch(line_copy(me, 2, 1))
    table_copy.start()
    for copy in meta_copies:
        copy.wait_recv()

    small_row = lax.broadcasted_iota(jnp.int32, (padded, 128), 0)
    small_lane = lax.broadcasted_iota(jnp.int32, (padded, 128), 1)
    wide_row = lax.broadcasted_iota(jnp.int32, (padded, span), 0)
    wide_lane = lax.broadcasted_iota(jnp.int32, (padded, span), 1)
    tall_row = lax.broadcasted_iota(jnp.int32, (span, 128), 0)
    entry_row = lax.broadcasted_iota(jnp.int32, (entries, 128), 0)
    entry_lane = lax.broadcasted_iota(jnp.int32, (entries, 128), 1).astype(jnp.float32)
    before = (
        lax.broadcasted_iota(jnp.int32, (entries, entries), 0)
        > lax.broadcasted_iota(jnp.int32, (entries, entries), 1)
    ).astype(jnp.float32).astype(jnp.bfloat16)
    ones = jnp.ones((128, 128), jnp.bfloat16)

    def dot(a, b):
        return jnp.dot(a, b, preferred_element_type=jnp.float32)

    def chosen(cell):
        columns = jnp.transpose(meta_all[cell])[0:padded]
        pieces = []
        for b in range(width):
            hit = (columns[:, b:b + 1] == wide_lane) & (wide_lane != wide_row + cell * n)
            pieces.append(jnp.where(hit, 1.0, 0.0))
        return jnp.concatenate(pieces, axis=0).astype(jnp.bfloat16)

    def listing(cell):
        rows = meta_all[cell]
        weight = jnp.zeros((span, 128), jnp.float32)
        for a in range(width):
            weight = jnp.where(rows[a:a + 1] == tall_row, a + 1.0, weight)
        return weight.astype(jnp.bfloat16)

    def inner_listing(source, cell):
        rows = meta_all[cell]
        weight = jnp.zeros((padded, 128), jnp.float32)
        for a in range(width):
            weight = jnp.where(rows[a:a + 1] == small_row + source * n, a + 1.0, weight)
        weight = jnp.where(small_row + source * n == small_lane + cell * n, 0.0, weight)
        return jnp.concatenate([weight] * width, axis=0)

    def matches(picked, listed, inner):
        goal = dot(picked, listed)
        hit = jnp.where((goal > 0) & (inner > 0), 1.0, 0.0)
        needed = jnp.where(dot(hit.astype(jnp.bfloat16), ones) > 0, 1.0, 0.0)
        return goal, hit, needed

    def rank_of(needed):
        return dot(before, needed.astype(jnp.bfloat16))

    def count_of(needed):
        return jnp.sum(needed, axis=0, keepdims=True)

    def picks_of(needed, rank, value):
        chosen_values = jnp.where((rank == entry_lane) & (needed > 0), value, 0.0)
        return jnp.sum(chosen_values, axis=0, keepdims=True)

    slot_value = (
        lax.rem(entry_row, padded) * width + lax.div(entry_row, padded)
    ).astype(jnp.float32)
    mine, theirs = chosen(me), chosen(opposite)
    none = jnp.zeros((entries, 128), jnp.float32)
    my_rows = pl.ds(pl.multiple_of(l * quarter, quarter), quarter)

    def lent_step(at, wanted):
        cell = (1 - r) * col_count + at
        return jnp.maximum(wanted, matches(mine, listing(cell), inner_listing(me, cell))[2])

    wanted = lax.fori_loop(0, col_count, lent_step, none, unroll=True)
    send_list[0:1] = picks_of(wanted, rank_of(wanted), slot_value).astype(jnp.int32)
    lent_most = count_of(wanted)
    lent_list = pltpu.make_async_copy(send_list.at[0], send_smem.at[0], local_sem.at[4])
    lent_list.start()
    lent_list.wait()
    left_copy.wait()

    def own_piece(code):
        code = jnp.clip(code, 0, n * width - 1)
        return left[lax.div(code, width), lax.rem(code, width), my_rows]

    def lent_pack(m, carry):
        lent[m] = own_piece(send_smem[0, m])
        return carry

    lax.fori_loop(0, per_lent, lent_pack, 0, unroll=4)
    lent_copy = remote(lent, borrowed, lent_sem.at[0], lent_sem.at[1], across)
    launch(lent_copy)

    def share(cell, condition=True, wide=False):
        launch(side_copy(cell, 0), condition)
        if not wide:
            launch(side_copy(cell, 1), condition)

    def take_line(cell, has, way, wide):
        await_recv(line_copy(cell, way), has)
        launch(line_copy(cell, way), jnp.logical_and(has, has_up if way == 0 else has_down))
        share(cell, has, wide)
        launch(line_copy(cell, 2), has)

    line, beyond = [], []
    for step in range(1, col_count):
        for origin, has, way in ((c - step, c >= step, 0), (c + step, c + step < col_count, 1)):
            origin = jnp.clip(origin, 0, col_count - 1)
            line.append((r * col_count + origin, has, way, step == 1))
            beyond.append(((1 - r) * col_count + origin, has))

    for entry in line[:2]:
        take_line(*entry)

    def plane_step(at, wanted):
        cell = r * col_count + at
        listed = listing(cell)
        own = matches(mine, listed, inner_listing(me, cell))[2]
        send_list[pl.ds(8 + at, 1)] = picks_of(own, rank_of(own), slot_value).astype(jnp.int32)
        their = matches(theirs, listed, inner_listing(opposite, cell))[2]
        needs[at] = their
        ranks[at] = rank_of(their) + count_of(own)
        return jnp.maximum(wanted, their)

    wanted = lax.fori_loop(0, col_count, plane_step, none, unroll=True)
    borrowed_value = rank_of(wanted) + float(n * width)

    def plane_finish(at, carry):
        picks = picks_of(needs[at], ranks[at], borrowed_value).astype(jnp.int32)
        send_list[pl.ds(8 + at, 1)] += picks
        return carry

    lax.fori_loop(0, col_count, plane_finish, 0, unroll=True)
    rows_used = send_list.shape[0] - 8
    plane_list = pltpu.make_async_copy(
        send_list.at[pl.ds(8, rows_used)], send_smem.at[pl.ds(8, rows_used)], local_sem.at[4]
    )
    plane_list.start()

    await_recv(line_copy(opposite, 2))
    share(opposite, True, True)
    await_recv(line_copy(opposite, 2, 1))
    launch(side_copy(opposite, 2))
    plane_list.wait()
    await_recv(lent_copy)

    def plane_piece(at, m):
        code = send_smem[8 + at, m]
        loaned = borrowed[jnp.clip(code - n * width, 0, per_lent - 1)]
        return jnp.where(code < n * width, own_piece(code), loaned)

    def plane_pack(m, carry):
        for offset in range(col_count):
            at = lax.rem(c + offset, col_count)
            if offset:
                pack[offset, m] = plane_piece(at, m)
            else:
                arrived[c, m] = plane_piece(at, m)
        return carry

    lax.fori_loop(0, per_plane, plane_pack, 0, unroll=2)

    def pack_copy(offset, origin):
        return remote(
            pack.at[offset], arrived.at[origin], pack_send.at[offset], pack_recv.at[origin],
            {"col": lax.rem(c + offset, col_count)},
        )

    for offset in range(1, col_count):
        launch(pack_copy(offset, c))
    launch(line_copy(me, 0, 1), has_up)
    launch(line_copy(me, 1, 1), has_down)

    def take_beyond(cell, has):
        await_recv(line_copy(cell, 2), has)
        share(cell, has)

    for entry in line[2:4]:
        take_line(*entry)
    for entry in beyond[:2]:
        take_beyond(*entry)

    listed = listing(me)
    list_row = lax.broadcasted_iota(jnp.int32, (lists + 8, 128), 0)

    def row_step(at, carry):
        held, running, pooled, in_plane, most = carry
        plane, far = lax.div(at, 2), lax.rem(at, 2)
        source = jnp.where(far == 0, r, 1 - r) * col_count + plane
        in_plane = jnp.where(far == 0, 0.0, in_plane)
        inner = inner_listing(source, me)
        goal, hit, needed = matches(chosen(source), listed, inner)
        rank = rank_of(needed)
        place = dot(before, hit.astype(jnp.bfloat16)) + running
        value = (((rank + pooled) * 16.0 + (inner - 1.0)) * 16.0 + goal) * hit
        for q in range(per_row):
            line_sum = jnp.sum(jnp.where(place == float(q), value, 0.0), axis=0, keepdims=True)
            held = held + jnp.where(list_row == q, line_sum, 0.0)
        spot = rank + in_plane + (plane * per_plane).astype(jnp.float32)
        held = held + jnp.where(list_row == lists, picks_of(needed, rank + pooled, spot), 0.0)
        count = count_of(needed)
        in_plane = in_plane + count
        return held, running + count_of(hit), pooled + count, in_plane, jnp.maximum(most, in_plane)

    zero = jnp.zeros((1, 128), jnp.float32)
    held, running, pooled, _, most = lax.fori_loop(
        0, cells, row_step, (jnp.zeros((lists + 8, 128), jnp.float32), zero, zero, zero, zero),
        unroll=2,
    )
    row_list[...] = held.astype(jnp.int32)
    over = (most > per_plane) | (running > per_row) | (pooled > pool) | (lent_most > per_lent)
    flag_all[me] = jnp.broadcast_to(jnp.max(jnp.where(over, 1, 0)), (8, 128))
    row_copy = pltpu.make_async_copy(row_list, row_smem, local_sem.at[5])
    row_copy.start()
    flag_copies = []
    for offset in range(1, cells):
        copy = remote(
            flag_all.at[me], flag_all.at[me], flag_send.at[offset], flag_recv.at[offset],
            cell_id(other_cell(offset)),
        )
        copy.start()
        flag_copies.append(copy)

    def pass_on(cell, condition=True):
        await_recv(side_copy(cell, 1), condition)
        launch(side_copy(cell, 2), condition)

    def take_wide(cell, has, way, wide):
        await_recv(line_copy(cell, way, 1), has)
        launch(side_copy(cell, 2), has)

    for entry in line[4:]:
        take_line(*entry)
    for entry in beyond[2:]:
        take_beyond(*entry)
    for entry in line[:2]:
        take_wide(*entry)
    row_copy.wait()
    for offset in range(1, col_count):
        await_recv(pack_copy(offset, lax.rem(c + offset, col_count)))

    def pool_pack(m, carry):
        code = jnp.clip(row_smem[lists, m], 0, col_count * per_plane - 1)
        extra[m, my_rows] = arrived[lax.div(code, per_plane), lax.rem(code, per_plane)]
        return carry

    lax.fori_loop(0, pool, pool_pack, 0, unroll=4)

    def extra_copy(way):
        device = (partner, facing, partner)[way]
        piece = extra.at[:, pl.ds((facing_layer if way == 2 else l) * quarter, quarter)]
        return remote(piece, piece, extra_send.at[way], extra_recv.at[way], device)

    launch(extra_copy(0))
    launch(extra_copy(1))
    for cell, has, _, _ in line[2:]:
        pass_on(cell, has)
    for cell, has in beyond:
        pass_on(cell, has)
    for offset in range(1, cells):
        await_recv(side_copy(other_cell(offset), 0))
        await_recv(side_copy(other_cell(offset), 2))
    table_copy.wait()

    def near_row(i, carry):
        own = left[i, own_slot, my_rows]
        pieces = []
        for t in range(width):
            column = meta_smem[t, i]
            lower = diag[jnp.maximum(column, 0)]
            own_left = left[i, t, my_rows]
            own_left = jnp.where(own_slot == t, jnp.zeros_like(own_left), own_left)
            value = dot(
                jnp.concatenate([own, own_left], axis=1),
                jnp.concatenate([left[i, t], lower], axis=0),
            )
            pieces.append(jnp.where(column >= 0, value, 0.0))
        total[i] = jnp.concatenate(pieces, axis=0)
        return carry

    lax.fori_loop(0, n, near_row, 0, unroll=2)
    await_recv(extra_copy(1))
    launch(extra_copy(2))
    await_recv(extra_copy(0))
    await_recv(extra_copy(2))

    def far_row(i, carry):
        lefts, rights = [], []
        for q in range(per_row):
            code = jnp.clip(row_smem[q, i], 0, pool * 256 - 1)
            goal = lax.rem(code, 16)
            at = jnp.minimum(lax.rem(lax.div(code, 16), 16), width - 1)
            piece = left[i, at, my_rows]
            lefts.append(jnp.concatenate(
                [jnp.where(goal == t + 1, piece, jnp.zeros_like(piece)) for t in range(width)], axis=0
            ))
            rights.append(extra[lax.div(code, 256)])
        value = total[i] + dot(
            jnp.concatenate(lefts, axis=1), jnp.concatenate(rights, axis=0)
        )
        stage[i] = value.astype(stage.dtype).reshape(width, quarter, tile)
        return carry

    lax.fori_loop(0, n, far_row, 0, unroll=4)
    out_copy = pltpu.make_async_copy(stage, out_ref, local_sem.at[6])
    out_copy.start()
    for copy in flag_copies:
        copy.wait_recv()
    flag_ref[...] = jnp.max(flag_all[...], axis=0)
    for copy in meta_copies + flag_copies:
        copy.wait_send()
    for copy, condition in sent:
        if condition is True:
            copy.wait_send()
        else:
            @pl.when(condition)
            def _():
                copy.wait_send()
    out_copy.wait()


def on_device_sparse(density_tiles, tile_columns):
    row_count = lax.axis_size("row")
    col_count = lax.axis_size("col")
    layer_count = lax.axis_size("layer")
    n, group_count, slots, tile, _ = density_tiles.shape
    cells = row_count * col_count
    quarter = tile // layer_count
    width = group_count * slots
    per_lent, per_plane, pool, per_row = 32, 24, 56, 8
    padded = -(-n // 32) * 32
    dtype = density_tiles.dtype
    sizes = (row_count, col_count, layer_count, group_count, per_row, padded)
    lists = -(-per_row // 8) * 8
    planes = -(-col_count // 8) * 8
    out, flag = pl.pallas_call(
        functools.partial(sparse_kernel, sizes),
        out_shape=(
            jax.ShapeDtypeStruct((n, width, quarter, tile), dtype),
            jax.ShapeDtypeStruct((8, 128), jnp.int32),
        ),
        in_specs=[
            pl.BlockSpec(memory_space=pl.ANY),
            pl.BlockSpec(memory_space=pltpu.VMEM),
        ],
        out_specs=(
            pl.BlockSpec(memory_space=pl.ANY),
            pl.BlockSpec(memory_space=pltpu.VMEM),
        ),
        scratch_shapes=[
            pltpu.VMEM((n, width, tile, tile), dtype),
            pltpu.VMEM((cells * n, tile, tile), dtype),
            pltpu.VMEM((pool, tile, tile), dtype),
            pltpu.VMEM((per_lent, quarter, tile), dtype),
            pltpu.VMEM((per_lent, quarter, tile), dtype),
            pltpu.VMEM((col_count, per_plane, quarter, tile), dtype),
            pltpu.VMEM((col_count, per_plane, quarter, tile), dtype),
            pltpu.VMEM((n, width, quarter, tile), dtype),
            pltpu.VMEM((n, width * quarter, tile), jnp.float32),
            pltpu.VMEM((col_count, padded * width, 128), jnp.float32),
            pltpu.VMEM((col_count, padded * width, 128), jnp.float32),
            pltpu.VMEM((width, 128), jnp.int32),
            pltpu.VMEM((cells, width, 128), jnp.int32),
            pltpu.SMEM((width, 128), jnp.int32),
            pltpu.VMEM((8 + planes, 128), jnp.int32),
            pltpu.SMEM((8 + planes, 128), jnp.int32),
            pltpu.VMEM((lists + 8, 128), jnp.int32),
            pltpu.SMEM((lists + 8, 128), jnp.int32),
            pltpu.VMEM((cells, 8, 128), jnp.int32),
            pltpu.SemaphoreType.DMA((7,)),
            pltpu.SemaphoreType.DMA((cells,)),
            pltpu.SemaphoreType.DMA((cells,)),
            pltpu.SemaphoreType.DMA((cells,)),
            pltpu.SemaphoreType.DMA((cells,)),
            pltpu.SemaphoreType.DMA((2, 3, cells)),
            pltpu.SemaphoreType.DMA((2, cells)),
            pltpu.SemaphoreType.DMA((3, cells)),
            pltpu.SemaphoreType.DMA((3, cells)),
            pltpu.SemaphoreType.DMA((2,)),
            pltpu.SemaphoreType.DMA((col_count,)),
            pltpu.SemaphoreType.DMA((col_count,)),
            pltpu.SemaphoreType.DMA((3,)),
            pltpu.SemaphoreType.DMA((3,)),
        ],
        compiler_params=pltpu.CompilerParams(
            collective_id=2, has_side_effects=True, vmem_limit_bytes=60 * 1024 * 1024
        ),
    )(density_tiles.reshape(n, width, tile, tile), tile_columns.reshape(n, width).T)
    out = out.reshape(n, group_count, slots, quarter, tile)
    return lax.cond(
        flag[0, 0] > 0,
        lambda: on_device_paired(density_tiles, tile_columns),
        lambda: out,
    )


def solution(mesh):
    paired = mesh.shape["row"] == 2 and mesh.shape["layer"] % 2 == 0
    four = paired and mesh.shape["layer"] == 4

    def on_each(density_tiles, tile_columns):
        n, group_count, slots, tile, _ = density_tiles.shape
        block_count = n * mesh.shape["row"] * mesh.shape["col"]
        fits = four and n % 8 == 0 and n <= 128 and group_count * slots <= 15 and slots > 0
        fits = fits and (block_count // group_count) % n == 0 and tile % 128 == 0
        fits = fits and mesh.shape["col"] <= 16
        if fits:
            return on_device_sparse(density_tiles, tile_columns)
        return (on_device_paired if paired else on_device)(density_tiles, tile_columns)

    in_specs = (P(("row", "col"), None, None, None, None), P(("row", "col"), None, None))
    out_specs = P(("row", "col"), None, None, "layer", None)
    return jax.shard_map(
        on_each, mesh=mesh, in_specs=in_specs, out_specs=out_specs, check_vma=False
    )
```

```python
import functools

import jax
import jax.numpy as jnp
from jax import lax
from jax.experimental import pallas as pl
from jax.experimental.pallas import tpu as pltpu
from jax.sharding import PartitionSpec as P

MESH = pl.DeviceIdType.MESH


def divisor(total, most):
    return max(d for d in range(1, most + 1) if total % d == 0)


def kernel(
    sizes, columns_ref, tiles_ref, meta_ref, out_ref,
    left, right, meta_all, meta_smem, stage,
    local_sem, meta_send, meta_recv, send_sem, recv_sem, out_send, out_recv,
):
    row_count, col_count, layer_count, chunks, out_chunks, is_balanced = sizes
    n, group_count, slots, tile, _ = tiles_ref.shape
    cells = row_count * col_count
    per_layer = group_count // layer_count
    quarter = tile // layer_count
    width = group_count * slots
    r, c, l = lax.axis_index("row"), lax.axis_index("col"), lax.axis_index("layer")
    me = r * col_count + c
    own_groups = pl.ds(l * per_layer, per_layer)

    own_copy = pltpu.make_async_copy(
        tiles_ref.at[:, own_groups], right.at[pl.ds(me * n, n)], local_sem.at[0]
    )
    left_copy = pltpu.make_async_copy(tiles_ref, left, local_sem.at[1])
    meta_copy = pltpu.make_async_copy(meta_ref, meta_all.at[pl.ds(me * n, n)], local_sem.at[2])
    own_copy.start()
    meta_copy.start()
    left_copy.start()
    right[cells * n] = jnp.zeros(right.shape[1:], right.dtype)

    def cell_id(offset):
        target = lax.rem(me + offset, cells)
        return {"row": lax.div(target, col_count), "col": lax.rem(target, col_count)}

    def layer_id(offset):
        return {"layer": lax.rem(l + offset, layer_count)}

    barrier = pltpu.get_barrier_semaphore()
    for offset in range(1, cells):
        pl.semaphore_signal(barrier, inc=1, device_id=cell_id(offset), device_id_type=MESH)
    for offset in range(1, layer_count):
        pl.semaphore_signal(barrier, inc=1, device_id=layer_id(offset), device_id_type=MESH)
    pl.semaphore_wait(barrier, cells - 1 + layer_count - 1)
    own_copy.wait()

    step_rows = n // chunks
    sent = []

    def rows_of(cell, chunk):
        return pl.ds(cell * n + chunk * step_rows, step_rows)

    def copy_of(cell, chunk, way, device):
        return pltpu.make_async_remote_copy(
            src_ref=right.at[rows_of(cell, chunk)],
            dst_ref=right.at[rows_of(cell, chunk)],
            send_sem=send_sem.at[way, cell, chunk],
            recv_sem=recv_sem.at[cell, chunk],
            device_id=device,
            device_id_type=MESH,
        )

    ways = {
        "up": (0, c < col_count - 1, {"col": jnp.minimum(c + 1, col_count - 1)}),
        "down": (1, c > 0, {"col": jnp.maximum(c - 1, 0)}),
        "south": (2, r < row_count - 1, {"row": jnp.minimum(r + 1, row_count - 1)}),
        "north": (3, r > 0, {"row": jnp.maximum(r - 1, 0)}),
    }

    def send(cell, chunk, way, condition=True):
        index, exists, device = ways[way]
        wanted = jnp.logical_and(exists, condition)

        @pl.when(wanted)
        def _():
            copy_of(cell, chunk, index, device).start()

        sent.append((wanted, cell, chunk, index, device))

    def await_arrival(cell, chunk):
        copy_of(cell, chunk, 0, {"col": c}).wait_recv()

    for chunk in range(chunks):
        for way in ("up", "down", "south", "north"):
            send(me, chunk, way)

    meta_copy.wait()
    meta_copies = []
    for offset in range(1, cells):
        copy = pltpu.make_async_remote_copy(
            src_ref=meta_ref,
            dst_ref=meta_all.at[pl.ds(me * n, n)],
            send_sem=meta_send.at[offset],
            recv_sem=meta_recv.at[offset],
            device_id=cell_id(offset),
            device_id_type=MESH,
        )
        copy.start()
        meta_copies.append(copy)

    even = lax.rem(c, 2) == 0
    for step in range(1, col_count):
        for chunk in range(chunks):
            for origin, has, way, is_pair in (
                (c - step, c >= step, "up", jnp.logical_not(even)),
                (c + step, c + step < col_count, "down", even),
            ):
                origin = jnp.clip(origin, 0, col_count - 1)
                cell = r * col_count + origin

                @pl.when(has)
                def _():
                    await_arrival(cell, chunk)

                send(cell, chunk, way, has)
                across = has
                if is_balanced and step == 1 and chunk >= chunks // 2:
                    across = jnp.logical_and(has, jnp.logical_not(is_pair))
                send(cell, chunk, "south", across)
                send(cell, chunk, "north", across)

    if is_balanced:
        other = (1 - r) * col_count + c
        for chunk in range(chunks):
            await_arrival(other, chunk)
            if chunk >= chunks // 2:
                send(other, chunk, "up", even)
                send(other, chunk, "down", jnp.logical_not(even))
        for step in range(1, col_count):
            origin = (1 - r) * col_count + lax.rem(c + step, col_count)
            for chunk in range(chunks):
                await_arrival(origin, chunk)
    else:
        for step in range(1, row_count):
            for shift in range(col_count):
                for chunk in range(chunks):
                    for origin, has, way in (
                        (r - step, r >= step, "south"),
                        (r + step, r + step < row_count, "north"),
                    ):
                        origin = jnp.clip(origin, 0, row_count - 1)
                        cell = origin * col_count + lax.rem(c + shift, col_count)

                        @pl.when(has)
                        def _():
                            await_arrival(cell, chunk)

                        send(cell, chunk, way, has)

    for copy in meta_copies:
        copy.wait()
    table_copy = pltpu.make_async_copy(meta_all, meta_smem, local_sem.at[3])
    table_copy.start()
    table_copy.wait()
    left_copy.wait()

    def one_row(i, carry):
        targets = [
            columns_ref[i * width + l * per_layer * slots + s] for s in range(per_layer * slots)
        ]
        strips = []
        for a in range(width):
            k = columns_ref[i * width + a]
            inner = jnp.maximum(k, 0)
            pieces = []
            for s in range(per_layer * slots):
                group = s // slots
                row_index = jnp.int32(cells * n)
                slot_index = jnp.int32(0)
                is_live = (k >= 0) & (targets[s] >= 0)
                for t in range(slots):
                    hit = (meta_smem[inner, 0, group * slots + t] == targets[s]) & is_live
                    row_index = jnp.where(hit, inner, row_index)
                    slot_index = jnp.where(hit, t, slot_index)
                pieces.append(right[row_index, group, slot_index])
            strips.append(jnp.concatenate(pieces, axis=1))
        rights = jnp.concatenate(strips, axis=0)
        lefts = jnp.concatenate(
            [left[i, a // slots, a % slots] for a in range(width)], axis=1
        )
        total = jnp.dot(lefts, rights, preferred_element_type=jnp.float32).astype(stage.dtype)
        for q in range(layer_count):
            for s in range(per_layer * slots):
                stage[q, i, s // slots, s % slots] = total[
                    q * quarter:(q + 1) * quarter, s * tile:(s + 1) * tile
                ]
        return carry

    out_rows = n // out_chunks

    def out_copies(chunk):
        rows = pl.ds(chunk * out_rows, out_rows)
        copies = []
        for offset in range(layer_count):
            q = lax.rem(l + offset, layer_count)
            if offset == 0:
                copies.append(pltpu.make_async_copy(
                    stage.at[q, rows], out_ref.at[rows, own_groups], out_send.at[0, chunk]
                ))
            else:
                copies.append(pltpu.make_async_remote_copy(
                    src_ref=stage.at[q, rows],
                    dst_ref=out_ref.at[rows, own_groups],
                    send_sem=out_send.at[offset, chunk],
                    recv_sem=out_recv.at[offset, chunk],
                    device_id=layer_id(offset),
                    device_id_type=MESH,
                ))
        return copies

    all_out = []
    for chunk in range(out_chunks + 1):
        if chunk < out_chunks:
            lax.fori_loop(chunk * out_rows, (chunk + 1) * out_rows, one_row, 0)
        if chunk > 0:
            copies = out_copies(chunk - 1)
            for copy in copies[1:] + copies[:1]:
                copy.start()
            all_out.extend(copies)

    for wanted, cell, chunk, index, device in sent:
        @pl.when(wanted)
        def _():
            copy_of(cell, chunk, index, device).wait_send()

    for copy in all_out:
        copy.wait()


def on_device(density_tiles, tile_columns):
    row_count = lax.axis_size("row")
    col_count = lax.axis_size("col")
    layer_count = lax.axis_size("layer")
    n, group_count, slots, tile, _ = density_tiles.shape
    cells = row_count * col_count
    per_layer = group_count // layer_count
    quarter = tile // layer_count
    kept = per_layer * slots
    chunks = divisor(n, 4)
    out_chunks = divisor(n, 4)
    is_balanced = row_count == 2 and col_count % 2 == 0 and chunks % 2 == 0
    own = lax.dynamic_slice_in_dim(tile_columns, lax.axis_index("layer") * per_layer, per_layer, 1)
    meta = jnp.pad(own.reshape(n, 1, kept), ((0, 0), (0, 0), (0, 128 - kept)), constant_values=-1)
    dtype = density_tiles.dtype
    sizes = (row_count, col_count, layer_count, chunks, out_chunks, is_balanced)
    return pl.pallas_call(
        functools.partial(kernel, sizes),
        out_shape=jax.ShapeDtypeStruct((n, group_count, slots, quarter, tile), dtype),
        in_specs=[
            pl.BlockSpec(memory_space=pltpu.SMEM),
            pl.BlockSpec(memory_space=pl.ANY),
            pl.BlockSpec(memory_space=pltpu.VMEM),
        ],
        out_specs=pl.BlockSpec(memory_space=pl.ANY),
        scratch_shapes=[
            pltpu.VMEM(density_tiles.shape, dtype),
            pltpu.VMEM((cells * n + 1, per_layer, slots, tile, tile), dtype),
            pltpu.VMEM((cells * n, 1, 128), jnp.int32),
            pltpu.SMEM((cells * n, 1, 128), jnp.int32),
            pltpu.VMEM((layer_count, n, per_layer, slots, quarter, tile), dtype),
            pltpu.SemaphoreType.DMA((4,)),
            pltpu.SemaphoreType.DMA((cells,)),
            pltpu.SemaphoreType.DMA((cells,)),
            pltpu.SemaphoreType.DMA((4, cells, chunks)),
            pltpu.SemaphoreType.DMA((cells, chunks)),
            pltpu.SemaphoreType.DMA((layer_count, out_chunks)),
            pltpu.SemaphoreType.DMA((layer_count, out_chunks)),
        ],
        compiler_params=pltpu.CompilerParams(
            collective_id=0, has_side_effects=True, vmem_limit_bytes=60 * 1024 * 1024
        ),
    )(tile_columns.reshape(-1), density_tiles, meta)


def paired_kernel(
    sizes, tiles_ref, meta_ref, out_ref,
    left, right, meta_all, meta_smem, stage,
    local_sem, meta_send, meta_recv, send_sem, recv_sem, left_send, left_recv, out_send, out_recv,
):
    col_count, layer_count, chunks, out_chunks = sizes
    n, group_count, slots, tile, _ = tiles_ref.shape
    cells = 2 * col_count
    per_layer = group_count // layer_count
    quarter = tile // layer_count
    width = group_count * slots
    r, c, l = lax.axis_index("row"), lax.axis_index("col"), lax.axis_index("layer")
    high, k = lax.div(l, 2), lax.rem(l, 2)
    me = r * col_count + c
    base = k * col_count + c
    is_home = k == r
    is_guest = jnp.logical_not(is_home)
    group = 2 * high + r
    own_groups = pl.ds(group * per_layer, per_layer)
    other_groups = pl.ds((2 * high + 1 - r) * per_layer, per_layer)
    facing = {"row": 1 - r}
    partner = {"layer": 2 * high + 1 - k}

    own_copy = pltpu.make_async_copy(
        tiles_ref.at[:, own_groups], right.at[pl.ds(me * n, n)], local_sem.at[0]
    )
    left_copy = pltpu.make_async_copy(tiles_ref, left, local_sem.at[1])
    meta_copy = pltpu.make_async_copy(meta_ref, meta_all.at[pl.ds(me * n, n)], local_sem.at[2])
    own_copy.start()
    meta_copy.start()

    @pl.when(is_home)
    def _():
        left_copy.start()

    right[cells * n] = jnp.zeros(right.shape[1:], right.dtype)

    def cell_id(offset):
        target = lax.rem(me + offset, cells)
        return {"row": lax.div(target, col_count), "col": lax.rem(target, col_count)}

    barrier = pltpu.get_barrier_semaphore()
    for offset in range(1, cells):
        pl.semaphore_signal(barrier, inc=1, device_id=cell_id(offset), device_id_type=MESH)
    for offset in range(1, layer_count):
        for row in (r, 1 - r):
            pl.semaphore_signal(
                barrier,
                inc=1,
                device_id={"row": row, "layer": lax.rem(l + offset, layer_count)},
                device_id_type=MESH,
            )
    pl.semaphore_wait(barrier, cells - 1 + 2 * (layer_count - 1))

    step_rows = n // chunks
    sent = []

    def rows_of(cell, chunk):
        return pl.ds(cell * n + chunk * step_rows, step_rows)

    def copy_of(cell, chunk, way, device):
        source = right.at[rows_of(cell, chunk)]
        if way == 3:
            source = tiles_ref.at[pl.ds(chunk * step_rows, step_rows), other_groups]
        return pltpu.make_async_remote_copy(
            src_ref=source,
            dst_ref=right.at[rows_of(cell, chunk)],
            send_sem=send_sem.at[way, cell, chunk],
            recv_sem=recv_sem.at[cell, chunk],
            device_id=device,
            device_id_type=MESH,
        )

    ways = {
        "up": (0, c < col_count - 1, {"col": jnp.minimum(c + 1, col_count - 1)}),
        "down": (1, c > 0, {"col": jnp.maximum(c - 1, 0)}),
        "partner": (2, True, partner),
        "facing": (3, True, facing),
    }

    def send(cell, chunk, way, condition):
        index, exists, device = ways[way]
        wanted = jnp.logical_and(exists, condition)

        @pl.when(wanted)
        def _():
            copy_of(cell, chunk, index, device).start()

        sent.append((wanted, cell, chunk, index, device))

    def await_arrival(cell, chunk, condition):
        @pl.when(condition)
        def _():
            copy_of(cell, chunk, 2, partner).wait_recv()

    for chunk in range(chunks):
        send(me, chunk, "facing", is_home)
    own_copy.wait()
    for chunk in range(chunks):
        for way in ("up", "down"):
            send(me, chunk, way, is_home)
    left_out = pltpu.make_async_remote_copy(
        src_ref=tiles_ref, dst_ref=left, send_sem=left_send, recv_sem=left_recv,
        device_id=facing, device_id_type=MESH,
    )

    meta_copy.wait()
    meta_copies = []
    for offset in range(1, cells):
        copy = pltpu.make_async_remote_copy(
            src_ref=meta_ref,
            dst_ref=meta_all.at[pl.ds(me * n, n)],
            send_sem=meta_send.at[offset],
            recv_sem=meta_recv.at[offset],
            device_id=cell_id(offset),
            device_id_type=MESH,
        )
        copy.start()
        meta_copies.append(copy)

    @pl.when(is_home)
    def _():
        left_out.start()

    for chunk in range(chunks):
        await_arrival(base, chunk, is_guest)
        for way in ("up", "down", "partner"):
            send(base, chunk, way, is_guest)

    for step in range(1, col_count):
        for chunk in range(chunks):
            for origin, has, way in (
                (c - step, c >= step, "up"),
                (c + step, c + step < col_count, "down"),
            ):
                cell = k * col_count + jnp.clip(origin, 0, col_count - 1)
                await_arrival(cell, chunk, has)
                send(cell, chunk, way, has)
                send(cell, chunk, "partner", has)

    for chunk in range(chunks):
        await_arrival((1 - k) * col_count + c, chunk, is_home)
    for step in range(1, col_count):
        cell = (1 - k) * col_count + lax.rem(c + step, col_count)
        for chunk in range(chunks):
            await_arrival(cell, chunk, True)

    for copy in meta_copies:
        copy.wait()
    table_copy = pltpu.make_async_copy(meta_all, meta_smem, local_sem.at[3])
    table_copy.start()
    table_copy.wait()

    @pl.when(is_home)
    def _():
        left_copy.wait()

    @pl.when(is_guest)
    def _():
        left_out.wait_recv()

    first = group * per_layer * slots

    def one_row(i, carry):
        block_row = base * n + i
        targets = [meta_smem[block_row, 0, first + s] for s in range(per_layer * slots)]
        strips = []
        for a in range(width):
            column = meta_smem[block_row, 0, a]
            inner = jnp.maximum(column, 0)
            pieces = []
            for s in range(per_layer * slots):
                part = s // slots
                row_index = jnp.int32(cells * n)
                slot_index = jnp.int32(0)
                is_live = (column >= 0) & (targets[s] >= 0)
                for t in range(slots):
                    hit = (meta_smem[inner, 0, first + part * slots + t] == targets[s]) & is_live
                    row_index = jnp.where(hit, inner, row_index)
                    slot_index = jnp.where(hit, t, slot_index)
                pieces.append(right[row_index, part, slot_index])
            strips.append(jnp.concatenate(pieces, axis=1))
        rights = jnp.concatenate(strips, axis=0)
        lefts = jnp.concatenate(
            [left[i, a // slots, a % slots] for a in range(width)], axis=1
        )
        total = jnp.dot(lefts, rights, preferred_element_type=jnp.float32).astype(stage.dtype)
        for q in range(layer_count):
            for s in range(per_layer * slots):
                stage[q, i, s // slots, s % slots] = total[
                    q * quarter:(q + 1) * quarter, s * tile:(s + 1) * tile
                ]
        return carry

    out_rows = n // out_chunks

    def out_copy(chunk, q, source):
        rows = pl.ds(chunk * out_rows, out_rows)
        return pltpu.make_async_remote_copy(
            src_ref=stage.at[q, rows],
            dst_ref=out_ref.at[rows, pl.ds(source * per_layer, per_layer)],
            send_sem=out_send.at[q, chunk],
            recv_sem=out_recv.at[source, chunk],
            device_id={"row": k, "layer": q},
            device_id_type=MESH,
        )

    def kept_copy(chunk):
        rows = pl.ds(chunk * out_rows, out_rows)
        return pltpu.make_async_copy(
            stage.at[l, rows], out_ref.at[rows, own_groups], out_send.at[l, chunk]
        )

    for chunk in range(out_chunks + 1):
        if chunk < out_chunks:
            lax.fori_loop(chunk * out_rows, (chunk + 1) * out_rows, one_row, 0)
        if chunk > 0:
            for offset in range(layer_count - 1, -1, -1):
                q = lax.rem(l + offset, layer_count)
                if offset:
                    out_copy(chunk - 1, q, group).start()
                else:
                    @pl.when(is_guest)
                    def _():
                        out_copy(chunk - 1, q, group).start()

                    @pl.when(is_home)
                    def _():
                        kept_copy(chunk - 1).start()

    for wanted, cell, chunk, index, device in sent:
        @pl.when(wanted)
        def _():
            copy_of(cell, chunk, index, device).wait_send()

    @pl.when(is_home)
    def _():
        left_out.wait_send()

    for chunk in range(out_chunks):
        for offset in range(layer_count):
            q = lax.rem(l + offset, layer_count)
            source = lax.rem(group + offset, layer_count)
            if offset:
                out_copy(chunk, q, source).wait()
            else:
                @pl.when(is_guest)
                def _():
                    out_copy(chunk, q, source).wait()

                @pl.when(is_home)
                def _():
                    kept_copy(chunk).wait()


def on_device_paired(density_tiles, tile_columns):
    col_count = lax.axis_size("col")
    layer_count = lax.axis_size("layer")
    n, group_count, slots, tile, _ = density_tiles.shape
    cells = 2 * col_count
    per_layer = group_count // layer_count
    quarter = tile // layer_count
    width = group_count * slots
    chunks = divisor(n, 2)
    out_chunks = divisor(n, 12)
    lanes = -(-width // 128) * 128
    meta = jnp.pad(
        tile_columns.reshape(n, 1, width), ((0, 0), (0, 0), (0, lanes - width)), constant_values=-1
    )
    dtype = density_tiles.dtype
    return pl.pallas_call(
        functools.partial(paired_kernel, (col_count, layer_count, chunks, out_chunks)),
        out_shape=jax.ShapeDtypeStruct((n, group_count, slots, quarter, tile), dtype),
        in_specs=[
            pl.BlockSpec(memory_space=pl.ANY),
            pl.BlockSpec(memory_space=pltpu.VMEM),
        ],
        out_specs=pl.BlockSpec(memory_space=pl.ANY),
        scratch_shapes=[
            pltpu.VMEM(density_tiles.shape, dtype),
            pltpu.VMEM((cells * n + 1, per_layer, slots, tile, tile), dtype),
            pltpu.VMEM((cells * n, 1, lanes), jnp.int32),
            pltpu.SMEM((cells * n, 1, lanes), jnp.int32),
            pltpu.VMEM((layer_count, n, per_layer, slots, quarter, tile), dtype),
            pltpu.SemaphoreType.DMA((4,)),
            pltpu.SemaphoreType.DMA((cells,)),
            pltpu.SemaphoreType.DMA((cells,)),
            pltpu.SemaphoreType.DMA((4, cells, chunks)),
            pltpu.SemaphoreType.DMA((cells, chunks)),
            pltpu.SemaphoreType.DMA,
            pltpu.SemaphoreType.DMA,
            pltpu.SemaphoreType.DMA((layer_count, out_chunks)),
            pltpu.SemaphoreType.DMA((layer_count, out_chunks)),
        ],
        compiler_params=pltpu.CompilerParams(
            collective_id=1, has_side_effects=True, vmem_limit_bytes=60 * 1024 * 1024
        ),
    )(density_tiles, meta)


def sparse_kernel(
    sizes, tiles_ref, columns_ref, out_ref, flag_ref,
    left, diag, extra, lent, borrowed, pack, arrived, stage, total, needs, ranks, meta_own, meta_all, meta_smem,
    send_list, send_smem, row_list, row_smem, flag_all,
    local_sem, meta_send, meta_recv, flag_send, flag_recv,
    main_send, main_recv, side_send, side_recv, lent_sem, pack_send, pack_recv, extra_send, extra_recv,
):
    row_count, col_count, layer_count, group_count, per_row, padded = sizes
    n, width, tile, _ = tiles_ref.shape
    per_lent, per_plane, pool = lent.shape[0], pack.shape[1], extra.shape[0]
    cells = row_count * col_count
    quarter = tile // layer_count
    entries = padded * width
    span = -(-(cells * n) // 128) * 128
    lists = -(-per_row // 8) * 8
    r, c, l = lax.axis_index("row"), lax.axis_index("col"), lax.axis_index("layer")
    x, k = lax.div(l, 2), lax.rem(l, 2)
    facing_layer = 2 * (1 - x) + k
    me = r * col_count + c
    opposite = (1 - r) * col_count + c
    own_slot = lax.div(me * n * group_count, cells * n) * (width // group_count)
    partner = {"layer": 2 * x + 1 - k}
    facing = {"layer": facing_layer}

    diag_copy = pltpu.make_async_copy(
        tiles_ref.at[:, own_slot], diag.at[pl.ds(me * n, n)], local_sem.at[1]
    )
    left_copy = pltpu.make_async_copy(tiles_ref, left, local_sem.at[2])
    table_copy = pltpu.make_async_copy(meta_own, meta_smem, local_sem.at[3])
    diag_copy.start()
    left_copy.start()
    meta_own[...] = jnp.full(meta_own.shape, -1, jnp.int32)
    meta_own[:, 0:n] = columns_ref[...]
    meta_all[me] = meta_own[...]

    def cell_id(cell):
        return {"row": lax.div(cell, col_count), "col": lax.rem(cell, col_count)}

    def other_cell(offset):
        return lax.rem(me + offset, cells)

    barrier = pltpu.get_barrier_semaphore()
    for offset in range(1, cells):
        pl.semaphore_signal(
            barrier, inc=1, device_id=cell_id(other_cell(offset)), device_id_type=MESH
        )
    for device in (partner, facing):
        pl.semaphore_signal(barrier, inc=1, device_id=device, device_id_type=MESH)
    pl.semaphore_wait(barrier, cells - 1 + 2)

    sent = []

    def remote(source, target, send, recv, device):
        return pltpu.make_async_remote_copy(
            src_ref=source, dst_ref=target, send_sem=send, recv_sem=recv,
            device_id=device, device_id_type=MESH,
        )

    def launch(copy, condition=True):
        if condition is True:
            copy.start()
        else:
            @pl.when(condition)
            def _():
                copy.start()
        sent.append((copy, condition))

    def await_recv(copy, condition=True):
        if condition is True:
            copy.wait_recv()
        else:
            @pl.when(condition)
            def _():
                copy.wait_recv()

    def part(cell, q):
        return diag.at[pl.ds(cell * n, n), pl.ds(q * quarter, quarter)]

    up = {"col": jnp.minimum(c + 1, col_count - 1)}
    down = {"col": jnp.maximum(c - 1, 0)}
    across = {"row": 1 - r}

    def line_copy(cell, way, wide=0):
        device = (up, down, across)[way]
        piece = part(cell, facing_layer if wide else l)
        return remote(
            piece, piece, main_send.at[wide, way, cell], main_recv.at[wide, cell], device
        )

    def side_copy(cell, way):
        device = (partner, facing, partner)[way]
        piece = part(cell, facing_layer if way == 2 else l)
        return remote(piece, piece, side_send.at[way, cell], side_recv.at[way, cell], device)

    meta_copies = []
    for offset in range(1, cells):
        copy = remote(
            meta_own, meta_all.at[me], meta_send.at[offset], meta_recv.at[offset],
            cell_id(other_cell(offset)),
        )
        copy.start()
        meta_copies.append(copy)
    diag_copy.wait()
    has_up, has_down = c < col_count - 1, c > 0
    launch(line_copy(me, 0), has_up)
    launch(line_copy(me, 1), has_down)
    launch(line_copy(me, 2))
    table_copy.start()
    for copy in meta_copies:
        copy.wait_recv()

    small_row = lax.broadcasted_iota(jnp.int32, (padded, 128), 0)
    small_lane = lax.broadcasted_iota(jnp.int32, (padded, 128), 1)
    wide_row = lax.broadcasted_iota(jnp.int32, (padded, span), 0)
    wide_lane = lax.broadcasted_iota(jnp.int32, (padded, span), 1)
    tall_row = lax.broadcasted_iota(jnp.int32, (span, 128), 0)
    entry_row = lax.broadcasted_iota(jnp.int32, (entries, 128), 0)
    entry_lane = lax.broadcasted_iota(jnp.int32, (entries, 128), 1).astype(jnp.float32)
    before = (
        lax.broadcasted_iota(jnp.int32, (entries, entries), 0)
        > lax.broadcasted_iota(jnp.int32, (entries, entries), 1)
    ).astype(jnp.float32).astype(jnp.bfloat16)
    ones = jnp.ones((128, 128), jnp.bfloat16)

    def dot(a, b):
        return jnp.dot(a, b, preferred_element_type=jnp.float32)

    def chosen(cell):
        columns = jnp.transpose(meta_all[cell])[0:padded]
        pieces = []
        for b in range(width):
            hit = (columns[:, b:b + 1] == wide_lane) & (wide_lane != wide_row + cell * n)
            pieces.append(jnp.where(hit, 1.0, 0.0))
        return jnp.concatenate(pieces, axis=0).astype(jnp.bfloat16)

    def listing(cell):
        rows = meta_all[cell]
        weight = jnp.zeros((span, 128), jnp.float32)
        for a in range(width):
            weight = jnp.where(rows[a:a + 1] == tall_row, a + 1.0, weight)
        return weight.astype(jnp.bfloat16)

    def inner_listing(source, cell):
        rows = meta_all[cell]
        weight = jnp.zeros((padded, 128), jnp.float32)
        for a in range(width):
            weight = jnp.where(rows[a:a + 1] == small_row + source * n, a + 1.0, weight)
        weight = jnp.where(small_row + source * n == small_lane + cell * n, 0.0, weight)
        return jnp.concatenate([weight] * width, axis=0)

    def matches(picked, listed, inner):
        goal = dot(picked, listed)
        hit = jnp.where((goal > 0) & (inner > 0), 1.0, 0.0)
        needed = jnp.where(dot(hit.astype(jnp.bfloat16), ones) > 0, 1.0, 0.0)
        return goal, hit, needed

    def rank_of(needed):
        return dot(before, needed.astype(jnp.bfloat16))

    def count_of(needed):
        return jnp.sum(needed, axis=0, keepdims=True)

    def picks_of(needed, rank, value):
        chosen_values = jnp.where((rank == entry_lane) & (needed > 0), value, 0.0)
        return jnp.sum(chosen_values, axis=0, keepdims=True)

    slot_value = (
        lax.rem(entry_row, padded) * width + lax.div(entry_row, padded)
    ).astype(jnp.float32)
    mine, theirs = chosen(me), chosen(opposite)
    none = jnp.zeros((entries, 128), jnp.float32)
    my_rows = pl.ds(pl.multiple_of(l * quarter, quarter), quarter)

    def lent_step(at, wanted):
        cell = (1 - r) * col_count + at
        return jnp.maximum(wanted, matches(mine, listing(cell), inner_listing(me, cell))[2])

    wanted = lax.fori_loop(0, col_count, lent_step, none, unroll=True)
    send_list[0:1] = picks_of(wanted, rank_of(wanted), slot_value).astype(jnp.int32)
    lent_most = count_of(wanted)
    lent_list = pltpu.make_async_copy(send_list.at[0], send_smem.at[0], local_sem.at[4])
    lent_list.start()
    lent_list.wait()
    left_copy.wait()

    def own_piece(code):
        code = jnp.clip(code, 0, n * width - 1)
        return left[lax.div(code, width), lax.rem(code, width), my_rows]

    def lent_pack(m, carry):
        lent[m] = own_piece(send_smem[0, m])
        return carry

    lax.fori_loop(0, per_lent, lent_pack, 0, unroll=4)
    lent_copy = remote(lent, borrowed, lent_sem.at[0], lent_sem.at[1], across)
    launch(lent_copy)

    def share(cell, condition=True, wide=False):
        launch(side_copy(cell, 0), condition)
        if not wide:
            launch(side_copy(cell, 1), condition)

    def take_line(cell, has, way, wide):
        await_recv(line_copy(cell, way), has)
        launch(line_copy(cell, way), jnp.logical_and(has, has_up if way == 0 else has_down))
        share(cell, has, wide)
        launch(line_copy(cell, 2), has)

    line, beyond = [], []
    for step in range(1, col_count):
        for origin, has, way in ((c - step, c >= step, 0), (c + step, c + step < col_count, 1)):
            origin = jnp.clip(origin, 0, col_count - 1)
            line.append((r * col_count + origin, has, way, step == 1))
            beyond.append(((1 - r) * col_count + origin, has))

    for entry in line[:2]:
        take_line(*entry)

    for entry in line[2:4]:
        take_line(*entry)
    launch(line_copy(me, 2, 1))

    def plane_step(at, wanted):
        cell = r * col_count + at
        listed = listing(cell)
        own = matches(mine, listed, inner_listing(me, cell))[2]
        send_list[pl.ds(8 + at, 1)] = picks_of(own, rank_of(own), slot_value).astype(jnp.int32)
        their = matches(theirs, listed, inner_listing(opposite, cell))[2]
        needs[at] = their
        ranks[at] = rank_of(their) + count_of(own)
        return jnp.maximum(wanted, their)

    wanted = lax.fori_loop(0, col_count, plane_step, none, unroll=True)
    borrowed_value = rank_of(wanted) + float(n * width)

    def plane_finish(at, carry):
        picks = picks_of(needs[at], ranks[at], borrowed_value).astype(jnp.int32)
        send_list[pl.ds(8 + at, 1)] += picks
        return carry

    lax.fori_loop(0, col_count, plane_finish, 0, unroll=True)
    rows_used = send_list.shape[0] - 8
    plane_list = pltpu.make_async_copy(
        send_list.at[pl.ds(8, rows_used)], send_smem.at[pl.ds(8, rows_used)], local_sem.at[4]
    )
    plane_list.start()

    await_recv(line_copy(opposite, 2))
    share(opposite, True, True)
    plane_list.wait()
    await_recv(lent_copy)

    def plane_piece(at, m):
        code = send_smem[8 + at, m]
        loaned = borrowed[jnp.clip(code - n * width, 0, per_lent - 1)]
        return jnp.where(code < n * width, own_piece(code), loaned)

    def plane_pack(m, carry):
        for offset in range(col_count):
            at = lax.rem(c + offset, col_count)
            if offset:
                pack[offset, m] = plane_piece(at, m)
            else:
                arrived[c, m] = plane_piece(at, m)
        return carry

    lax.fori_loop(0, per_plane, plane_pack, 0, unroll=2)

    def pack_copy(offset, origin):
        return remote(
            pack.at[offset], arrived.at[origin], pack_send.at[offset], pack_recv.at[origin],
            {"col": lax.rem(c + offset, col_count)},
        )

    for offset in sorted(range(1, col_count), key=lambda o: abs(2 * o - col_count)):
        launch(pack_copy(offset, c))

    def take_beyond(cell, has):
        await_recv(line_copy(cell, 2), has)
        share(cell, has)

    for entry in line[4:]:
        take_line(*entry)
    for entry in beyond[:2]:
        take_beyond(*entry)

    listed = listing(me)
    list_row = lax.broadcasted_iota(jnp.int32, (lists + 8, 128), 0)

    def row_step(at, carry):
        held, running, pooled, in_plane, most = carry
        plane, far = lax.div(at, 2), lax.rem(at, 2)
        source = jnp.where(far == 0, r, 1 - r) * col_count + plane
        in_plane = jnp.where(far == 0, 0.0, in_plane)
        inner = inner_listing(source, me)
        goal, hit, needed = matches(chosen(source), listed, inner)
        rank = rank_of(needed)
        place = dot(before, hit.astype(jnp.bfloat16)) + running
        value = (((rank + pooled) * 16.0 + (inner - 1.0)) * 16.0 + goal) * hit
        for q in range(per_row):
            line_sum = jnp.sum(jnp.where(place == float(q), value, 0.0), axis=0, keepdims=True)
            held = held + jnp.where(list_row == q, line_sum, 0.0)
        spot = rank + in_plane + (plane * per_plane).astype(jnp.float32)
        held = held + jnp.where(list_row == lists, picks_of(needed, rank + pooled, spot), 0.0)
        count = count_of(needed)
        in_plane = in_plane + count
        return held, running + count_of(hit), pooled + count, in_plane, jnp.maximum(most, in_plane)

    zero = jnp.zeros((1, 128), jnp.float32)
    held, running, pooled, _, most = lax.fori_loop(
        0, cells, row_step, (jnp.zeros((lists + 8, 128), jnp.float32), zero, zero, zero, zero),
        unroll=2,
    )
    row_list[...] = held.astype(jnp.int32)
    over = (most > per_plane) | (running > per_row) | (pooled > pool) | (lent_most > per_lent)
    flag_all[me] = jnp.broadcast_to(jnp.max(jnp.where(over, 1, 0)), (8, 128))
    row_copy = pltpu.make_async_copy(row_list, row_smem, local_sem.at[5])
    row_copy.start()
    flag_copies = []
    for offset in range(1, cells):
        copy = remote(
            flag_all.at[me], flag_all.at[me], flag_send.at[offset], flag_recv.at[offset],
            cell_id(other_cell(offset)),
        )
        copy.start()
        flag_copies.append(copy)

    def pass_on(cell, condition=True):
        await_recv(side_copy(cell, 1), condition)
        launch(side_copy(cell, 2), condition)

    def take_wide(cell, has, way, wide):
        await_recv(line_copy(cell, way, 1), has)
        launch(side_copy(cell, 2), has)

    for entry in beyond[2:]:
        take_beyond(*entry)
    launch(line_copy(me, 0, 1), has_up)
    launch(line_copy(me, 1, 1), has_down)
    row_copy.wait()
    for offset in range(1, col_count):
        await_recv(pack_copy(offset, lax.rem(c + offset, col_count)))

    def pool_pack(m, carry):
        code = jnp.clip(row_smem[lists, m], 0, col_count * per_plane - 1)
        extra[m, my_rows] = arrived[lax.div(code, per_plane), lax.rem(code, per_plane)]
        return carry

    lax.fori_loop(0, pool, pool_pack, 0, unroll=4)

    def extra_copy(way):
        device = (partner, facing, partner)[way]
        piece = extra.at[:, pl.ds((facing_layer if way == 2 else l) * quarter, quarter)]
        return remote(piece, piece, extra_send.at[way], extra_recv.at[way], device)

    launch(extra_copy(0))
    launch(extra_copy(1))
    for entry in line[:2]:
        take_wide(*entry)
    await_recv(line_copy(opposite, 2, 1))
    launch(side_copy(opposite, 2))
    for cell, has, _, _ in line[2:]:
        pass_on(cell, has)
    for cell, has in beyond:
        pass_on(cell, has)
    for offset in range(1, cells):
        await_recv(side_copy(other_cell(offset), 0))
        await_recv(side_copy(other_cell(offset), 2))
    table_copy.wait()

    def near_row(i, carry):
        own = left[i, own_slot, my_rows]
        pieces = []
        for t in range(width):
            column = meta_smem[t, i]
            lower = diag[jnp.maximum(column, 0)]
            own_left = left[i, t, my_rows]
            own_left = jnp.where(own_slot == t, jnp.zeros_like(own_left), own_left)
            value = dot(
                jnp.concatenate([own, own_left], axis=1),
                jnp.concatenate([left[i, t], lower], axis=0),
            )
            pieces.append(jnp.where(column >= 0, value, 0.0))
        total[i] = jnp.concatenate(pieces, axis=0)
        return carry

    lax.fori_loop(0, n, near_row, 0, unroll=2)
    await_recv(extra_copy(1))
    launch(extra_copy(2))
    await_recv(extra_copy(0))
    await_recv(extra_copy(2))

    def far_row(i, carry):
        lefts, rights = [], []
        for q in range(per_row):
            code = jnp.clip(row_smem[q, i], 0, pool * 256 - 1)
            goal = lax.rem(code, 16)
            at = jnp.minimum(lax.rem(lax.div(code, 16), 16), width - 1)
            piece = left[i, at, my_rows]
            lefts.append(jnp.concatenate(
                [jnp.where(goal == t + 1, piece, jnp.zeros_like(piece)) for t in range(width)], axis=0
            ))
            rights.append(extra[lax.div(code, 256)])
        value = total[i] + dot(
            jnp.concatenate(lefts, axis=1), jnp.concatenate(rights, axis=0)
        )
        stage[i] = value.astype(stage.dtype).reshape(width, quarter, tile)
        return carry

    lax.fori_loop(0, n, far_row, 0, unroll=8)
    out_copy = pltpu.make_async_copy(stage, out_ref, local_sem.at[6])
    out_copy.start()
    for copy in flag_copies:
        copy.wait_recv()
    flag_ref[0, 0] = jnp.max(flag_all[...])
    for copy in meta_copies + flag_copies:
        copy.wait_send()
    for copy, condition in sent:
        if condition is True:
            copy.wait_send()
        else:
            @pl.when(condition)
            def _():
                copy.wait_send()
    out_copy.wait()


def on_device_sparse(density_tiles, tile_columns):
    row_count = lax.axis_size("row")
    col_count = lax.axis_size("col")
    layer_count = lax.axis_size("layer")
    n, group_count, slots, tile, _ = density_tiles.shape
    cells = row_count * col_count
    quarter = tile // layer_count
    width = group_count * slots
    per_lent, per_plane, pool, per_row = 32, 24, 56, 8
    padded = -(-n // 32) * 32
    dtype = density_tiles.dtype
    sizes = (row_count, col_count, layer_count, group_count, per_row, padded)
    lists = -(-per_row // 8) * 8
    planes = -(-col_count // 8) * 8
    out, flag = pl.pallas_call(
        functools.partial(sparse_kernel, sizes),
        out_shape=(
            jax.ShapeDtypeStruct((n, width, quarter, tile), dtype),
            jax.ShapeDtypeStruct((1, 1), jnp.int32),
        ),
        in_specs=[
            pl.BlockSpec(memory_space=pl.ANY),
            pl.BlockSpec(memory_space=pltpu.VMEM),
        ],
        out_specs=(
            pl.BlockSpec(memory_space=pl.ANY),
            pl.BlockSpec(memory_space=pltpu.SMEM),
        ),
        scratch_shapes=[
            pltpu.VMEM((n, width, tile, tile), dtype),
            pltpu.VMEM((cells * n, tile, tile), dtype),
            pltpu.VMEM((pool, tile, tile), dtype),
            pltpu.VMEM((per_lent, quarter, tile), dtype),
            pltpu.VMEM((per_lent, quarter, tile), dtype),
            pltpu.VMEM((col_count, per_plane, quarter, tile), dtype),
            pltpu.VMEM((col_count, per_plane, quarter, tile), dtype),
            pltpu.VMEM((n, width, quarter, tile), dtype),
            pltpu.VMEM((n, width * quarter, tile), jnp.float32),
            pltpu.VMEM((col_count, padded * width, 128), jnp.float32),
            pltpu.VMEM((col_count, padded * width, 128), jnp.float32),
            pltpu.VMEM((width, 128), jnp.int32),
            pltpu.VMEM((cells, width, 128), jnp.int32),
            pltpu.SMEM((width, 128), jnp.int32),
            pltpu.VMEM((8 + planes, 128), jnp.int32),
            pltpu.SMEM((8 + planes, 128), jnp.int32),
            pltpu.VMEM((lists + 8, 128), jnp.int32),
            pltpu.SMEM((lists + 8, 128), jnp.int32),
            pltpu.VMEM((cells, 8, 128), jnp.int32),
            pltpu.SemaphoreType.DMA((7,)),
            pltpu.SemaphoreType.DMA((cells,)),
            pltpu.SemaphoreType.DMA((cells,)),
            pltpu.SemaphoreType.DMA((cells,)),
            pltpu.SemaphoreType.DMA((cells,)),
            pltpu.SemaphoreType.DMA((2, 3, cells)),
            pltpu.SemaphoreType.DMA((2, cells)),
            pltpu.SemaphoreType.DMA((3, cells)),
            pltpu.SemaphoreType.DMA((3, cells)),
            pltpu.SemaphoreType.DMA((2,)),
            pltpu.SemaphoreType.DMA((col_count,)),
            pltpu.SemaphoreType.DMA((col_count,)),
            pltpu.SemaphoreType.DMA((3,)),
            pltpu.SemaphoreType.DMA((3,)),
        ],
        compiler_params=pltpu.CompilerParams(
            collective_id=2, has_side_effects=True, vmem_limit_bytes=60 * 1024 * 1024
        ),
    )(density_tiles.reshape(n, width, tile, tile), tile_columns.reshape(n, width).T)
    out = out.reshape(n, group_count, slots, quarter, tile)
    return lax.cond(
        flag[0, 0] > 0,
        lambda: on_device_paired(density_tiles, tile_columns),
        lambda: out,
    )


def solution(mesh):
    paired = mesh.shape["row"] == 2 and mesh.shape["layer"] % 2 == 0
    four = paired and mesh.shape["layer"] == 4

    def on_each(density_tiles, tile_columns):
        n, group_count, slots, tile, _ = density_tiles.shape
        block_count = n * mesh.shape["row"] * mesh.shape["col"]
        fits = four and n % 8 == 0 and n <= 128 and group_count * slots <= 15 and slots > 0
        fits = fits and (block_count // group_count) % n == 0 and tile % 128 == 0
        fits = fits and mesh.shape["col"] <= 16
        if fits:
            return on_device_sparse(density_tiles, tile_columns)
        return (on_device_paired if paired else on_device)(density_tiles, tile_columns)

    in_specs = (P(("row", "col"), None, None, None, None), P(("row", "col"), None, None))
    out_specs = P(("row", "col"), None, None, "layer", None)
    return jax.shard_map(
        on_each, mesh=mesh, in_specs=in_specs, out_specs=out_specs, check_vma=False
    )
```

```python
import functools

import jax
import jax.numpy as jnp
from jax import lax
from jax.experimental import pallas as pl
from jax.experimental.pallas import tpu as pltpu
from jax.sharding import PartitionSpec as P

MESH = pl.DeviceIdType.MESH


def divisor(total, most):
    return max(d for d in range(1, most + 1) if total % d == 0)


def kernel(
    sizes, columns_ref, tiles_ref, meta_ref, out_ref,
    left, right, meta_all, meta_smem, stage,
    local_sem, meta_send, meta_recv, send_sem, recv_sem, out_send, out_recv,
):
    row_count, col_count, layer_count, chunks, out_chunks, is_balanced = sizes
    n, group_count, slots, tile, _ = tiles_ref.shape
    cells = row_count * col_count
    per_layer = group_count // layer_count
    quarter = tile // layer_count
    width = group_count * slots
    r, c, l = lax.axis_index("row"), lax.axis_index("col"), lax.axis_index("layer")
    me = r * col_count + c
    own_groups = pl.ds(l * per_layer, per_layer)

    own_copy = pltpu.make_async_copy(
        tiles_ref.at[:, own_groups], right.at[pl.ds(me * n, n)], local_sem.at[0]
    )
    left_copy = pltpu.make_async_copy(tiles_ref, left, local_sem.at[1])
    meta_copy = pltpu.make_async_copy(meta_ref, meta_all.at[pl.ds(me * n, n)], local_sem.at[2])
    own_copy.start()
    meta_copy.start()
    left_copy.start()
    right[cells * n] = jnp.zeros(right.shape[1:], right.dtype)

    def cell_id(offset):
        target = lax.rem(me + offset, cells)
        return {"row": lax.div(target, col_count), "col": lax.rem(target, col_count)}

    def layer_id(offset):
        return {"layer": lax.rem(l + offset, layer_count)}

    barrier = pltpu.get_barrier_semaphore()
    for offset in range(1, cells):
        pl.semaphore_signal(barrier, inc=1, device_id=cell_id(offset), device_id_type=MESH)
    for offset in range(1, layer_count):
        pl.semaphore_signal(barrier, inc=1, device_id=layer_id(offset), device_id_type=MESH)
    pl.semaphore_wait(barrier, cells - 1 + layer_count - 1)
    own_copy.wait()

    step_rows = n // chunks
    sent = []

    def rows_of(cell, chunk):
        return pl.ds(cell * n + chunk * step_rows, step_rows)

    def copy_of(cell, chunk, way, device):
        return pltpu.make_async_remote_copy(
            src_ref=right.at[rows_of(cell, chunk)],
            dst_ref=right.at[rows_of(cell, chunk)],
            send_sem=send_sem.at[way, cell, chunk],
            recv_sem=recv_sem.at[cell, chunk],
            device_id=device,
            device_id_type=MESH,
        )

    ways = {
        "up": (0, c < col_count - 1, {"col": jnp.minimum(c + 1, col_count - 1)}),
        "down": (1, c > 0, {"col": jnp.maximum(c - 1, 0)}),
        "south": (2, r < row_count - 1, {"row": jnp.minimum(r + 1, row_count - 1)}),
        "north": (3, r > 0, {"row": jnp.maximum(r - 1, 0)}),
    }

    def send(cell, chunk, way, condition=True):
        index, exists, device = ways[way]
        wanted = jnp.logical_and(exists, condition)

        @pl.when(wanted)
        def _():
            copy_of(cell, chunk, index, device).start()

        sent.append((wanted, cell, chunk, index, device))

    def await_arrival(cell, chunk):
        copy_of(cell, chunk, 0, {"col": c}).wait_recv()

    for chunk in range(chunks):
        for way in ("up", "down", "south", "north"):
            send(me, chunk, way)

    meta_copy.wait()
    meta_copies = []
    for offset in range(1, cells):
        copy = pltpu.make_async_remote_copy(
            src_ref=meta_ref,
            dst_ref=meta_all.at[pl.ds(me * n, n)],
            send_sem=meta_send.at[offset],
            recv_sem=meta_recv.at[offset],
            device_id=cell_id(offset),
            device_id_type=MESH,
        )
        copy.start()
        meta_copies.append(copy)

    even = lax.rem(c, 2) == 0
    for step in range(1, col_count):
        for chunk in range(chunks):
            for origin, has, way, is_pair in (
                (c - step, c >= step, "up", jnp.logical_not(even)),
                (c + step, c + step < col_count, "down", even),
            ):
                origin = jnp.clip(origin, 0, col_count - 1)
                cell = r * col_count + origin

                @pl.when(has)
                def _():
                    await_arrival(cell, chunk)

                send(cell, chunk, way, has)
                across = has
                if is_balanced and step == 1 and chunk >= chunks // 2:
                    across = jnp.logical_and(has, jnp.logical_not(is_pair))
                send(cell, chunk, "south", across)
                send(cell, chunk, "north", across)

    if is_balanced:
        other = (1 - r) * col_count + c
        for chunk in range(chunks):
            await_arrival(other, chunk)
            if chunk >= chunks // 2:
                send(other, chunk, "up", even)
                send(other, chunk, "down", jnp.logical_not(even))
        for step in range(1, col_count):
            origin = (1 - r) * col_count + lax.rem(c + step, col_count)
            for chunk in range(chunks):
                await_arrival(origin, chunk)
    else:
        for step in range(1, row_count):
            for shift in range(col_count):
                for chunk in range(chunks):
                    for origin, has, way in (
                        (r - step, r >= step, "south"),
                        (r + step, r + step < row_count, "north"),
                    ):
                        origin = jnp.clip(origin, 0, row_count - 1)
                        cell = origin * col_count + lax.rem(c + shift, col_count)

                        @pl.when(has)
                        def _():
                            await_arrival(cell, chunk)

                        send(cell, chunk, way, has)

    for copy in meta_copies:
        copy.wait()
    table_copy = pltpu.make_async_copy(meta_all, meta_smem, local_sem.at[3])
    table_copy.start()
    table_copy.wait()
    left_copy.wait()

    def one_row(i, carry):
        targets = [
            columns_ref[i * width + l * per_layer * slots + s] for s in range(per_layer * slots)
        ]
        strips = []
        for a in range(width):
            k = columns_ref[i * width + a]
            inner = jnp.maximum(k, 0)
            pieces = []
            for s in range(per_layer * slots):
                group = s // slots
                row_index = jnp.int32(cells * n)
                slot_index = jnp.int32(0)
                is_live = (k >= 0) & (targets[s] >= 0)
                for t in range(slots):
                    hit = (meta_smem[inner, 0, group * slots + t] == targets[s]) & is_live
                    row_index = jnp.where(hit, inner, row_index)
                    slot_index = jnp.where(hit, t, slot_index)
                pieces.append(right[row_index, group, slot_index])
            strips.append(jnp.concatenate(pieces, axis=1))
        rights = jnp.concatenate(strips, axis=0)
        lefts = jnp.concatenate(
            [left[i, a // slots, a % slots] for a in range(width)], axis=1
        )
        total = jnp.dot(lefts, rights, preferred_element_type=jnp.float32).astype(stage.dtype)
        for q in range(layer_count):
            for s in range(per_layer * slots):
                stage[q, i, s // slots, s % slots] = total[
                    q * quarter:(q + 1) * quarter, s * tile:(s + 1) * tile
                ]
        return carry

    out_rows = n // out_chunks

    def out_copies(chunk):
        rows = pl.ds(chunk * out_rows, out_rows)
        copies = []
        for offset in range(layer_count):
            q = lax.rem(l + offset, layer_count)
            if offset == 0:
                copies.append(pltpu.make_async_copy(
                    stage.at[q, rows], out_ref.at[rows, own_groups], out_send.at[0, chunk]
                ))
            else:
                copies.append(pltpu.make_async_remote_copy(
                    src_ref=stage.at[q, rows],
                    dst_ref=out_ref.at[rows, own_groups],
                    send_sem=out_send.at[offset, chunk],
                    recv_sem=out_recv.at[offset, chunk],
                    device_id=layer_id(offset),
                    device_id_type=MESH,
                ))
        return copies

    all_out = []
    for chunk in range(out_chunks + 1):
        if chunk < out_chunks:
            lax.fori_loop(chunk * out_rows, (chunk + 1) * out_rows, one_row, 0)
        if chunk > 0:
            copies = out_copies(chunk - 1)
            for copy in copies[1:] + copies[:1]:
                copy.start()
            all_out.extend(copies)

    for wanted, cell, chunk, index, device in sent:
        @pl.when(wanted)
        def _():
            copy_of(cell, chunk, index, device).wait_send()

    for copy in all_out:
        copy.wait()


def on_device(density_tiles, tile_columns):
    row_count = lax.axis_size("row")
    col_count = lax.axis_size("col")
    layer_count = lax.axis_size("layer")
    n, group_count, slots, tile, _ = density_tiles.shape
    cells = row_count * col_count
    per_layer = group_count // layer_count
    quarter = tile // layer_count
    kept = per_layer * slots
    chunks = divisor(n, 4)
    out_chunks = divisor(n, 4)
    is_balanced = row_count == 2 and col_count % 2 == 0 and chunks % 2 == 0
    own = lax.dynamic_slice_in_dim(tile_columns, lax.axis_index("layer") * per_layer, per_layer, 1)
    meta = jnp.pad(own.reshape(n, 1, kept), ((0, 0), (0, 0), (0, 128 - kept)), constant_values=-1)
    dtype = density_tiles.dtype
    sizes = (row_count, col_count, layer_count, chunks, out_chunks, is_balanced)
    return pl.pallas_call(
        functools.partial(kernel, sizes),
        out_shape=jax.ShapeDtypeStruct((n, group_count, slots, quarter, tile), dtype),
        in_specs=[
            pl.BlockSpec(memory_space=pltpu.SMEM),
            pl.BlockSpec(memory_space=pl.ANY),
            pl.BlockSpec(memory_space=pltpu.VMEM),
        ],
        out_specs=pl.BlockSpec(memory_space=pl.ANY),
        scratch_shapes=[
            pltpu.VMEM(density_tiles.shape, dtype),
            pltpu.VMEM((cells * n + 1, per_layer, slots, tile, tile), dtype),
            pltpu.VMEM((cells * n, 1, 128), jnp.int32),
            pltpu.SMEM((cells * n, 1, 128), jnp.int32),
            pltpu.VMEM((layer_count, n, per_layer, slots, quarter, tile), dtype),
            pltpu.SemaphoreType.DMA((4,)),
            pltpu.SemaphoreType.DMA((cells,)),
            pltpu.SemaphoreType.DMA((cells,)),
            pltpu.SemaphoreType.DMA((4, cells, chunks)),
            pltpu.SemaphoreType.DMA((cells, chunks)),
            pltpu.SemaphoreType.DMA((layer_count, out_chunks)),
            pltpu.SemaphoreType.DMA((layer_count, out_chunks)),
        ],
        compiler_params=pltpu.CompilerParams(
            collective_id=0, has_side_effects=True, vmem_limit_bytes=60 * 1024 * 1024
        ),
    )(tile_columns.reshape(-1), density_tiles, meta)


def paired_kernel(
    sizes, tiles_ref, meta_ref, out_ref,
    left, right, meta_all, meta_smem, stage,
    local_sem, meta_send, meta_recv, send_sem, recv_sem, left_send, left_recv, out_send, out_recv,
):
    col_count, layer_count, chunks, out_chunks = sizes
    n, group_count, slots, tile, _ = tiles_ref.shape
    cells = 2 * col_count
    per_layer = group_count // layer_count
    quarter = tile // layer_count
    width = group_count * slots
    r, c, l = lax.axis_index("row"), lax.axis_index("col"), lax.axis_index("layer")
    high, k = lax.div(l, 2), lax.rem(l, 2)
    me = r * col_count + c
    base = k * col_count + c
    is_home = k == r
    is_guest = jnp.logical_not(is_home)
    group = 2 * high + r
    own_groups = pl.ds(group * per_layer, per_layer)
    other_groups = pl.ds((2 * high + 1 - r) * per_layer, per_layer)
    facing = {"row": 1 - r}
    partner = {"layer": 2 * high + 1 - k}

    own_copy = pltpu.make_async_copy(
        tiles_ref.at[:, own_groups], right.at[pl.ds(me * n, n)], local_sem.at[0]
    )
    left_copy = pltpu.make_async_copy(tiles_ref, left, local_sem.at[1])
    meta_copy = pltpu.make_async_copy(meta_ref, meta_all.at[pl.ds(me * n, n)], local_sem.at[2])
    own_copy.start()
    meta_copy.start()

    @pl.when(is_home)
    def _():
        left_copy.start()

    right[cells * n] = jnp.zeros(right.shape[1:], right.dtype)

    def cell_id(offset):
        target = lax.rem(me + offset, cells)
        return {"row": lax.div(target, col_count), "col": lax.rem(target, col_count)}

    barrier = pltpu.get_barrier_semaphore()
    for offset in range(1, cells):
        pl.semaphore_signal(barrier, inc=1, device_id=cell_id(offset), device_id_type=MESH)
    for offset in range(1, layer_count):
        for row in (r, 1 - r):
            pl.semaphore_signal(
                barrier,
                inc=1,
                device_id={"row": row, "layer": lax.rem(l + offset, layer_count)},
                device_id_type=MESH,
            )
    pl.semaphore_wait(barrier, cells - 1 + 2 * (layer_count - 1))

    step_rows = n // chunks
    sent = []

    def rows_of(cell, chunk):
        return pl.ds(cell * n + chunk * step_rows, step_rows)

    def copy_of(cell, chunk, way, device):
        source = right.at[rows_of(cell, chunk)]
        if way == 3:
            source = tiles_ref.at[pl.ds(chunk * step_rows, step_rows), other_groups]
        return pltpu.make_async_remote_copy(
            src_ref=source,
            dst_ref=right.at[rows_of(cell, chunk)],
            send_sem=send_sem.at[way, cell, chunk],
            recv_sem=recv_sem.at[cell, chunk],
            device_id=device,
            device_id_type=MESH,
        )

    ways = {
        "up": (0, c < col_count - 1, {"col": jnp.minimum(c + 1, col_count - 1)}),
        "down": (1, c > 0, {"col": jnp.maximum(c - 1, 0)}),
        "partner": (2, True, partner),
        "facing": (3, True, facing),
    }

    def send(cell, chunk, way, condition):
        index, exists, device = ways[way]
        wanted = jnp.logical_and(exists, condition)

        @pl.when(wanted)
        def _():
            copy_of(cell, chunk, index, device).start()

        sent.append((wanted, cell, chunk, index, device))

    def await_arrival(cell, chunk, condition):
        @pl.when(condition)
        def _():
            copy_of(cell, chunk, 2, partner).wait_recv()

    for chunk in range(chunks):
        send(me, chunk, "facing", is_home)
    own_copy.wait()
    for chunk in range(chunks):
        for way in ("up", "down"):
            send(me, chunk, way, is_home)
    left_out = pltpu.make_async_remote_copy(
        src_ref=tiles_ref, dst_ref=left, send_sem=left_send, recv_sem=left_recv,
        device_id=facing, device_id_type=MESH,
    )

    meta_copy.wait()
    meta_copies = []
    for offset in range(1, cells):
        copy = pltpu.make_async_remote_copy(
            src_ref=meta_ref,
            dst_ref=meta_all.at[pl.ds(me * n, n)],
            send_sem=meta_send.at[offset],
            recv_sem=meta_recv.at[offset],
            device_id=cell_id(offset),
            device_id_type=MESH,
        )
        copy.start()
        meta_copies.append(copy)

    @pl.when(is_home)
    def _():
        left_out.start()

    for chunk in range(chunks):
        await_arrival(base, chunk, is_guest)
        for way in ("up", "down", "partner"):
            send(base, chunk, way, is_guest)

    for step in range(1, col_count):
        for chunk in range(chunks):
            for origin, has, way in (
                (c - step, c >= step, "up"),
                (c + step, c + step < col_count, "down"),
            ):
                cell = k * col_count + jnp.clip(origin, 0, col_count - 1)
                await_arrival(cell, chunk, has)
                send(cell, chunk, way, has)
                send(cell, chunk, "partner", has)

    for chunk in range(chunks):
        await_arrival((1 - k) * col_count + c, chunk, is_home)
    for step in range(1, col_count):
        cell = (1 - k) * col_count + lax.rem(c + step, col_count)
        for chunk in range(chunks):
            await_arrival(cell, chunk, True)

    for copy in meta_copies:
        copy.wait()
    table_copy = pltpu.make_async_copy(meta_all, meta_smem, local_sem.at[3])
    table_copy.start()
    table_copy.wait()

    @pl.when(is_home)
    def _():
        left_copy.wait()

    @pl.when(is_guest)
    def _():
        left_out.wait_recv()

    first = group * per_layer * slots

    def one_row(i, carry):
        block_row = base * n + i
        targets = [meta_smem[block_row, 0, first + s] for s in range(per_layer * slots)]
        strips = []
        for a in range(width):
            column = meta_smem[block_row, 0, a]
            inner = jnp.maximum(column, 0)
            pieces = []
            for s in range(per_layer * slots):
                part = s // slots
                row_index = jnp.int32(cells * n)
                slot_index = jnp.int32(0)
                is_live = (column >= 0) & (targets[s] >= 0)
                for t in range(slots):
                    hit = (meta_smem[inner, 0, first + part * slots + t] == targets[s]) & is_live
                    row_index = jnp.where(hit, inner, row_index)
                    slot_index = jnp.where(hit, t, slot_index)
                pieces.append(right[row_index, part, slot_index])
            strips.append(jnp.concatenate(pieces, axis=1))
        rights = jnp.concatenate(strips, axis=0)
        lefts = jnp.concatenate(
            [left[i, a // slots, a % slots] for a in range(width)], axis=1
        )
        total = jnp.dot(lefts, rights, preferred_element_type=jnp.float32).astype(stage.dtype)
        for q in range(layer_count):
            for s in range(per_layer * slots):
                stage[q, i, s // slots, s % slots] = total[
                    q * quarter:(q + 1) * quarter, s * tile:(s + 1) * tile
                ]
        return carry

    out_rows = n // out_chunks

    def out_copy(chunk, q, source):
        rows = pl.ds(chunk * out_rows, out_rows)
        return pltpu.make_async_remote_copy(
            src_ref=stage.at[q, rows],
            dst_ref=out_ref.at[rows, pl.ds(source * per_layer, per_layer)],
            send_sem=out_send.at[q, chunk],
            recv_sem=out_recv.at[source, chunk],
            device_id={"row": k, "layer": q},
            device_id_type=MESH,
        )

    def kept_copy(chunk):
        rows = pl.ds(chunk * out_rows, out_rows)
        return pltpu.make_async_copy(
            stage.at[l, rows], out_ref.at[rows, own_groups], out_send.at[l, chunk]
        )

    for chunk in range(out_chunks + 1):
        if chunk < out_chunks:
            lax.fori_loop(chunk * out_rows, (chunk + 1) * out_rows, one_row, 0)
        if chunk > 0:
            for offset in range(layer_count - 1, -1, -1):
                q = lax.rem(l + offset, layer_count)
                if offset:
                    out_copy(chunk - 1, q, group).start()
                else:
                    @pl.when(is_guest)
                    def _():
                        out_copy(chunk - 1, q, group).start()

                    @pl.when(is_home)
                    def _():
                        kept_copy(chunk - 1).start()

    for wanted, cell, chunk, index, device in sent:
        @pl.when(wanted)
        def _():
            copy_of(cell, chunk, index, device).wait_send()

    @pl.when(is_home)
    def _():
        left_out.wait_send()

    for chunk in range(out_chunks):
        for offset in range(layer_count):
            q = lax.rem(l + offset, layer_count)
            source = lax.rem(group + offset, layer_count)
            if offset:
                out_copy(chunk, q, source).wait()
            else:
                @pl.when(is_guest)
                def _():
                    out_copy(chunk, q, source).wait()

                @pl.when(is_home)
                def _():
                    kept_copy(chunk).wait()


def on_device_paired(density_tiles, tile_columns):
    col_count = lax.axis_size("col")
    layer_count = lax.axis_size("layer")
    n, group_count, slots, tile, _ = density_tiles.shape
    cells = 2 * col_count
    per_layer = group_count // layer_count
    quarter = tile // layer_count
    width = group_count * slots
    chunks = divisor(n, 2)
    out_chunks = divisor(n, 12)
    lanes = -(-width // 128) * 128
    meta = jnp.pad(
        tile_columns.reshape(n, 1, width), ((0, 0), (0, 0), (0, lanes - width)), constant_values=-1
    )
    dtype = density_tiles.dtype
    return pl.pallas_call(
        functools.partial(paired_kernel, (col_count, layer_count, chunks, out_chunks)),
        out_shape=jax.ShapeDtypeStruct((n, group_count, slots, quarter, tile), dtype),
        in_specs=[
            pl.BlockSpec(memory_space=pl.ANY),
            pl.BlockSpec(memory_space=pltpu.VMEM),
        ],
        out_specs=pl.BlockSpec(memory_space=pl.ANY),
        scratch_shapes=[
            pltpu.VMEM(density_tiles.shape, dtype),
            pltpu.VMEM((cells * n + 1, per_layer, slots, tile, tile), dtype),
            pltpu.VMEM((cells * n, 1, lanes), jnp.int32),
            pltpu.SMEM((cells * n, 1, lanes), jnp.int32),
            pltpu.VMEM((layer_count, n, per_layer, slots, quarter, tile), dtype),
            pltpu.SemaphoreType.DMA((4,)),
            pltpu.SemaphoreType.DMA((cells,)),
            pltpu.SemaphoreType.DMA((cells,)),
            pltpu.SemaphoreType.DMA((4, cells, chunks)),
            pltpu.SemaphoreType.DMA((cells, chunks)),
            pltpu.SemaphoreType.DMA,
            pltpu.SemaphoreType.DMA,
            pltpu.SemaphoreType.DMA((layer_count, out_chunks)),
            pltpu.SemaphoreType.DMA((layer_count, out_chunks)),
        ],
        compiler_params=pltpu.CompilerParams(
            collective_id=1, has_side_effects=True, vmem_limit_bytes=60 * 1024 * 1024
        ),
    )(density_tiles, meta)


def sparse_kernel(
    sizes, tiles_ref, columns_ref, out_ref, flag_ref,
    left, diag, extra, lent, borrowed, pack, arrived, stage, total, needs, ranks, meta_own, meta_all, meta_smem,
    send_list, send_smem, row_list, row_smem, flag_all,
    local_sem, meta_send, meta_recv, flag_send, flag_recv,
    main_send, main_recv, side_send, side_recv, lent_sem, pack_send, pack_recv, extra_send, extra_recv, out_sem,
):
    row_count, col_count, layer_count, group_count, per_row, padded = sizes
    n, width, tile, _ = tiles_ref.shape
    per_lent, per_plane, pool = lent.shape[0], pack.shape[1], extra.shape[0]
    cells = row_count * col_count
    quarter = tile // layer_count
    entries = padded * width
    span = -(-(cells * n) // 128) * 128
    lists = -(-per_row // 8) * 8
    r, c, l = lax.axis_index("row"), lax.axis_index("col"), lax.axis_index("layer")
    x, k = lax.div(l, 2), lax.rem(l, 2)
    facing_layer = 2 * (1 - x) + k
    me = r * col_count + c
    opposite = (1 - r) * col_count + c
    own_slot = lax.div(me * n * group_count, cells * n) * (width // group_count)
    partner = {"layer": 2 * x + 1 - k}
    facing = {"layer": facing_layer}

    diag_copy = pltpu.make_async_copy(
        tiles_ref.at[:, own_slot], diag.at[pl.ds(me * n, n)], local_sem.at[1]
    )
    left_copy = pltpu.make_async_copy(tiles_ref, left, local_sem.at[2])
    table_copy = pltpu.make_async_copy(meta_own, meta_smem, local_sem.at[3])
    diag_copy.start()
    left_copy.start()
    meta_own[...] = jnp.full(meta_own.shape, -1, jnp.int32)
    meta_own[:, 0:n] = columns_ref[...]
    meta_all[me] = meta_own[...]

    def cell_id(cell):
        return {"row": lax.div(cell, col_count), "col": lax.rem(cell, col_count)}

    def other_cell(offset):
        return lax.rem(me + offset, cells)

    barrier = pltpu.get_barrier_semaphore()
    for offset in range(1, cells):
        pl.semaphore_signal(
            barrier, inc=1, device_id=cell_id(other_cell(offset)), device_id_type=MESH
        )
    for device in (partner, facing):
        pl.semaphore_signal(barrier, inc=1, device_id=device, device_id_type=MESH)
    pl.semaphore_wait(barrier, cells - 1 + 2)

    sent = []

    def remote(source, target, send, recv, device):
        return pltpu.make_async_remote_copy(
            src_ref=source, dst_ref=target, send_sem=send, recv_sem=recv,
            device_id=device, device_id_type=MESH,
        )

    def launch(copy, condition=True):
        if condition is True:
            copy.start()
        else:
            @pl.when(condition)
            def _():
                copy.start()
        sent.append((copy, condition))

    def await_recv(copy, condition=True):
        if condition is True:
            copy.wait_recv()
        else:
            @pl.when(condition)
            def _():
                copy.wait_recv()

    def part(cell, q):
        return diag.at[pl.ds(cell * n, n), pl.ds(q * quarter, quarter)]

    up = {"col": jnp.minimum(c + 1, col_count - 1)}
    down = {"col": jnp.maximum(c - 1, 0)}
    across = {"row": 1 - r}

    def line_copy(cell, way, wide=0):
        device = (up, down, across)[way]
        piece = part(cell, facing_layer if wide else l)
        return remote(
            piece, piece, main_send.at[wide, way, cell], main_recv.at[wide, cell], device
        )

    def side_copy(cell, way):
        device = (partner, facing, partner)[way]
        piece = part(cell, facing_layer if way == 2 else l)
        return remote(piece, piece, side_send.at[way, cell], side_recv.at[way, cell], device)

    meta_copies = []
    for offset in range(1, cells):
        copy = remote(
            meta_own, meta_all.at[me], meta_send.at[offset], meta_recv.at[offset],
            cell_id(other_cell(offset)),
        )
        copy.start()
        meta_copies.append(copy)
    diag_copy.wait()
    has_up, has_down = c < col_count - 1, c > 0
    launch(line_copy(me, 0), has_up)
    launch(line_copy(me, 1), has_down)
    launch(line_copy(me, 2))
    table_copy.start()
    for copy in meta_copies:
        copy.wait_recv()

    small_row = lax.broadcasted_iota(jnp.int32, (padded, 128), 0)
    small_lane = lax.broadcasted_iota(jnp.int32, (padded, 128), 1)
    wide_row = lax.broadcasted_iota(jnp.int32, (padded, span), 0)
    wide_lane = lax.broadcasted_iota(jnp.int32, (padded, span), 1)
    tall_row = lax.broadcasted_iota(jnp.int32, (span, 128), 0)
    entry_row = lax.broadcasted_iota(jnp.int32, (entries, 128), 0)
    entry_lane = lax.broadcasted_iota(jnp.int32, (entries, 128), 1).astype(jnp.float32)
    before = (
        lax.broadcasted_iota(jnp.int32, (entries, entries), 0)
        > lax.broadcasted_iota(jnp.int32, (entries, entries), 1)
    ).astype(jnp.float32).astype(jnp.bfloat16)
    ones = jnp.ones((128, 128), jnp.bfloat16)

    def dot(a, b):
        return jnp.dot(a, b, preferred_element_type=jnp.float32)

    def chosen(cell):
        columns = jnp.transpose(meta_all[cell])[0:padded]
        pieces = []
        for b in range(width):
            hit = (columns[:, b:b + 1] == wide_lane) & (wide_lane != wide_row + cell * n)
            pieces.append(jnp.where(hit, 1.0, 0.0))
        return jnp.concatenate(pieces, axis=0).astype(jnp.bfloat16)

    def listing(cell):
        rows = meta_all[cell]
        weight = jnp.zeros((span, 128), jnp.float32)
        for a in range(width):
            weight = jnp.where(rows[a:a + 1] == tall_row, a + 1.0, weight)
        return weight.astype(jnp.bfloat16)

    def inner_listing(source, cell):
        rows = meta_all[cell]
        weight = jnp.zeros((padded, 128), jnp.float32)
        for a in range(width):
            weight = jnp.where(rows[a:a + 1] == small_row + source * n, a + 1.0, weight)
        weight = jnp.where(small_row + source * n == small_lane + cell * n, 0.0, weight)
        return jnp.concatenate([weight] * width, axis=0)

    def matches(picked, listed, inner):
        goal = dot(picked, listed)
        hit = jnp.where((goal > 0) & (inner > 0), 1.0, 0.0)
        needed = jnp.where(dot(hit.astype(jnp.bfloat16), ones) > 0, 1.0, 0.0)
        return goal, hit, needed

    def rank_of(needed):
        return dot(before, needed.astype(jnp.bfloat16))

    def count_of(needed):
        return jnp.sum(needed, axis=0, keepdims=True)

    def picks_of(needed, rank, value):
        chosen_values = jnp.where((rank == entry_lane) & (needed > 0), value, 0.0)
        return jnp.sum(chosen_values, axis=0, keepdims=True)

    slot_value = (
        lax.rem(entry_row, padded) * width + lax.div(entry_row, padded)
    ).astype(jnp.float32)
    mine, theirs = chosen(me), chosen(opposite)
    none = jnp.zeros((entries, 128), jnp.float32)
    my_rows = pl.ds(pl.multiple_of(l * quarter, quarter), quarter)

    def lent_step(at, wanted):
        cell = (1 - r) * col_count + at
        return jnp.maximum(wanted, matches(mine, listing(cell), inner_listing(me, cell))[2])

    wanted = lax.fori_loop(0, col_count, lent_step, none, unroll=True)
    send_list[0:1] = picks_of(wanted, rank_of(wanted), slot_value).astype(jnp.int32)
    lent_most = count_of(wanted)
    lent_list = pltpu.make_async_copy(send_list.at[0], send_smem.at[0], local_sem.at[4])
    lent_list.start()
    lent_list.wait()
    left_copy.wait()

    def own_piece(code):
        code = jnp.clip(code, 0, n * width - 1)
        return left[lax.div(code, width), lax.rem(code, width), my_rows]

    def lent_pack(m, carry):
        lent[m] = own_piece(send_smem[0, m])
        return carry

    lax.fori_loop(0, per_lent, lent_pack, 0, unroll=8)
    lent_copy = remote(lent, borrowed, lent_sem.at[0], lent_sem.at[1], across)
    launch(lent_copy)

    def share(cell, condition=True, wide=False):
        launch(side_copy(cell, 0), condition)
        if not wide:
            launch(side_copy(cell, 1), condition)

    def take_line(cell, has, way, wide):
        await_recv(line_copy(cell, way), has)
        launch(line_copy(cell, way), jnp.logical_and(has, has_up if way == 0 else has_down))
        share(cell, has, wide)
        launch(line_copy(cell, 2), has)

    line, beyond = [], []
    for step in range(1, col_count):
        for origin, has, way in ((c - step, c >= step, 0), (c + step, c + step < col_count, 1)):
            origin = jnp.clip(origin, 0, col_count - 1)
            line.append((r * col_count + origin, has, way, step == 1))
            beyond.append(((1 - r) * col_count + origin, has))

    for entry in line[:2]:
        take_line(*entry)

    for entry in line[2:4]:
        take_line(*entry)
    launch(line_copy(me, 2, 1))

    def plane_step(at, wanted):
        cell = r * col_count + at
        listed = listing(cell)
        own = matches(mine, listed, inner_listing(me, cell))[2]
        send_list[pl.ds(8 + at, 1)] = picks_of(own, rank_of(own), slot_value).astype(jnp.int32)
        their = matches(theirs, listed, inner_listing(opposite, cell))[2]
        needs[at] = their
        ranks[at] = rank_of(their) + count_of(own)
        return jnp.maximum(wanted, their)

    wanted = lax.fori_loop(0, col_count, plane_step, none, unroll=True)
    borrowed_value = rank_of(wanted) + float(n * width)

    def plane_finish(at, carry):
        picks = picks_of(needs[at], ranks[at], borrowed_value).astype(jnp.int32)
        send_list[pl.ds(8 + at, 1)] += picks
        return carry

    lax.fori_loop(0, col_count, plane_finish, 0, unroll=True)
    rows_used = send_list.shape[0] - 8
    plane_list = pltpu.make_async_copy(
        send_list.at[pl.ds(8, rows_used)], send_smem.at[pl.ds(8, rows_used)], local_sem.at[4]
    )
    plane_list.start()

    await_recv(line_copy(opposite, 2))
    share(opposite, True, True)
    plane_list.wait()
    await_recv(lent_copy)

    def plane_piece(at, m):
        code = send_smem[8 + at, m]
        loaned = borrowed[jnp.clip(code - n * width, 0, per_lent - 1)]
        return jnp.where(code < n * width, own_piece(code), loaned)

    def plane_pack(m, carry):
        for offset in range(col_count):
            at = lax.rem(c + offset, col_count)
            if offset:
                pack[offset, m] = plane_piece(at, m)
            else:
                arrived[c, m] = plane_piece(at, m)
        return carry

    lax.fori_loop(0, per_plane, plane_pack, 0, unroll=4)

    def pack_copy(offset, origin):
        return remote(
            pack.at[offset], arrived.at[origin], pack_send.at[offset], pack_recv.at[origin],
            {"col": lax.rem(c + offset, col_count)},
        )

    for offset in sorted(range(1, col_count), key=lambda o: abs(2 * o - col_count)):
        launch(pack_copy(offset, c))

    def take_beyond(cell, has):
        await_recv(line_copy(cell, 2), has)
        share(cell, has)

    for entry in line[4:]:
        take_line(*entry)
    for entry in beyond[:2]:
        take_beyond(*entry)

    listed = listing(me)
    list_row = lax.broadcasted_iota(jnp.int32, (lists + 8, 128), 0)

    def row_step(at, carry):
        held, running, pooled, in_plane, most = carry
        plane, far = lax.div(at, 2), lax.rem(at, 2)
        source = jnp.where(far == 0, r, 1 - r) * col_count + plane
        in_plane = jnp.where(far == 0, 0.0, in_plane)
        inner = inner_listing(source, me)
        goal, hit, needed = matches(chosen(source), listed, inner)
        rank = rank_of(needed)
        place = dot(before, hit.astype(jnp.bfloat16)) + running
        value = (((rank + pooled) * 16.0 + (inner - 1.0)) * 16.0 + goal) * hit
        for q in range(per_row):
            line_sum = jnp.sum(jnp.where(place == float(q), value, 0.0), axis=0, keepdims=True)
            held = held + jnp.where(list_row == q, line_sum, 0.0)
        spot = rank + in_plane + (plane * per_plane).astype(jnp.float32)
        held = held + jnp.where(list_row == lists, picks_of(needed, rank + pooled, spot), 0.0)
        count = count_of(needed)
        in_plane = in_plane + count
        return held, running + count_of(hit), pooled + count, in_plane, jnp.maximum(most, in_plane)

    zero = jnp.zeros((1, 128), jnp.float32)
    held, running, pooled, _, most = lax.fori_loop(
        0, cells, row_step, (jnp.zeros((lists + 8, 128), jnp.float32), zero, zero, zero, zero),
        unroll=2,
    )
    row_list[...] = held.astype(jnp.int32)
    over = (most > per_plane) | (running > per_row) | (pooled > pool) | (lent_most > per_lent)
    flag_all[me] = jnp.broadcast_to(jnp.max(jnp.where(over, 1, 0)), (8, 128))
    row_copy = pltpu.make_async_copy(row_list, row_smem, local_sem.at[5])
    row_copy.start()
    flag_copies = []
    for offset in range(1, cells):
        copy = remote(
            flag_all.at[me], flag_all.at[me], flag_send.at[offset], flag_recv.at[offset],
            cell_id(other_cell(offset)),
        )
        copy.start()
        flag_copies.append(copy)

    def pass_on(cell, condition=True):
        await_recv(side_copy(cell, 1), condition)
        launch(side_copy(cell, 2), condition)

    def take_wide(cell, has, way, wide):
        await_recv(line_copy(cell, way, 1), has)
        launch(side_copy(cell, 2), has)

    for entry in beyond[2:]:
        take_beyond(*entry)
    launch(line_copy(me, 0, 1), has_up)
    launch(line_copy(me, 1, 1), has_down)
    row_copy.wait()
    for offset in range(1, col_count):
        await_recv(pack_copy(offset, lax.rem(c + offset, col_count)))

    def pool_pack(m, carry):
        code = jnp.clip(row_smem[lists, m], 0, col_count * per_plane - 1)
        extra[m, my_rows] = arrived[lax.div(code, per_plane), lax.rem(code, per_plane)]
        return carry

    lax.fori_loop(0, pool, pool_pack, 0, unroll=8)

    def extra_copy(way, half):
        device = (partner, facing, partner)[way]
        piece = extra.at[
            pl.ds(half * (pool // 2), pool // 2),
            pl.ds((facing_layer if way == 2 else l) * quarter, quarter),
        ]
        return remote(piece, piece, extra_send.at[way, half], extra_recv.at[way, half], device)

    for half in range(2):
        launch(extra_copy(1, half))
    for half in range(2):
        launch(extra_copy(0, half))
    for entry in line[:2]:
        take_wide(*entry)
    await_recv(line_copy(opposite, 2, 1))
    launch(side_copy(opposite, 2))
    for cell, has, _, _ in line[2:]:
        pass_on(cell, has)
    for cell, has in beyond:
        pass_on(cell, has)
    for offset in range(1, cells):
        await_recv(side_copy(other_cell(offset), 0))
        await_recv(side_copy(other_cell(offset), 2))
    table_copy.wait()

    def near_row(i, carry):
        own = left[i, own_slot, my_rows]
        pieces = []
        for t in range(width):
            column = meta_smem[t, i]
            lower = diag[jnp.maximum(column, 0)]
            own_left = left[i, t, my_rows]
            own_left = jnp.where(own_slot == t, jnp.zeros_like(own_left), own_left)
            value = dot(
                jnp.concatenate([own, own_left], axis=1),
                jnp.concatenate([left[i, t], lower], axis=0),
            )
            pieces.append(jnp.where(column >= 0, value, 0.0))
        total[i] = jnp.concatenate(pieces, axis=0)
        return carry

    lax.fori_loop(0, n, near_row, 0, unroll=2)
    for half in range(2):
        await_recv(extra_copy(1, half))
        launch(extra_copy(2, half))
    for half in range(2):
        await_recv(extra_copy(0, half))
        await_recv(extra_copy(2, half))

    def far_row(i, carry):
        values = [total[i, t * quarter:(t + 1) * quarter] for t in range(width)]
        for q in range(per_row):
            code = jnp.clip(row_smem[q, i], 0, pool * 256 - 1)
            goal = lax.rem(code, 16)
            at = jnp.minimum(lax.rem(lax.div(code, 16), 16), width - 1)
            value = dot(left[i, at, my_rows], extra[lax.div(code, 256)])
            values = [v + jnp.where(goal == t + 1, value, 0.0) for t, v in enumerate(values)]
        for t in range(width):
            stage[i, t] = values[t].astype(stage.dtype)
        return carry

    out_copies = []
    for chunk in range(n // 8):
        lax.fori_loop(chunk * 8, chunk * 8 + 8, far_row, 0, unroll=8)
        rows = pl.ds(chunk * 8, 8)
        out_copies.append(pltpu.make_async_copy(
            stage.at[rows], out_ref.at[rows], out_sem.at[chunk]
        ))
        out_copies[-1].start()
    for copy in flag_copies:
        copy.wait_recv()
    flag_ref[0, 0] = jnp.max(flag_all[...])
    for copy in meta_copies + flag_copies:
        copy.wait_send()
    for copy, condition in sent:
        if condition is True:
            copy.wait_send()
        else:
            @pl.when(condition)
            def _():
                copy.wait_send()
    for copy in out_copies:
        copy.wait()


def on_device_sparse(density_tiles, tile_columns):
    row_count = lax.axis_size("row")
    col_count = lax.axis_size("col")
    layer_count = lax.axis_size("layer")
    n, group_count, slots, tile, _ = density_tiles.shape
    cells = row_count * col_count
    quarter = tile // layer_count
    width = group_count * slots
    per_lent, per_plane, pool, per_row = 32, 24, 56, 8
    padded = -(-n // 32) * 32
    dtype = density_tiles.dtype
    sizes = (row_count, col_count, layer_count, group_count, per_row, padded)
    lists = -(-per_row // 8) * 8
    planes = -(-col_count // 8) * 8
    out, flag = pl.pallas_call(
        functools.partial(sparse_kernel, sizes),
        out_shape=(
            jax.ShapeDtypeStruct((n, width, quarter, tile), dtype),
            jax.ShapeDtypeStruct((1, 1), jnp.int32),
        ),
        in_specs=[
            pl.BlockSpec(memory_space=pl.ANY),
            pl.BlockSpec(memory_space=pltpu.VMEM),
        ],
        out_specs=(
            pl.BlockSpec(memory_space=pl.ANY),
            pl.BlockSpec(memory_space=pltpu.SMEM),
        ),
        scratch_shapes=[
            pltpu.VMEM((n, width, tile, tile), dtype),
            pltpu.VMEM((cells * n, tile, tile), dtype),
            pltpu.VMEM((pool, tile, tile), dtype),
            pltpu.VMEM((per_lent, quarter, tile), dtype),
            pltpu.VMEM((per_lent, quarter, tile), dtype),
            pltpu.VMEM((col_count, per_plane, quarter, tile), dtype),
            pltpu.VMEM((col_count, per_plane, quarter, tile), dtype),
            pltpu.VMEM((n, width, quarter, tile), dtype),
            pltpu.VMEM((n, width * quarter, tile), jnp.float32),
            pltpu.VMEM((col_count, padded * width, 128), jnp.float32),
            pltpu.VMEM((col_count, padded * width, 128), jnp.float32),
            pltpu.VMEM((width, 128), jnp.int32),
            pltpu.VMEM((cells, width, 128), jnp.int32),
            pltpu.SMEM((width, 128), jnp.int32),
            pltpu.VMEM((8 + planes, 128), jnp.int32),
            pltpu.SMEM((8 + planes, 128), jnp.int32),
            pltpu.VMEM((lists + 8, 128), jnp.int32),
            pltpu.SMEM((lists + 8, 128), jnp.int32),
            pltpu.VMEM((cells, 8, 128), jnp.int32),
            pltpu.SemaphoreType.DMA((7,)),
            pltpu.SemaphoreType.DMA((cells,)),
            pltpu.SemaphoreType.DMA((cells,)),
            pltpu.SemaphoreType.DMA((cells,)),
            pltpu.SemaphoreType.DMA((cells,)),
            pltpu.SemaphoreType.DMA((2, 3, cells)),
            pltpu.SemaphoreType.DMA((2, cells)),
            pltpu.SemaphoreType.DMA((3, cells)),
            pltpu.SemaphoreType.DMA((3, cells)),
            pltpu.SemaphoreType.DMA((2,)),
            pltpu.SemaphoreType.DMA((col_count,)),
            pltpu.SemaphoreType.DMA((col_count,)),
            pltpu.SemaphoreType.DMA((3, 2)),
            pltpu.SemaphoreType.DMA((3, 2)),
            pltpu.SemaphoreType.DMA((n // 8,)),
        ],
        compiler_params=pltpu.CompilerParams(
            collective_id=2, has_side_effects=True, vmem_limit_bytes=60 * 1024 * 1024
        ),
    )(density_tiles.reshape(n, width, tile, tile), tile_columns.reshape(n, width).T)
    out = out.reshape(n, group_count, slots, quarter, tile)
    return lax.cond(
        flag[0, 0] > 0,
        lambda: on_device_paired(density_tiles, tile_columns),
        lambda: out,
    )


def solution(mesh):
    paired = mesh.shape["row"] == 2 and mesh.shape["layer"] % 2 == 0
    four = paired and mesh.shape["layer"] == 4

    def on_each(density_tiles, tile_columns):
        n, group_count, slots, tile, _ = density_tiles.shape
        block_count = n * mesh.shape["row"] * mesh.shape["col"]
        fits = four and n % 8 == 0 and n <= 128 and group_count * slots <= 15 and slots > 0
        fits = fits and (block_count // group_count) % n == 0 and tile % 128 == 0
        fits = fits and mesh.shape["col"] <= 16
        if fits:
            return on_device_sparse(density_tiles, tile_columns)
        return (on_device_paired if paired else on_device)(density_tiles, tile_columns)

    in_specs = (P(("row", "col"), None, None, None, None), P(("row", "col"), None, None))
    out_specs = P(("row", "col"), None, None, "layer", None)
    return jax.shard_map(
        on_each, mesh=mesh, in_specs=in_specs, out_specs=out_specs, check_vma=False
    )
```

```python
import functools

import jax
import jax.numpy as jnp
from jax import lax
from jax.experimental import pallas as pl
from jax.experimental.pallas import tpu as pltpu
from jax.sharding import PartitionSpec as P

MESH = pl.DeviceIdType.MESH


def divisor(total, most):
    return max(d for d in range(1, most + 1) if total % d == 0)


def kernel(
    sizes, columns_ref, tiles_ref, meta_ref, out_ref,
    left, right, meta_all, meta_smem, stage,
    local_sem, meta_send, meta_recv, send_sem, recv_sem, out_send, out_recv,
):
    row_count, col_count, layer_count, chunks, out_chunks, is_balanced = sizes
    n, group_count, slots, tile, _ = tiles_ref.shape
    cells = row_count * col_count
    per_layer = group_count // layer_count
    quarter = tile // layer_count
    width = group_count * slots
    r, c, l = lax.axis_index("row"), lax.axis_index("col"), lax.axis_index("layer")
    me = r * col_count + c
    own_groups = pl.ds(l * per_layer, per_layer)

    own_copy = pltpu.make_async_copy(
        tiles_ref.at[:, own_groups], right.at[pl.ds(me * n, n)], local_sem.at[0]
    )
    left_copy = pltpu.make_async_copy(tiles_ref, left, local_sem.at[1])
    meta_copy = pltpu.make_async_copy(meta_ref, meta_all.at[pl.ds(me * n, n)], local_sem.at[2])
    own_copy.start()
    meta_copy.start()
    left_copy.start()
    right[cells * n] = jnp.zeros(right.shape[1:], right.dtype)

    def cell_id(offset):
        target = lax.rem(me + offset, cells)
        return {"row": lax.div(target, col_count), "col": lax.rem(target, col_count)}

    def layer_id(offset):
        return {"layer": lax.rem(l + offset, layer_count)}

    barrier = pltpu.get_barrier_semaphore()
    for offset in range(1, cells):
        pl.semaphore_signal(barrier, inc=1, device_id=cell_id(offset), device_id_type=MESH)
    for offset in range(1, layer_count):
        pl.semaphore_signal(barrier, inc=1, device_id=layer_id(offset), device_id_type=MESH)
    pl.semaphore_wait(barrier, cells - 1 + layer_count - 1)
    own_copy.wait()

    step_rows = n // chunks
    sent = []

    def rows_of(cell, chunk):
        return pl.ds(cell * n + chunk * step_rows, step_rows)

    def copy_of(cell, chunk, way, device):
        return pltpu.make_async_remote_copy(
            src_ref=right.at[rows_of(cell, chunk)],
            dst_ref=right.at[rows_of(cell, chunk)],
            send_sem=send_sem.at[way, cell, chunk],
            recv_sem=recv_sem.at[cell, chunk],
            device_id=device,
            device_id_type=MESH,
        )

    ways = {
        "up": (0, c < col_count - 1, {"col": jnp.minimum(c + 1, col_count - 1)}),
        "down": (1, c > 0, {"col": jnp.maximum(c - 1, 0)}),
        "south": (2, r < row_count - 1, {"row": jnp.minimum(r + 1, row_count - 1)}),
        "north": (3, r > 0, {"row": jnp.maximum(r - 1, 0)}),
    }

    def send(cell, chunk, way, condition=True):
        index, exists, device = ways[way]
        wanted = jnp.logical_and(exists, condition)

        @pl.when(wanted)
        def _():
            copy_of(cell, chunk, index, device).start()

        sent.append((wanted, cell, chunk, index, device))

    def await_arrival(cell, chunk):
        copy_of(cell, chunk, 0, {"col": c}).wait_recv()

    for chunk in range(chunks):
        for way in ("up", "down", "south", "north"):
            send(me, chunk, way)

    meta_copy.wait()
    meta_copies = []
    for offset in range(1, cells):
        copy = pltpu.make_async_remote_copy(
            src_ref=meta_ref,
            dst_ref=meta_all.at[pl.ds(me * n, n)],
            send_sem=meta_send.at[offset],
            recv_sem=meta_recv.at[offset],
            device_id=cell_id(offset),
            device_id_type=MESH,
        )
        copy.start()
        meta_copies.append(copy)

    even = lax.rem(c, 2) == 0
    for step in range(1, col_count):
        for chunk in range(chunks):
            for origin, has, way, is_pair in (
                (c - step, c >= step, "up", jnp.logical_not(even)),
                (c + step, c + step < col_count, "down", even),
            ):
                origin = jnp.clip(origin, 0, col_count - 1)
                cell = r * col_count + origin

                @pl.when(has)
                def _():
                    await_arrival(cell, chunk)

                send(cell, chunk, way, has)
                across = has
                if is_balanced and step == 1 and chunk >= chunks // 2:
                    across = jnp.logical_and(has, jnp.logical_not(is_pair))
                send(cell, chunk, "south", across)
                send(cell, chunk, "north", across)

    if is_balanced:
        other = (1 - r) * col_count + c
        for chunk in range(chunks):
            await_arrival(other, chunk)
            if chunk >= chunks // 2:
                send(other, chunk, "up", even)
                send(other, chunk, "down", jnp.logical_not(even))
        for step in range(1, col_count):
            origin = (1 - r) * col_count + lax.rem(c + step, col_count)
            for chunk in range(chunks):
                await_arrival(origin, chunk)
    else:
        for step in range(1, row_count):
            for shift in range(col_count):
                for chunk in range(chunks):
                    for origin, has, way in (
                        (r - step, r >= step, "south"),
                        (r + step, r + step < row_count, "north"),
                    ):
                        origin = jnp.clip(origin, 0, row_count - 1)
                        cell = origin * col_count + lax.rem(c + shift, col_count)

                        @pl.when(has)
                        def _():
                            await_arrival(cell, chunk)

                        send(cell, chunk, way, has)

    for copy in meta_copies:
        copy.wait()
    table_copy = pltpu.make_async_copy(meta_all, meta_smem, local_sem.at[3])
    table_copy.start()
    table_copy.wait()
    left_copy.wait()

    def one_row(i, carry):
        targets = [
            columns_ref[i * width + l * per_layer * slots + s] for s in range(per_layer * slots)
        ]
        strips = []
        for a in range(width):
            k = columns_ref[i * width + a]
            inner = jnp.maximum(k, 0)
            pieces = []
            for s in range(per_layer * slots):
                group = s // slots
                row_index = jnp.int32(cells * n)
                slot_index = jnp.int32(0)
                is_live = (k >= 0) & (targets[s] >= 0)
                for t in range(slots):
                    hit = (meta_smem[inner, 0, group * slots + t] == targets[s]) & is_live
                    row_index = jnp.where(hit, inner, row_index)
                    slot_index = jnp.where(hit, t, slot_index)
                pieces.append(right[row_index, group, slot_index])
            strips.append(jnp.concatenate(pieces, axis=1))
        rights = jnp.concatenate(strips, axis=0)
        lefts = jnp.concatenate(
            [left[i, a // slots, a % slots] for a in range(width)], axis=1
        )
        total = jnp.dot(lefts, rights, preferred_element_type=jnp.float32).astype(stage.dtype)
        for q in range(layer_count):
            for s in range(per_layer * slots):
                stage[q, i, s // slots, s % slots] = total[
                    q * quarter:(q + 1) * quarter, s * tile:(s + 1) * tile
                ]
        return carry

    out_rows = n // out_chunks

    def out_copies(chunk):
        rows = pl.ds(chunk * out_rows, out_rows)
        copies = []
        for offset in range(layer_count):
            q = lax.rem(l + offset, layer_count)
            if offset == 0:
                copies.append(pltpu.make_async_copy(
                    stage.at[q, rows], out_ref.at[rows, own_groups], out_send.at[0, chunk]
                ))
            else:
                copies.append(pltpu.make_async_remote_copy(
                    src_ref=stage.at[q, rows],
                    dst_ref=out_ref.at[rows, own_groups],
                    send_sem=out_send.at[offset, chunk],
                    recv_sem=out_recv.at[offset, chunk],
                    device_id=layer_id(offset),
                    device_id_type=MESH,
                ))
        return copies

    all_out = []
    for chunk in range(out_chunks + 1):
        if chunk < out_chunks:
            lax.fori_loop(chunk * out_rows, (chunk + 1) * out_rows, one_row, 0)
        if chunk > 0:
            copies = out_copies(chunk - 1)
            for copy in copies[1:] + copies[:1]:
                copy.start()
            all_out.extend(copies)

    for wanted, cell, chunk, index, device in sent:
        @pl.when(wanted)
        def _():
            copy_of(cell, chunk, index, device).wait_send()

    for copy in all_out:
        copy.wait()


def on_device(density_tiles, tile_columns):
    row_count = lax.axis_size("row")
    col_count = lax.axis_size("col")
    layer_count = lax.axis_size("layer")
    n, group_count, slots, tile, _ = density_tiles.shape
    cells = row_count * col_count
    per_layer = group_count // layer_count
    quarter = tile // layer_count
    kept = per_layer * slots
    chunks = divisor(n, 4)
    out_chunks = divisor(n, 4)
    is_balanced = row_count == 2 and col_count % 2 == 0 and chunks % 2 == 0
    own = lax.dynamic_slice_in_dim(tile_columns, lax.axis_index("layer") * per_layer, per_layer, 1)
    meta = jnp.pad(own.reshape(n, 1, kept), ((0, 0), (0, 0), (0, 128 - kept)), constant_values=-1)
    dtype = density_tiles.dtype
    sizes = (row_count, col_count, layer_count, chunks, out_chunks, is_balanced)
    return pl.pallas_call(
        functools.partial(kernel, sizes),
        out_shape=jax.ShapeDtypeStruct((n, group_count, slots, quarter, tile), dtype),
        in_specs=[
            pl.BlockSpec(memory_space=pltpu.SMEM),
            pl.BlockSpec(memory_space=pl.ANY),
            pl.BlockSpec(memory_space=pltpu.VMEM),
        ],
        out_specs=pl.BlockSpec(memory_space=pl.ANY),
        scratch_shapes=[
            pltpu.VMEM(density_tiles.shape, dtype),
            pltpu.VMEM((cells * n + 1, per_layer, slots, tile, tile), dtype),
            pltpu.VMEM((cells * n, 1, 128), jnp.int32),
            pltpu.SMEM((cells * n, 1, 128), jnp.int32),
            pltpu.VMEM((layer_count, n, per_layer, slots, quarter, tile), dtype),
            pltpu.SemaphoreType.DMA((4,)),
            pltpu.SemaphoreType.DMA((cells,)),
            pltpu.SemaphoreType.DMA((cells,)),
            pltpu.SemaphoreType.DMA((4, cells, chunks)),
            pltpu.SemaphoreType.DMA((cells, chunks)),
            pltpu.SemaphoreType.DMA((layer_count, out_chunks)),
            pltpu.SemaphoreType.DMA((layer_count, out_chunks)),
        ],
        compiler_params=pltpu.CompilerParams(
            collective_id=0, has_side_effects=True, vmem_limit_bytes=60 * 1024 * 1024
        ),
    )(tile_columns.reshape(-1), density_tiles, meta)


def paired_kernel(
    sizes, tiles_ref, meta_ref, out_ref,
    left, right, meta_all, meta_smem, stage,
    local_sem, meta_send, meta_recv, send_sem, recv_sem, left_send, left_recv, out_send, out_recv,
):
    col_count, layer_count, chunks, out_chunks = sizes
    n, group_count, slots, tile, _ = tiles_ref.shape
    cells = 2 * col_count
    per_layer = group_count // layer_count
    quarter = tile // layer_count
    width = group_count * slots
    r, c, l = lax.axis_index("row"), lax.axis_index("col"), lax.axis_index("layer")
    high, k = lax.div(l, 2), lax.rem(l, 2)
    me = r * col_count + c
    base = k * col_count + c
    is_home = k == r
    is_guest = jnp.logical_not(is_home)
    group = 2 * high + r
    own_groups = pl.ds(group * per_layer, per_layer)
    other_groups = pl.ds((2 * high + 1 - r) * per_layer, per_layer)
    facing = {"row": 1 - r}
    partner = {"layer": 2 * high + 1 - k}

    own_copy = pltpu.make_async_copy(
        tiles_ref.at[:, own_groups], right.at[pl.ds(me * n, n)], local_sem.at[0]
    )
    left_copy = pltpu.make_async_copy(tiles_ref, left, local_sem.at[1])
    meta_copy = pltpu.make_async_copy(meta_ref, meta_all.at[pl.ds(me * n, n)], local_sem.at[2])
    own_copy.start()
    meta_copy.start()

    @pl.when(is_home)
    def _():
        left_copy.start()

    right[cells * n] = jnp.zeros(right.shape[1:], right.dtype)

    def cell_id(offset):
        target = lax.rem(me + offset, cells)
        return {"row": lax.div(target, col_count), "col": lax.rem(target, col_count)}

    barrier = pltpu.get_barrier_semaphore()
    for offset in range(1, cells):
        pl.semaphore_signal(barrier, inc=1, device_id=cell_id(offset), device_id_type=MESH)
    for offset in range(1, layer_count):
        for row in (r, 1 - r):
            pl.semaphore_signal(
                barrier,
                inc=1,
                device_id={"row": row, "layer": lax.rem(l + offset, layer_count)},
                device_id_type=MESH,
            )
    pl.semaphore_wait(barrier, cells - 1 + 2 * (layer_count - 1))

    step_rows = n // chunks
    sent = []

    def rows_of(cell, chunk):
        return pl.ds(cell * n + chunk * step_rows, step_rows)

    def copy_of(cell, chunk, way, device):
        source = right.at[rows_of(cell, chunk)]
        if way == 3:
            source = tiles_ref.at[pl.ds(chunk * step_rows, step_rows), other_groups]
        return pltpu.make_async_remote_copy(
            src_ref=source,
            dst_ref=right.at[rows_of(cell, chunk)],
            send_sem=send_sem.at[way, cell, chunk],
            recv_sem=recv_sem.at[cell, chunk],
            device_id=device,
            device_id_type=MESH,
        )

    ways = {
        "up": (0, c < col_count - 1, {"col": jnp.minimum(c + 1, col_count - 1)}),
        "down": (1, c > 0, {"col": jnp.maximum(c - 1, 0)}),
        "partner": (2, True, partner),
        "facing": (3, True, facing),
    }

    def send(cell, chunk, way, condition):
        index, exists, device = ways[way]
        wanted = jnp.logical_and(exists, condition)

        @pl.when(wanted)
        def _():
            copy_of(cell, chunk, index, device).start()

        sent.append((wanted, cell, chunk, index, device))

    def await_arrival(cell, chunk, condition):
        @pl.when(condition)
        def _():
            copy_of(cell, chunk, 2, partner).wait_recv()

    for chunk in range(chunks):
        send(me, chunk, "facing", is_home)
    own_copy.wait()
    for chunk in range(chunks):
        for way in ("up", "down"):
            send(me, chunk, way, is_home)
    left_out = pltpu.make_async_remote_copy(
        src_ref=tiles_ref, dst_ref=left, send_sem=left_send, recv_sem=left_recv,
        device_id=facing, device_id_type=MESH,
    )

    meta_copy.wait()
    meta_copies = []
    for offset in range(1, cells):
        copy = pltpu.make_async_remote_copy(
            src_ref=meta_ref,
            dst_ref=meta_all.at[pl.ds(me * n, n)],
            send_sem=meta_send.at[offset],
            recv_sem=meta_recv.at[offset],
            device_id=cell_id(offset),
            device_id_type=MESH,
        )
        copy.start()
        meta_copies.append(copy)

    @pl.when(is_home)
    def _():
        left_out.start()

    for chunk in range(chunks):
        await_arrival(base, chunk, is_guest)
        for way in ("up", "down", "partner"):
            send(base, chunk, way, is_guest)

    for step in range(1, col_count):
        for chunk in range(chunks):
            for origin, has, way in (
                (c - step, c >= step, "up"),
                (c + step, c + step < col_count, "down"),
            ):
                cell = k * col_count + jnp.clip(origin, 0, col_count - 1)
                await_arrival(cell, chunk, has)
                send(cell, chunk, way, has)
                send(cell, chunk, "partner", has)

    for chunk in range(chunks):
        await_arrival((1 - k) * col_count + c, chunk, is_home)
    for step in range(1, col_count):
        cell = (1 - k) * col_count + lax.rem(c + step, col_count)
        for chunk in range(chunks):
            await_arrival(cell, chunk, True)

    for copy in meta_copies:
        copy.wait()
    table_copy = pltpu.make_async_copy(meta_all, meta_smem, local_sem.at[3])
    table_copy.start()
    table_copy.wait()

    @pl.when(is_home)
    def _():
        left_copy.wait()

    @pl.when(is_guest)
    def _():
        left_out.wait_recv()

    first = group * per_layer * slots

    def one_row(i, carry):
        block_row = base * n + i
        targets = [meta_smem[block_row, 0, first + s] for s in range(per_layer * slots)]
        strips = []
        for a in range(width):
            column = meta_smem[block_row, 0, a]
            inner = jnp.maximum(column, 0)
            pieces = []
            for s in range(per_layer * slots):
                part = s // slots
                row_index = jnp.int32(cells * n)
                slot_index = jnp.int32(0)
                is_live = (column >= 0) & (targets[s] >= 0)
                for t in range(slots):
                    hit = (meta_smem[inner, 0, first + part * slots + t] == targets[s]) & is_live
                    row_index = jnp.where(hit, inner, row_index)
                    slot_index = jnp.where(hit, t, slot_index)
                pieces.append(right[row_index, part, slot_index])
            strips.append(jnp.concatenate(pieces, axis=1))
        rights = jnp.concatenate(strips, axis=0)
        lefts = jnp.concatenate(
            [left[i, a // slots, a % slots] for a in range(width)], axis=1
        )
        total = jnp.dot(lefts, rights, preferred_element_type=jnp.float32).astype(stage.dtype)
        for q in range(layer_count):
            for s in range(per_layer * slots):
                stage[q, i, s // slots, s % slots] = total[
                    q * quarter:(q + 1) * quarter, s * tile:(s + 1) * tile
                ]
        return carry

    out_rows = n // out_chunks

    def out_copy(chunk, q, source):
        rows = pl.ds(chunk * out_rows, out_rows)
        return pltpu.make_async_remote_copy(
            src_ref=stage.at[q, rows],
            dst_ref=out_ref.at[rows, pl.ds(source * per_layer, per_layer)],
            send_sem=out_send.at[q, chunk],
            recv_sem=out_recv.at[source, chunk],
            device_id={"row": k, "layer": q},
            device_id_type=MESH,
        )

    def kept_copy(chunk):
        rows = pl.ds(chunk * out_rows, out_rows)
        return pltpu.make_async_copy(
            stage.at[l, rows], out_ref.at[rows, own_groups], out_send.at[l, chunk]
        )

    for chunk in range(out_chunks + 1):
        if chunk < out_chunks:
            lax.fori_loop(chunk * out_rows, (chunk + 1) * out_rows, one_row, 0)
        if chunk > 0:
            for offset in range(layer_count - 1, -1, -1):
                q = lax.rem(l + offset, layer_count)
                if offset:
                    out_copy(chunk - 1, q, group).start()
                else:
                    @pl.when(is_guest)
                    def _():
                        out_copy(chunk - 1, q, group).start()

                    @pl.when(is_home)
                    def _():
                        kept_copy(chunk - 1).start()

    for wanted, cell, chunk, index, device in sent:
        @pl.when(wanted)
        def _():
            copy_of(cell, chunk, index, device).wait_send()

    @pl.when(is_home)
    def _():
        left_out.wait_send()

    for chunk in range(out_chunks):
        for offset in range(layer_count):
            q = lax.rem(l + offset, layer_count)
            source = lax.rem(group + offset, layer_count)
            if offset:
                out_copy(chunk, q, source).wait()
            else:
                @pl.when(is_guest)
                def _():
                    out_copy(chunk, q, source).wait()

                @pl.when(is_home)
                def _():
                    kept_copy(chunk).wait()


def on_device_paired(density_tiles, tile_columns):
    col_count = lax.axis_size("col")
    layer_count = lax.axis_size("layer")
    n, group_count, slots, tile, _ = density_tiles.shape
    cells = 2 * col_count
    per_layer = group_count // layer_count
    quarter = tile // layer_count
    width = group_count * slots
    chunks = divisor(n, 2)
    out_chunks = divisor(n, 12)
    lanes = -(-width // 128) * 128
    meta = jnp.pad(
        tile_columns.reshape(n, 1, width), ((0, 0), (0, 0), (0, lanes - width)), constant_values=-1
    )
    dtype = density_tiles.dtype
    return pl.pallas_call(
        functools.partial(paired_kernel, (col_count, layer_count, chunks, out_chunks)),
        out_shape=jax.ShapeDtypeStruct((n, group_count, slots, quarter, tile), dtype),
        in_specs=[
            pl.BlockSpec(memory_space=pl.ANY),
            pl.BlockSpec(memory_space=pltpu.VMEM),
        ],
        out_specs=pl.BlockSpec(memory_space=pl.ANY),
        scratch_shapes=[
            pltpu.VMEM(density_tiles.shape, dtype),
            pltpu.VMEM((cells * n + 1, per_layer, slots, tile, tile), dtype),
            pltpu.VMEM((cells * n, 1, lanes), jnp.int32),
            pltpu.SMEM((cells * n, 1, lanes), jnp.int32),
            pltpu.VMEM((layer_count, n, per_layer, slots, quarter, tile), dtype),
            pltpu.SemaphoreType.DMA((4,)),
            pltpu.SemaphoreType.DMA((cells,)),
            pltpu.SemaphoreType.DMA((cells,)),
            pltpu.SemaphoreType.DMA((4, cells, chunks)),
            pltpu.SemaphoreType.DMA((cells, chunks)),
            pltpu.SemaphoreType.DMA,
            pltpu.SemaphoreType.DMA,
            pltpu.SemaphoreType.DMA((layer_count, out_chunks)),
            pltpu.SemaphoreType.DMA((layer_count, out_chunks)),
        ],
        compiler_params=pltpu.CompilerParams(
            collective_id=1, has_side_effects=True, vmem_limit_bytes=60 * 1024 * 1024
        ),
    )(density_tiles, meta)


def sparse_kernel(
    sizes, tiles_ref, columns_ref, out_ref, flag_ref,
    left, diag, extra, lent, borrowed, pack, arrived, stage, total, needs, ranks, meta_own, meta_all, meta_smem,
    send_list, send_smem, row_list, row_smem, flag_all,
    local_sem, meta_send, meta_recv, flag_send, flag_recv,
    main_send, main_recv, side_send, side_recv, lent_sem, pack_send, pack_recv, extra_send, extra_recv, out_sem,
):
    row_count, col_count, layer_count, group_count, per_row, padded = sizes
    n, width, tile, _ = tiles_ref.shape
    per_lent, per_plane, pool = lent.shape[0], pack.shape[1], extra.shape[0]
    cells = row_count * col_count
    quarter = tile // layer_count
    entries = padded * width
    span = -(-(cells * n) // 128) * 128
    lists = -(-per_row // 8) * 8
    r, c, l = lax.axis_index("row"), lax.axis_index("col"), lax.axis_index("layer")
    x, k = lax.div(l, 2), lax.rem(l, 2)
    facing_layer = 2 * (1 - x) + k
    me = r * col_count + c
    opposite = (1 - r) * col_count + c
    own_slot = lax.div(me * n * group_count, cells * n) * (width // group_count)
    partner = {"layer": 2 * x + 1 - k}
    facing = {"layer": facing_layer}

    diag_copy = pltpu.make_async_copy(
        tiles_ref.at[:, own_slot], diag.at[pl.ds(me * n, n)], local_sem.at[1]
    )
    left_copy = pltpu.make_async_copy(tiles_ref, left, local_sem.at[2])
    table_copy = pltpu.make_async_copy(meta_own, meta_smem, local_sem.at[3])
    diag_copy.start()
    left_copy.start()
    meta_own[...] = jnp.full(meta_own.shape, -1, jnp.int32)
    meta_own[:, 0:n] = columns_ref[...]
    meta_all[me] = meta_own[...]

    def cell_id(cell):
        return {"row": lax.div(cell, col_count), "col": lax.rem(cell, col_count)}

    def other_cell(offset):
        return lax.rem(me + offset, cells)

    barrier = pltpu.get_barrier_semaphore()
    for offset in range(1, cells):
        pl.semaphore_signal(
            barrier, inc=1, device_id=cell_id(other_cell(offset)), device_id_type=MESH
        )
    for device in (partner, facing):
        pl.semaphore_signal(barrier, inc=1, device_id=device, device_id_type=MESH)
    pl.semaphore_wait(barrier, cells - 1 + 2)

    sent = []

    def remote(source, target, send, recv, device):
        return pltpu.make_async_remote_copy(
            src_ref=source, dst_ref=target, send_sem=send, recv_sem=recv,
            device_id=device, device_id_type=MESH,
        )

    def launch(copy, condition=True):
        if condition is True:
            copy.start()
        else:
            @pl.when(condition)
            def _():
                copy.start()
        sent.append((copy, condition))

    def await_recv(copy, condition=True):
        if condition is True:
            copy.wait_recv()
        else:
            @pl.when(condition)
            def _():
                copy.wait_recv()

    def part(cell, q):
        return diag.at[pl.ds(cell * n, n), pl.ds(q * quarter, quarter)]

    up = {"col": jnp.minimum(c + 1, col_count - 1)}
    down = {"col": jnp.maximum(c - 1, 0)}
    across = {"row": 1 - r}

    def line_copy(cell, way, wide=0):
        device = (up, down, across)[way]
        piece = part(cell, facing_layer if wide else l)
        return remote(
            piece, piece, main_send.at[wide, way, cell], main_recv.at[wide, cell], device
        )

    def side_copy(cell, way):
        device = (partner, facing, partner)[way]
        piece = part(cell, facing_layer if way == 2 else l)
        return remote(piece, piece, side_send.at[way, cell], side_recv.at[way, cell], device)

    meta_copies = []
    for offset in range(1, cells):
        copy = remote(
            meta_own, meta_all.at[me], meta_send.at[offset], meta_recv.at[offset],
            cell_id(other_cell(offset)),
        )
        copy.start()
        meta_copies.append(copy)
    diag_copy.wait()
    has_up, has_down = c < col_count - 1, c > 0
    launch(line_copy(me, 0), has_up)
    launch(line_copy(me, 1), has_down)
    launch(line_copy(me, 2))
    table_copy.start()
    for copy in meta_copies:
        copy.wait_recv()

    small_row = lax.broadcasted_iota(jnp.int32, (padded, 128), 0)
    small_lane = lax.broadcasted_iota(jnp.int32, (padded, 128), 1)
    wide_row = lax.broadcasted_iota(jnp.int32, (padded, span), 0)
    wide_lane = lax.broadcasted_iota(jnp.int32, (padded, span), 1)
    tall_row = lax.broadcasted_iota(jnp.int32, (span, 128), 0)
    entry_row = lax.broadcasted_iota(jnp.int32, (entries, 128), 0)
    entry_lane = lax.broadcasted_iota(jnp.int32, (entries, 128), 1).astype(jnp.float32)
    before = (
        lax.broadcasted_iota(jnp.int32, (entries, entries), 0)
        > lax.broadcasted_iota(jnp.int32, (entries, entries), 1)
    ).astype(jnp.float32).astype(jnp.bfloat16)
    ones = jnp.ones((128, 128), jnp.bfloat16)

    def dot(a, b):
        return jnp.dot(a, b, preferred_element_type=jnp.float32)

    def chosen(cell):
        columns = jnp.transpose(meta_all[cell])[0:padded]
        pieces = []
        for b in range(width):
            hit = (columns[:, b:b + 1] == wide_lane) & (wide_lane != wide_row + cell * n)
            pieces.append(jnp.where(hit, 1.0, 0.0))
        return jnp.concatenate(pieces, axis=0).astype(jnp.bfloat16)

    def listing(cell):
        rows = meta_all[cell]
        weight = jnp.zeros((span, 128), jnp.float32)
        for a in range(width):
            weight = jnp.where(rows[a:a + 1] == tall_row, a + 1.0, weight)
        return weight.astype(jnp.bfloat16)

    def inner_listing(source, cell):
        rows = meta_all[cell]
        weight = jnp.zeros((padded, 128), jnp.float32)
        for a in range(width):
            weight = jnp.where(rows[a:a + 1] == small_row + source * n, a + 1.0, weight)
        weight = jnp.where(small_row + source * n == small_lane + cell * n, 0.0, weight)
        return jnp.concatenate([weight] * width, axis=0)

    def matches(picked, listed, inner):
        goal = dot(picked, listed)
        hit = jnp.where((goal > 0) & (inner > 0), 1.0, 0.0)
        needed = jnp.where(dot(hit.astype(jnp.bfloat16), ones) > 0, 1.0, 0.0)
        return goal, hit, needed

    def rank_of(needed):
        return dot(before, needed.astype(jnp.bfloat16))

    def count_of(needed):
        return jnp.sum(needed, axis=0, keepdims=True)

    def picks_of(needed, rank, value):
        chosen_values = jnp.where((rank == entry_lane) & (needed > 0), value, 0.0)
        return jnp.sum(chosen_values, axis=0, keepdims=True)

    slot_value = (
        lax.rem(entry_row, padded) * width + lax.div(entry_row, padded)
    ).astype(jnp.float32)
    mine, theirs = chosen(me), chosen(opposite)
    none = jnp.zeros((entries, 128), jnp.float32)
    my_rows = pl.ds(pl.multiple_of(l * quarter, quarter), quarter)

    def lent_step(at, wanted):
        cell = (1 - r) * col_count + at
        return jnp.maximum(wanted, matches(mine, listing(cell), inner_listing(me, cell))[2])

    wanted = lax.fori_loop(0, col_count, lent_step, none, unroll=True)
    send_list[0:1] = picks_of(wanted, rank_of(wanted), slot_value).astype(jnp.int32)
    lent_most = count_of(wanted)
    lent_list = pltpu.make_async_copy(send_list.at[0], send_smem.at[0], local_sem.at[4])
    lent_list.start()
    lent_list.wait()
    left_copy.wait()

    def own_piece(code):
        code = jnp.clip(code, 0, n * width - 1)
        return left[lax.div(code, width), lax.rem(code, width), my_rows]

    def lent_pack(m, carry):
        lent[m] = own_piece(send_smem[0, m])
        return carry

    lax.fori_loop(0, per_lent, lent_pack, 0, unroll=8)
    lent_copy = remote(lent, borrowed, lent_sem.at[0], lent_sem.at[1], across)
    launch(lent_copy)

    def share(cell, condition=True, wide=False):
        launch(side_copy(cell, 0), condition)
        if not wide:
            launch(side_copy(cell, 1), condition)

    def take_line(cell, has, way, wide):
        await_recv(line_copy(cell, way), has)
        launch(line_copy(cell, way), jnp.logical_and(has, has_up if way == 0 else has_down))
        share(cell, has, wide)
        launch(line_copy(cell, 2), has)

    line, beyond = [], []
    for step in range(1, col_count):
        for origin, has, way in ((c - step, c >= step, 0), (c + step, c + step < col_count, 1)):
            origin = jnp.clip(origin, 0, col_count - 1)
            line.append((r * col_count + origin, has, way, step == 1))
            beyond.append(((1 - r) * col_count + origin, has))

    for entry in line[:2]:
        take_line(*entry)

    for entry in line[2:4]:
        take_line(*entry)

    def plane_step(at, wanted):
        cell = r * col_count + at
        listed = listing(cell)
        own = matches(mine, listed, inner_listing(me, cell))[2]
        send_list[pl.ds(8 + at, 1)] = picks_of(own, rank_of(own), slot_value).astype(jnp.int32)
        their = matches(theirs, listed, inner_listing(opposite, cell))[2]
        needs[at] = their
        ranks[at] = rank_of(their) + count_of(own)
        return jnp.maximum(wanted, their)

    wanted = lax.fori_loop(0, col_count, plane_step, none, unroll=True)
    borrowed_value = rank_of(wanted) + float(n * width)

    def plane_finish(at, carry):
        picks = picks_of(needs[at], ranks[at], borrowed_value).astype(jnp.int32)
        send_list[pl.ds(8 + at, 1)] += picks
        return carry

    lax.fori_loop(0, col_count, plane_finish, 0, unroll=True)
    rows_used = send_list.shape[0] - 8
    plane_list = pltpu.make_async_copy(
        send_list.at[pl.ds(8, rows_used)], send_smem.at[pl.ds(8, rows_used)], local_sem.at[4]
    )
    plane_list.start()

    await_recv(line_copy(opposite, 2))
    share(opposite, True, True)
    plane_list.wait()
    await_recv(lent_copy)

    def plane_piece(at, m):
        code = send_smem[8 + at, m]
        loaned = borrowed[jnp.clip(code - n * width, 0, per_lent - 1)]
        return jnp.where(code < n * width, own_piece(code), loaned)

    def plane_pack(m, carry):
        for offset in range(col_count):
            at = lax.rem(c + offset, col_count)
            if offset:
                pack[offset, m] = plane_piece(at, m)
            else:
                arrived[c, m] = plane_piece(at, m)
        return carry

    lax.fori_loop(0, per_plane, plane_pack, 0, unroll=4)

    def pack_copy(offset, origin):
        return remote(
            pack.at[offset], arrived.at[origin], pack_send.at[offset], pack_recv.at[origin],
            {"col": lax.rem(c + offset, col_count)},
        )

    for offset in sorted(range(1, col_count), key=lambda o: abs(2 * o - col_count)):
        launch(pack_copy(offset, c))

    def take_beyond(cell, has):
        await_recv(line_copy(cell, 2), has)
        share(cell, has)

    for entry in line[4:]:
        take_line(*entry)
    launch(line_copy(me, 2, 1))
    for entry in beyond[:2]:
        take_beyond(*entry)

    listed = listing(me)
    list_row = lax.broadcasted_iota(jnp.int32, (lists + 8, 128), 0)

    def row_step(at, carry):
        held, running, pooled, in_plane, most = carry
        plane, far = lax.div(at, 2), lax.rem(at, 2)
        source = jnp.where(far == 0, r, 1 - r) * col_count + plane
        in_plane = jnp.where(far == 0, 0.0, in_plane)
        inner = inner_listing(source, me)
        goal, hit, needed = matches(chosen(source), listed, inner)
        rank = rank_of(needed)
        place = dot(before, hit.astype(jnp.bfloat16)) + running
        value = (((rank + pooled) * 16.0 + (inner - 1.0)) * 16.0 + goal) * hit
        for q in range(per_row):
            line_sum = jnp.sum(jnp.where(place == float(q), value, 0.0), axis=0, keepdims=True)
            held = held + jnp.where(list_row == q, line_sum, 0.0)
        spot = rank + in_plane + (plane * per_plane).astype(jnp.float32)
        held = held + jnp.where(list_row == lists, picks_of(needed, rank + pooled, spot), 0.0)
        count = count_of(needed)
        in_plane = in_plane + count
        return held, running + count_of(hit), pooled + count, in_plane, jnp.maximum(most, in_plane)

    zero = jnp.zeros((1, 128), jnp.float32)
    held, running, pooled, _, most = lax.fori_loop(
        0, cells, row_step, (jnp.zeros((lists + 8, 128), jnp.float32), zero, zero, zero, zero),
        unroll=2,
    )
    row_list[...] = held.astype(jnp.int32)
    over = (most > per_plane) | (running > per_row) | (pooled > pool) | (lent_most > per_lent)
    flag_all[me] = jnp.broadcast_to(jnp.max(jnp.where(over, 1, 0)), (8, 128))
    row_copy = pltpu.make_async_copy(row_list, row_smem, local_sem.at[5])
    row_copy.start()
    flag_copies = []
    for offset in range(1, cells):
        copy = remote(
            flag_all.at[me], flag_all.at[me], flag_send.at[offset], flag_recv.at[offset],
            cell_id(other_cell(offset)),
        )
        copy.start()
        flag_copies.append(copy)

    def pass_on(cell, condition=True):
        await_recv(side_copy(cell, 1), condition)
        launch(side_copy(cell, 2), condition)

    def take_wide(cell, has, way, wide):
        await_recv(line_copy(cell, way, 1), has)
        launch(side_copy(cell, 2), has)

    for entry in beyond[2:]:
        take_beyond(*entry)
    launch(line_copy(me, 0, 1), has_up)
    launch(line_copy(me, 1, 1), has_down)
    row_copy.wait()
    for offset in range(1, col_count):
        await_recv(pack_copy(offset, lax.rem(c + offset, col_count)))

    def pool_pack(m, carry):
        code = jnp.clip(row_smem[lists, m], 0, col_count * per_plane - 1)
        extra[m, my_rows] = arrived[lax.div(code, per_plane), lax.rem(code, per_plane)]
        return carry

    lax.fori_loop(0, pool, pool_pack, 0, unroll=8)

    def extra_copy(way, half):
        device = (partner, facing, partner)[way]
        piece = extra.at[
            pl.ds(half * (pool // 2), pool // 2),
            pl.ds((facing_layer if way == 2 else l) * quarter, quarter),
        ]
        return remote(piece, piece, extra_send.at[way, half], extra_recv.at[way, half], device)

    for half in range(2):
        launch(extra_copy(1, half))
    for half in range(2):
        launch(extra_copy(0, half))
    for entry in line[:2]:
        take_wide(*entry)
    await_recv(line_copy(opposite, 2, 1))
    launch(side_copy(opposite, 2))
    for cell, has, _, _ in line[2:]:
        pass_on(cell, has)
    for cell, has in beyond:
        pass_on(cell, has)
    for offset in range(1, cells):
        await_recv(side_copy(other_cell(offset), 0))
        await_recv(side_copy(other_cell(offset), 2))
    table_copy.wait()

    def near_row(i, carry):
        own = left[i, own_slot, my_rows]
        pieces = []
        for t in range(width):
            column = meta_smem[t, i]
            lower = diag[jnp.maximum(column, 0)]
            own_left = left[i, t, my_rows]
            own_left = jnp.where(own_slot == t, jnp.zeros_like(own_left), own_left)
            value = dot(
                jnp.concatenate([own, own_left], axis=1),
                jnp.concatenate([left[i, t], lower], axis=0),
            )
            pieces.append(jnp.where(column >= 0, value, 0.0))
        total[i] = jnp.concatenate(pieces, axis=0)
        return carry

    lax.fori_loop(0, n, near_row, 0, unroll=2)
    for half in range(2):
        await_recv(extra_copy(1, half))
        launch(extra_copy(2, half))
    for half in range(2):
        await_recv(extra_copy(0, half))
        await_recv(extra_copy(2, half))

    def far_row(i, carry):
        values = [total[i, t * quarter:(t + 1) * quarter] for t in range(width)]
        for q in range(per_row):
            code = jnp.clip(row_smem[q, i], 0, pool * 256 - 1)
            goal = lax.rem(code, 16)
            at = jnp.minimum(lax.rem(lax.div(code, 16), 16), width - 1)
            value = dot(left[i, at, my_rows], extra[lax.div(code, 256)])
            values = [v + jnp.where(goal == t + 1, value, 0.0) for t, v in enumerate(values)]
        for t in range(width):
            stage[i, t] = values[t].astype(stage.dtype)
        return carry

    out_copies = []
    for chunk in range(n // 8):
        lax.fori_loop(chunk * 8, chunk * 8 + 8, far_row, 0, unroll=8)
        rows = pl.ds(chunk * 8, 8)
        out_copies.append(pltpu.make_async_copy(
            stage.at[rows], out_ref.at[rows], out_sem.at[chunk]
        ))
        out_copies[-1].start()
    for copy in flag_copies:
        copy.wait_recv()
    flag_ref[0, 0] = jnp.max(flag_all[...])
    for copy in meta_copies + flag_copies:
        copy.wait_send()
    for copy, condition in sent:
        if condition is True:
            copy.wait_send()
        else:
            @pl.when(condition)
            def _():
                copy.wait_send()
    for copy in out_copies:
        copy.wait()


def on_device_sparse(density_tiles, tile_columns):
    row_count = lax.axis_size("row")
    col_count = lax.axis_size("col")
    layer_count = lax.axis_size("layer")
    n, group_count, slots, tile, _ = density_tiles.shape
    cells = row_count * col_count
    quarter = tile // layer_count
    width = group_count * slots
    per_lent, per_plane, pool, per_row = 32, 24, 56, 8
    padded = -(-n // 32) * 32
    dtype = density_tiles.dtype
    sizes = (row_count, col_count, layer_count, group_count, per_row, padded)
    lists = -(-per_row // 8) * 8
    planes = -(-col_count // 8) * 8
    out, flag = pl.pallas_call(
        functools.partial(sparse_kernel, sizes),
        out_shape=(
            jax.ShapeDtypeStruct((n, width, quarter, tile), dtype),
            jax.ShapeDtypeStruct((1, 1), jnp.int32),
        ),
        in_specs=[
            pl.BlockSpec(memory_space=pl.ANY),
            pl.BlockSpec(memory_space=pltpu.VMEM),
        ],
        out_specs=(
            pl.BlockSpec(memory_space=pl.ANY),
            pl.BlockSpec(memory_space=pltpu.SMEM),
        ),
        scratch_shapes=[
            pltpu.VMEM((n, width, tile, tile), dtype),
            pltpu.VMEM((cells * n, tile, tile), dtype),
            pltpu.VMEM((pool, tile, tile), dtype),
            pltpu.VMEM((per_lent, quarter, tile), dtype),
            pltpu.VMEM((per_lent, quarter, tile), dtype),
            pltpu.VMEM((col_count, per_plane, quarter, tile), dtype),
            pltpu.VMEM((col_count, per_plane, quarter, tile), dtype),
            pltpu.VMEM((n, width, quarter, tile), dtype),
            pltpu.VMEM((n, width * quarter, tile), jnp.float32),
            pltpu.VMEM((col_count, padded * width, 128), jnp.float32),
            pltpu.VMEM((col_count, padded * width, 128), jnp.float32),
            pltpu.VMEM((width, 128), jnp.int32),
            pltpu.VMEM((cells, width, 128), jnp.int32),
            pltpu.SMEM((width, 128), jnp.int32),
            pltpu.VMEM((8 + planes, 128), jnp.int32),
            pltpu.SMEM((8 + planes, 128), jnp.int32),
            pltpu.VMEM((lists + 8, 128), jnp.int32),
            pltpu.SMEM((lists + 8, 128), jnp.int32),
            pltpu.VMEM((cells, 8, 128), jnp.int32),
            pltpu.SemaphoreType.DMA((7,)),
            pltpu.SemaphoreType.DMA((cells,)),
            pltpu.SemaphoreType.DMA((cells,)),
            pltpu.SemaphoreType.DMA((cells,)),
            pltpu.SemaphoreType.DMA((cells,)),
            pltpu.SemaphoreType.DMA((2, 3, cells)),
            pltpu.SemaphoreType.DMA((2, cells)),
            pltpu.SemaphoreType.DMA((3, cells)),
            pltpu.SemaphoreType.DMA((3, cells)),
            pltpu.SemaphoreType.DMA((2,)),
            pltpu.SemaphoreType.DMA((col_count,)),
            pltpu.SemaphoreType.DMA((col_count,)),
            pltpu.SemaphoreType.DMA((3, 2)),
            pltpu.SemaphoreType.DMA((3, 2)),
            pltpu.SemaphoreType.DMA((n // 8,)),
        ],
        compiler_params=pltpu.CompilerParams(
            collective_id=2, has_side_effects=True, vmem_limit_bytes=60 * 1024 * 1024
        ),
    )(density_tiles.reshape(n, width, tile, tile), tile_columns.reshape(n, width).T)
    out = out.reshape(n, group_count, slots, quarter, tile)
    return lax.cond(
        flag[0, 0] > 0,
        lambda: on_device_paired(density_tiles, tile_columns),
        lambda: out,
    )


def solution(mesh):
    paired = mesh.shape["row"] == 2 and mesh.shape["layer"] % 2 == 0
    four = paired and mesh.shape["layer"] == 4

    def on_each(density_tiles, tile_columns):
        n, group_count, slots, tile, _ = density_tiles.shape
        block_count = n * mesh.shape["row"] * mesh.shape["col"]
        fits = four and n % 8 == 0 and n <= 128 and group_count * slots <= 15 and slots > 0
        fits = fits and (block_count // group_count) % n == 0 and tile % 128 == 0
        fits = fits and mesh.shape["col"] <= 16
        if fits:
            return on_device_sparse(density_tiles, tile_columns)
        return (on_device_paired if paired else on_device)(density_tiles, tile_columns)

    in_specs = (P(("row", "col"), None, None, None, None), P(("row", "col"), None, None))
    out_specs = P(("row", "col"), None, None, "layer", None)
    return jax.shard_map(
        on_each, mesh=mesh, in_specs=in_specs, out_specs=out_specs, check_vma=False
    )
```
